16 devices in a mesh: dp: 2 (over y, z), tp: 8 (over x, core).
Axes of the slice: x: 4, y: 2, z: 1, core: 2. Of those that a mesh axis runs over, the one named last changes fastest.
The devices are a block of a 4x4x8 slice.
Arguments:
- hidden: bfloat16 [128, 1, 2048], P('dp'), parts along dimension 0
- ln_gain: bfloat16 [2, 2, 2048], replicated
- ln_shift: bfloat16 [2, 2, 2048], replicated
- w_qkv: bfloat16 [2, 2048, 6144], P(None, None, 'tp')
- b_qkv: bfloat16 [2, 6144], P(None, 'tp')
- w_out: bfloat16 [2, 2048, 2048], P(None, 'tp')
- b_out: bfloat16 [2, 2048], replicated
- w_up: bfloat16 [2, 2048, 8192], P(None, None, 'tp')
- b_up: bfloat16 [2, 8192], P(None, 'tp')
- w_down: bfloat16 [2, 8192, 2048], P(None, 'tp')
- b_down: bfloat16 [2, 2048], replicated
- k_cache: bfloat16 [2, 128, 256, 16, 128], P(None, 'dp', None, 'tp'), parts along dimension 1
- v_cache: bfloat16 [2, 128, 256, 16, 128], P(None, 'dp', None, 'tp'), parts along dimension 1
- write_slot: int32 [128], P('dp'), parts along dimension 0
- key_pos: int32 [128, 256], P('dp'), parts along dimension 0
- key_valid: int32 [128, 256], P('dp'), parts along dimension 0
Outputs:
- output 1: bfloat16 [128, 1, 2048], P('dp'), parts along dimension 0
- output 2: bfloat16 [2, 128, 256, 16, 128], P(None, 'dp', None, 'tp'), parts along dimension 1
- output 3: bfloat16 [2, 128, 256, 16, 128], P(None, 'dp', None, 'tp'), parts along dimension 1
There are 2 independent parts. The reference program is written for one: setup_inputs(seed, part) draws one part's arguments, and reference() takes and returns one part's arrays. A program takes and returns all parts, laid end to end along the dimension named above; an argument that names none is the same for every part.
All inputs are finite; a program needn't handle non-finite values.
Results may differ from the reference program's by a relative error of at most 0.0132686.
Values are sent between devices in bfloat16 or wider.
A program may use at most 768 MiB of HBM per device.

```python
import math
import jax
import jax.numpy as jnp
from jax import lax

HIDDEN = 2048
HEADS = 16
HEAD = 128
BATCH = 64
CACHE = 256
LAYERS = 2

FFN = 4 * HIDDEN
LN_EPS = 1e-5


def alibi_slopes(n_heads):
    return jnp.exp2(-8.0 * jnp.arange(1, n_heads + 1).astype(jnp.float32) / n_heads)


def layer_norm(x_rows, gain, shift):
    x_f32 = x_rows.astype(jnp.float32)
    mean_val = jnp.mean(x_f32, axis=-1, keepdims=True)
    centered = x_f32 - mean_val
    var_val = jnp.mean(centered * centered, axis=-1, keepdims=True)
    normed = centered * lax.rsqrt(var_val + LN_EPS)
    return (normed * gain.astype(jnp.float32) + shift.astype(jnp.float32)).astype(jnp.bfloat16)


def draw_normal(key, shape):
    return jax.random.normal(key, shape, jnp.float32)


def draw_layout(slot_key, pad_key):
    write_slot = jax.random.randint(slot_key, (BATCH,), 0, CACHE, dtype=jnp.int32)
    write_slot = write_slot.at[0].set(CACHE - 1)
    pad_len = jax.random.randint(pad_key, (BATCH,), 0, write_slot + 1, dtype=jnp.int32)
    pad_len = pad_len.at[0].set(0)
    t_index = jnp.arange(CACHE, dtype=jnp.int32)[None, :]
    in_row = jnp.logical_and(t_index >= pad_len[:, None], t_index <= write_slot[:, None])
    key_valid = jnp.logical_and(in_row, t_index < write_slot[:, None]).astype(jnp.int32)
    key_pos = jnp.where(in_row, t_index - pad_len[:, None], 0).astype(jnp.int32)
    return write_slot, key_pos, key_valid


def setup_inputs(seed: int = 0, part: int = 0) -> dict:
    root = jax.random.key(seed)
    wkeys = jax.random.split(root, 10)
    own_keys = jax.random.split(jax.random.fold_in(root, part), 5)
    scale_hid = HIDDEN ** -0.5
    scale_ffn = FFN ** -0.5
    write_slot, key_pos, key_valid = draw_layout(own_keys[3], own_keys[4])
    return {
        'hidden': draw_normal(own_keys[0], (BATCH, 1, HIDDEN)).astype(jnp.bfloat16),
        'ln_gain': (1.0 + 0.3 * draw_normal(wkeys[0], (LAYERS, 2, HIDDEN))).astype(jnp.bfloat16),
        'ln_shift': (0.3 * draw_normal(wkeys[1], (LAYERS, 2, HIDDEN))).astype(jnp.bfloat16),
        'w_qkv': (scale_hid * draw_normal(wkeys[2], (LAYERS, HIDDEN, 3 * HIDDEN))).astype(jnp.bfloat16),
        'b_qkv': (0.3 * draw_normal(wkeys[3], (LAYERS, 3 * HIDDEN))).astype(jnp.bfloat16),
        'w_out': (2.0 * scale_hid * draw_normal(wkeys[4], (LAYERS, HIDDEN, HIDDEN))).astype(jnp.bfloat16),
        'b_out': (0.5 * draw_normal(wkeys[5], (LAYERS, HIDDEN))).astype(jnp.bfloat16),
        'w_up': (scale_hid * draw_normal(wkeys[6], (LAYERS, HIDDEN, FFN))).astype(jnp.bfloat16),
        'b_up': (0.5 * draw_normal(wkeys[7], (LAYERS, FFN))).astype(jnp.bfloat16),
        'w_down': (scale_ffn * draw_normal(wkeys[8], (LAYERS, FFN, HIDDEN))).astype(jnp.bfloat16),
        'b_down': (0.5 * draw_normal(wkeys[9], (LAYERS, HIDDEN))).astype(jnp.bfloat16),
        'k_cache': draw_normal(own_keys[1], (LAYERS, BATCH, CACHE, HEADS, HEAD)).astype(jnp.bfloat16),
        'v_cache': draw_normal(own_keys[2], (LAYERS, BATCH, CACHE, HEADS, HEAD)).astype(jnp.bfloat16),
        'write_slot': write_slot,
        'key_pos': key_pos,
        'key_valid': key_valid,
    }


def reference(hidden, ln_gain, ln_shift, w_qkv, b_qkv, w_out, b_out, w_up, b_up, w_down, b_down, k_cache, v_cache, write_slot, key_pos, key_valid):
    slopes = alibi_slopes(HEADS)
    t_index = jnp.arange(CACHE, dtype=jnp.int32)[None, :]
    is_new = t_index == write_slot[:, None]
    allowed = jnp.logical_or(key_valid > 0, is_new)
    pos_bias = slopes[None, :, None] * key_pos.astype(jnp.float32)[:, None, :]
    pos_bias = jnp.where(allowed[:, None, :], pos_bias, -jnp.inf)
    new_mask = is_new[:, :, None, None]
    score_scale = 1.0 / math.sqrt(HEAD)

    def layer_step(x_cur, layer_args):
        gain, shift, wq_mat, bq_vec, wo_mat, bo_vec, wu_mat, bu_vec, wd_mat, bd_vec, k_old, v_old = layer_args
        normed = layer_norm(x_cur, gain[0], shift[0])
        qkv_out = (jnp.dot(normed, wq_mat, preferred_element_type=jnp.float32) + bq_vec.astype(jnp.float32)).astype(jnp.bfloat16)
        qkv_out = qkv_out.reshape(BATCH, HEADS, 3, HEAD)
        k_all = jnp.where(new_mask, qkv_out[:, None, :, 1, :], k_old)
        v_all = jnp.where(new_mask, qkv_out[:, None, :, 2, :], v_old)
        scores = jnp.einsum('bhd,bthd->bht', qkv_out[:, :, 0, :].astype(jnp.float32), k_all.astype(jnp.float32)) * score_scale + pos_bias
        attn_probs = jax.nn.softmax(scores, axis=-1).astype(jnp.bfloat16)
        attn_out = jnp.einsum('bht,bthd->bhd', attn_probs.astype(jnp.float32), v_all.astype(jnp.float32)).astype(jnp.bfloat16)
        proj_sum = jnp.dot(attn_out.reshape(BATCH, HIDDEN), wo_mat, preferred_element_type=jnp.float32)
        x_mid = (x_cur.astype(jnp.float32) + proj_sum + bo_vec.astype(jnp.float32)).astype(jnp.bfloat16)
        normed_mlp = layer_norm(x_mid, gain[1], shift[1])
        up_act = jnp.dot(normed_mlp, wu_mat, preferred_element_type=jnp.float32) + bu_vec.astype(jnp.float32)
        gelu_out = jax.nn.gelu(up_act, approximate=True).astype(jnp.bfloat16)
        down_sum = jnp.dot(gelu_out, wd_mat, preferred_element_type=jnp.float32)
        x_next = (x_mid.astype(jnp.float32) + down_sum + bd_vec.astype(jnp.float32)).astype(jnp.bfloat16)
        return x_next, (k_all, v_all)

    x_last, caches = lax.scan(layer_step, hidden[:, 0, :], (ln_gain, ln_shift, w_qkv, b_qkv, w_out, b_out, w_up, b_up, w_down, b_down, k_cache, v_cache))
    return x_last[:, None, :], caches[0], caches[1]
```

```python
import functools
import math

import jax
import jax.numpy as jnp
from jax import lax
from jax.experimental import pallas as pl
from jax.experimental.pallas import tpu as pltpu
from jax.sharding import PartitionSpec as P

LN_EPS = 1e-5
MESH = pl.DeviceIdType.MESH
F32 = jnp.float32
BF16 = jnp.bfloat16
GROUP = 8
MIB = 2 ** 20


def layer_norm_f32(x_f32, gain, shift):
    mean_val = jnp.mean(x_f32, axis=-1, keepdims=True)
    centered = x_f32 - mean_val
    var_val = jnp.mean(centered * centered, axis=-1, keepdims=True)
    normed = centered * lax.rsqrt(var_val + LN_EPS)
    return (normed * gain.astype(F32) + shift.astype(F32)).astype(BF16)


def attn_kernel(layer, n_heads, first, *refs):
    if first:
        (x_ref, gain_ref, shift_ref, wq_hbm, bq_ref, wo_hbm, slot_smem, slot_ref, pos_ref, valid_ref, k_hbm, v_hbm,
         part_ref, k_out, v_out,
         wq, wo, kbuf, vbuf, qkv, bias, attn, sem_w, sem_in, sem_out) = refs
    else:
        (x_ref, gain_ref, shift_ref, wq_hbm, bq_ref, wo_hbm, slot_smem, slot_ref, pos_ref, valid_ref, k_hbm, v_hbm,
         k_alias, v_alias,
         part_ref, k_out, v_out,
         wq, wo, kbuf, vbuf, qkv, bias, attn, sem_w, sem_in, sem_out) = refs
    n_batch, n_cols, head_dim = kbuf.shape
    n_groups = n_batch // GROUP
    n_local = attn.shape[1] // head_dim
    width = x_ref.shape[1]
    cache_len = n_cols // n_local
    n_chunk = 4
    step = width // n_chunk
    w_copies = [
        pltpu.make_async_copy(wq_hbm.at[layer, pl.ds(i * step, step)], wq.at[pl.ds(i * step, step)], sem_w.at[i])
        for i in range(n_chunk)
    ]
    for c in w_copies:
        c.start()

    def in_copy(which, g):
        src, dst = ((k_hbm, kbuf), (v_hbm, vbuf))[which]
        return pltpu.make_async_copy(src.at[layer, pl.ds(g * GROUP, GROUP)], dst.at[pl.ds(g * GROUP, GROUP)], sem_in.at[which, g])

    def out_copy(which, g):
        src, dst = ((kbuf, k_out), (vbuf, v_out))[which]
        return pltpu.make_async_copy(src.at[pl.ds(g * GROUP, GROUP)], dst.at[layer, pl.ds(g * GROUP, GROUP)], sem_out.at[which])

    for g in range(n_groups):
        in_copy(0, g).start()
        in_copy(1, g).start()
    wo_copy = pltpu.make_async_copy(wo_hbm.at[layer], wo, sem_w.at[n_chunk])
    wo_copy.start()

    t_row = lax.broadcasted_iota(jnp.int32, (cache_len, n_cols), 0)
    t_col = lax.broadcasted_iota(jnp.int32, (cache_len, n_cols), 1) // n_local
    spread = (t_row == t_col).astype(BF16)
    pos = jnp.dot(pos_ref[...].astype(F32).astype(BF16), spread, preferred_element_type=F32)
    valid = jnp.dot(valid_ref[...].astype(F32).astype(BF16), spread, preferred_element_type=F32)
    col = lax.broadcasted_iota(jnp.int32, (n_batch, n_cols), 1)
    allowed = jnp.logical_or(valid > 0.5, col // n_local == slot_ref[...])
    head0 = lax.axis_index('tp') * n_local
    for h in range(n_local):
        num = (jnp.full((n_batch, n_cols), 1 + h, jnp.int32) + head0).astype(F32)
        slope = jnp.exp2(-8.0 * num / n_heads)
        keep = jnp.logical_and(allowed, col % n_local == h)
        bias[h] = jnp.where(keep, slope * pos, -jnp.inf)

    if first:
        x_in = layer_norm_f32(x_ref[...].astype(F32), gain_ref[layer, 0:1], shift_ref[layer, 0:1])
    else:
        x_in = x_ref[...]
    acc = None
    for i in range(n_chunk):
        w_copies[i].wait()
        d = jnp.dot(x_in[:, i * step:(i + 1) * step], wq[i * step:(i + 1) * step], preferred_element_type=F32)
        acc = d if acc is None else acc + d
    qkv[...] = (acc + bq_ref[layer:layer + 1].astype(F32)).astype(BF16).astype(F32)

    scale = 1.0 / math.sqrt(head_dim)
    rows = n_local * GROUP

    def group(g, carry):
        in_copy(0, g).wait()
        in_copy(1, g).wait()
        base = pl.multiple_of(g * GROUP, GROUP)
        row16 = lax.broadcasted_iota(jnp.int32, (16, head_dim), 0)
        fresh = qkv[pl.ds(base, GROUP), :]
        for b in range(GROUP):
            first_row = slot_smem[g * GROUP + b] * n_local
            start = pl.multiple_of((first_row // 16) * 16, 16)
            off = first_row - start
            for which, buf in ((1, kbuf), (2, vbuf)):
                block = buf[base + b, pl.ds(start, 16), :].astype(F32)
                for h in range(n_local):
                    new = fresh[b:b + 1, (3 * h + which) * head_dim:(3 * h + which + 1) * head_dim]
                    block = jnp.where(row16 == off + h, new, block)
                buf[base + b, pl.ds(start, 16), :] = block.astype(BF16)
        q16 = jnp.concatenate(
            [fresh[:, 3 * h * head_dim:(3 * h + 1) * head_dim] for h in range(n_local)], axis=0
        ).astype(BF16)
        row_s = lax.broadcasted_iota(jnp.int32, (rows, n_cols), 0) % GROUP
        s = None
        for b in range(GROUP):
            sb = lax.dot_general(q16, kbuf[base + b], (((1,), (1,)), ((), ())), preferred_element_type=F32)
            s = sb if s is None else jnp.where(row_s == b, sb, s)
        s = s * scale + jnp.concatenate([bias[h, pl.ds(base, GROUP)] for h in range(n_local)], axis=0)
        top = jnp.max(s, axis=-1, keepdims=True)
        e = jnp.exp(s - top)
        p = (e * (1.0 / jnp.sum(e, axis=-1, keepdims=True))).astype(BF16)
        row_o = lax.broadcasted_iota(jnp.int32, (rows, head_dim), 0) % GROUP
        o = None
        for b in range(GROUP):
            ob = jnp.dot(p, vbuf[base + b], preferred_element_type=F32)
            o = ob if o is None else jnp.where(row_o == b, ob, o)
        for h in range(n_local):
            attn[pl.ds(base, GROUP), h * head_dim:(h + 1) * head_dim] = o[h * GROUP:(h + 1) * GROUP]
        out_copy(0, g).start()
        out_copy(1, g).start()
        return carry

    lax.fori_loop(0, n_groups, group, 0)
    wo_copy.wait()
    part_ref[...] = jnp.dot(attn[...].astype(BF16), wo[...], preferred_element_type=F32)
    for g in range(n_groups):
        out_copy(0, g).wait()
        out_copy(1, g).wait()


def reduce_kernel(layer, n_tp, last, *refs):
    n_out = 1 if last else 2
    (part_ref, res_ref, gain_ref, shift_ref, bo_ref, wu_hbm, bu_ref, wd_hbm, bd_ref) = refs[:9]
    out_ref = refs[9]
    own_ref = None if last else refs[10]
    (wu, wd, part2, d2d, mid, got, gath, gath2, sem_w, pair_s, pair_r, chip_s, chip_r, ag_s, ag_r, agp_s, agp_r) = refs[9 + n_out:]
    n_batch, width = part_ref.shape
    n_chip = n_tp // 2
    blk = n_batch // n_tp
    me = lax.axis_index('tp')
    x = me // 2
    c = me % 2
    partner = x * 2 + (1 - c)

    def chip(d):
        return lax.rem(x + d, n_chip)

    w_copies = [pltpu.make_async_copy(wu_hbm.at[layer], wu, sem_w.at[0]), pltpu.make_async_copy(wd_hbm.at[layer], wd, sem_w.at[1])]
    for w in w_copies:
        w.start()
    barrier = pltpu.get_barrier_semaphore()
    peers = [partner] + [chip(d) * 2 + c for d in range(1, n_chip)]
    for peer in peers:
        pl.semaphore_signal(barrier, inc=1, device_id={'tp': peer}, device_id_type=MESH)
    pl.semaphore_wait(barrier, len(peers))

    order = [2, 1, 3, 0] if n_chip == 4 else list(range(1, n_chip)) + [0]

    def rows_of(core, d):
        return pl.ds(pl.multiple_of((core * n_chip + chip(d)) * blk, blk), blk)

    def reduce_scatter(phase, src):
        pair = {
            d: pltpu.make_async_remote_copy(
                src_ref=src.at[rows_of(1 - c, d)], dst_ref=d2d.at[phase, d], send_sem=pair_s.at[phase, d],
                recv_sem=pair_r.at[phase, d], device_id={'tp': partner}, device_id_type=MESH)
            for d in order
        }
        for d in order:
            pair[d].start()
        hops = {}
        acc = None
        for d in order:
            pair[d].wait_recv()
            both = src[rows_of(c, d), :] + d2d[phase, d]
            if d == 0:
                acc = both
            else:
                mid[phase, d] = both
                hops[d] = pltpu.make_async_remote_copy(
                    src_ref=mid.at[phase, d], dst_ref=got.at[phase, d], send_sem=chip_s.at[phase, d],
                    recv_sem=chip_r.at[phase, d], device_id={'tp': chip(d) * 2 + c}, device_id_type=MESH)
                hops[d].start()
        for d in sorted(hops, key=lambda d: min(d, n_chip - d)):
            hops[d].wait_recv()
            acc = acc + got[phase, d]
        for d in order:
            pair[d].wait_send()
            if d:
                hops[d].wait_send()
        return acc

    def all_gather(phase, buf, value):
        buf[c, x] = value
        hops = {}
        for d in order[:-1]:
            hops[d] = pltpu.make_async_remote_copy(
                src_ref=buf.at[c, x], dst_ref=buf.at[c, x], send_sem=ag_s.at[phase, d], recv_sem=ag_r.at[phase, d],
                device_id={'tp': chip(d) * 2 + c}, device_id_type=MESH)
            hops[d].start()

        def pass_on(d):
            slot = lax.rem(x + n_chip - d, n_chip)
            cp = pltpu.make_async_remote_copy(
                src_ref=buf.at[c, slot], dst_ref=buf.at[c, slot], send_sem=agp_s.at[phase, d], recv_sem=agp_r.at[phase, d],
                device_id={'tp': partner}, device_id_type=MESH)
            cp.start()
            return cp

        passed = [pass_on(0)]
        for d in sorted(hops, key=lambda d: min(d, n_chip - d)):
            hops[d].wait_recv()
            passed.append(pass_on(d))
        for cp in passed:
            cp.wait()
        for d in hops:
            hops[d].wait_send()
        return buf[...].astype(F32).reshape(n_batch, width)

    if last:
        res = res_ref[...].astype(F32)
    else:
        res = res_ref[rows_of(c, 0), :].astype(F32)
    total = reduce_scatter(0, part_ref)
    x_mid = (res + total + bo_ref[layer:layer + 1].astype(F32)).astype(BF16).astype(F32)
    normed = all_gather(0, gath, layer_norm_f32(x_mid, gain_ref[layer, 1:2], shift_ref[layer, 1:2])).astype(BF16)
    w_copies[0].wait()
    up = jnp.dot(normed, wu[...], preferred_element_type=F32) + bu_ref[layer:layer + 1].astype(F32)
    act = jax.nn.gelu(up, approximate=True).astype(BF16)
    w_copies[1].wait()
    part2[...] = jnp.dot(act, wd[...], preferred_element_type=F32)
    total = reduce_scatter(1, part2)
    x_next = (x_mid + total + bd_ref[layer:layer + 1].astype(F32)).astype(BF16)
    if last:
        out_ref[...] = all_gather(1, gath2, x_next).astype(BF16)
    else:
        own_ref[...] = x_next
        nxt = layer_norm_f32(x_next.astype(F32), gain_ref[layer + 1, 0:1], shift_ref[layer + 1, 0:1])
        out_ref[...] = all_gather(1, gath2, nxt).astype(BF16)


def solution(mesh):
    tp_size = mesh.shape['tp']
    vm = pl.BlockSpec(memory_space=pltpu.VMEM)
    sm = pl.BlockSpec(memory_space=pltpu.SMEM)
    hbm = pl.BlockSpec(memory_space=pltpu.HBM)

    def device_step(hidden, ln_gain, ln_shift, w_qkv, b_qkv, w_out, b_out, w_up, b_up, w_down, b_down, k_cache, v_cache, write_slot, key_pos, key_valid):
        n_layers, n_batch, cache_len, n_local, head_dim = k_cache.shape
        width = hidden.shape[-1]
        n_cols = cache_len * n_local
        flat = (n_layers, n_batch, n_cols, head_dim)
        in_hbm = functools.partial(pltpu.with_memory_space_constraint, memory_space=pltpu.HBM)
        k_in, v_in = in_hbm(k_cache.reshape(flat)), in_hbm(v_cache.reshape(flat))
        w_qkv, w_out, w_up, w_down = map(in_hbm, (w_qkv, w_out, w_up, w_down))
        x0 = hidden.reshape(n_batch, width)
        slot_col = write_slot.reshape(n_batch, 1)
        n_groups = n_batch // GROUP
        blk = n_batch // tp_size
        n_chip = tp_size // 2

        def attn(layer, x_in, caches):
            first = caches is None
            ins = [x_in, ln_gain, ln_shift, w_qkv, b_qkv, w_out, write_slot, slot_col, key_pos, key_valid, k_in, v_in]
            specs = [vm, vm, vm, hbm, vm, hbm, sm, vm, vm, vm, hbm, hbm]
            alias = {}
            if not first:
                alias = {len(ins): 1, len(ins) + 1: 2}
                ins += list(caches)
                specs += [hbm, hbm]
            shape = jax.ShapeDtypeStruct(flat, BF16)
            return pl.pallas_call(
                functools.partial(attn_kernel, layer, n_local * tp_size, first),
                out_shape=(jax.ShapeDtypeStruct((n_batch, width), F32), shape, shape),
                in_specs=specs,
                out_specs=(vm, hbm, hbm),
                scratch_shapes=[
                    pltpu.VMEM(w_qkv.shape[1:], BF16),
                    pltpu.VMEM(w_out.shape[1:], BF16),
                    pltpu.VMEM(flat[1:], BF16),
                    pltpu.VMEM(flat[1:], BF16),
                    pltpu.VMEM((n_batch, b_qkv.shape[1]), F32),
                    pltpu.VMEM((n_local, n_batch, n_cols), F32),
                    pltpu.VMEM((n_batch, n_local * head_dim), F32),
                    pltpu.SemaphoreType.DMA((5,)),
                    pltpu.SemaphoreType.DMA((2, n_groups)),
                    pltpu.SemaphoreType.DMA((2,)),
                ],
                input_output_aliases=alias,
                compiler_params=pltpu.CompilerParams(vmem_limit_bytes=48 * MIB),
                name=f'attn_{layer}',
            )(*ins)

        def reduce(layer, part, res):
            last = layer == n_layers - 1
            ins = [part, res, ln_gain, ln_shift, b_out, w_up, b_up, w_down, b_down]
            specs = [vm, vm, vm, vm, vm, hbm, vm, hbm, vm]
            outs = [jax.ShapeDtypeStruct((n_batch, width), BF16)]
            if not last:
                outs.append(jax.ShapeDtypeStruct((blk, width), BF16))
            dma = pltpu.SemaphoreType.DMA((2, n_chip))
            return pl.pallas_call(
                functools.partial(reduce_kernel, layer, tp_size, last),
                out_shape=tuple(outs),
                in_specs=specs,
                out_specs=tuple([vm] * len(outs)),
                scratch_shapes=[
                    pltpu.VMEM(w_up.shape[1:], BF16),
                    pltpu.VMEM(w_down.shape[1:], BF16),
                    pltpu.VMEM((n_batch, width), F32),
                    pltpu.VMEM((2, n_chip, blk, width), F32),
                    pltpu.VMEM((2, n_chip, blk, width), F32),
                    pltpu.VMEM((2, n_chip, blk, width), F32),
                    pltpu.VMEM((2, n_chip, blk, width), BF16),
                    pltpu.VMEM((2, n_chip, blk, width), BF16),
                    pltpu.SemaphoreType.DMA((2,)),
                ] + [dma] * 8,
                compiler_params=pltpu.CompilerParams(vmem_limit_bytes=32 * MIB, collective_id=layer, has_side_effects=True),
                name=f'reduce_{layer}',
            )(*ins)

        caches, x_in, res = None, x0, x0
        for layer in range(n_layers):
            part, k_new, v_new = attn(layer, x_in, caches)
            caches = (k_new, v_new)
            outs = reduce(layer, part, res)
            x_in = outs[0]
            res = outs[-1]
        return x_in[:, None, :], caches[0].reshape(k_cache.shape), caches[1].reshape(v_cache.shape)

    cache_spec = P(None, 'dp', None, 'tp', None)
    in_specs = (P('dp', None, None), P(), P(), P(None, None, 'tp'), P(None, 'tp'), P(None, 'tp', None), P(), P(None, None, 'tp'), P(None, 'tp'), P(None, 'tp', None), P(), cache_spec, cache_spec, P('dp'), P('dp', None), P('dp', None))
    out_specs = (P('dp', None, None), cache_spec, cache_spec)
    return jax.shard_map(device_step, mesh=mesh, in_specs=in_specs, out_specs=out_specs, check_vma=False)
```

```python
import functools
import math

import jax
import jax.numpy as jnp
from jax import lax
from jax.experimental import pallas as pl
from jax.experimental.pallas import tpu as pltpu
from jax.sharding import PartitionSpec as P

LN_EPS = 1e-5
MESH = pl.DeviceIdType.MESH
F32 = jnp.float32
BF16 = jnp.bfloat16
GROUP = 8
MIB = 2 ** 20


def layer_norm_f32(x_f32, gain, shift):
    mean_val = jnp.mean(x_f32, axis=-1, keepdims=True)
    centered = x_f32 - mean_val
    var_val = jnp.mean(centered * centered, axis=-1, keepdims=True)
    normed = centered * lax.rsqrt(var_val + LN_EPS)
    return (normed * gain.astype(F32) + shift.astype(F32)).astype(BF16)


def attn_kernel(layer, n_heads, first, *refs):
    if first:
        (x_in_ref, gain_in, shift_in, bq_in, wq_hbm, wo_hbm, slot_hbm, pos_in, valid_in, k_hbm, v_hbm,
         part_ref, kall, vall,
         x_ref, gain_ref, shift_ref, bq_ref, pos_ref, valid_ref, slot_smem,
         wq, wo, qkv, bias, attn, sem_w, sem_s, sem_in) = refs
    else:
        (x_ref, bq_in, wq_hbm, wo_hbm, slot_hbm, pos_in, valid_in, k_raw, v_raw,
         part_ref, k_out, v_out, kall, vall,
         bq_ref, pos_ref, valid_ref, slot_smem,
         wq, wo, qkv, bias, attn, sem_w, sem_s, sem_out) = refs
    kbuf, vbuf = kall.at[layer], vall.at[layer]
    n_batch, n_cols, head_dim = kbuf.shape
    n_groups = n_batch // GROUP
    n_local = attn.shape[1] // head_dim
    width = x_ref.shape[1]
    cache_len = n_cols // n_local
    n_chunk = 4
    step = width // n_chunk
    pairs = [(slot_hbm, slot_smem), (pos_in, pos_ref), (valid_in, valid_ref), (bq_in, bq_ref)]
    if first:
        pairs = [(x_in_ref, x_ref), (gain_in, gain_ref), (shift_in, shift_ref)] + pairs
    small = [pltpu.make_async_copy(src, dst, sem_s.at[i]) for i, (src, dst) in enumerate(pairs)]
    for c in small:
        c.start()
    w_copies = [
        pltpu.make_async_copy(wq_hbm.at[layer, pl.ds(i * step, step)], wq.at[pl.ds(i * step, step)], sem_w.at[i])
        for i in range(n_chunk)
    ]
    for c in w_copies:
        c.start()
    wo_copy = pltpu.make_async_copy(wo_hbm.at[layer], wo, sem_w.at[n_chunk])

    def in_copy(which, g):
        src, dst = ((k_hbm, kbuf), (v_hbm, vbuf))[which]
        return pltpu.make_async_copy(src.at[layer, pl.ds(g * GROUP, GROUP)], dst.at[pl.ds(g * GROUP, GROUP)], sem_in.at[which, g])

    def out_copy(which, g):
        src, dst = ((kbuf, k_out), (vbuf, v_out))[which]
        return pltpu.make_async_copy(src.at[pl.ds(g * GROUP, GROUP)], dst.at[layer, pl.ds(g * GROUP, GROUP)], sem_out.at[which])

    if first:
        for g in range(n_groups):
            in_copy(0, g).start()
            in_copy(1, g).start()
        wo_copy.start()
        old = []
    else:
        wo_copy.start()
        old = [
            pltpu.make_async_copy(src.at[layer - 1, pl.ds(g * GROUP, GROUP)], dst.at[layer - 1, pl.ds(g * GROUP, GROUP)], sem_out.at[2 + i])
            for g in range(n_groups) for i, (src, dst) in enumerate(((kall, k_out), (vall, v_out)))
        ]
        for c in old:
            c.start()

    t_row = lax.broadcasted_iota(jnp.int32, (cache_len, n_cols), 0)
    t_col = lax.broadcasted_iota(jnp.int32, (cache_len, n_cols), 1) // n_local
    spread = (t_row == t_col).astype(BF16)
    for c in small:
        c.wait()
    pos = jnp.dot(pos_ref[...].astype(F32).astype(BF16), spread, preferred_element_type=F32)
    valid = jnp.dot(valid_ref[...].astype(F32).astype(BF16), spread, preferred_element_type=F32)
    bias[0] = pos
    bias[1] = valid

    if first:
        x_in = layer_norm_f32(x_ref[...].astype(F32), gain_ref[layer, 0:1], shift_ref[layer, 0:1])
    else:
        x_in = x_ref[...]
    acc = None
    for i in range(n_chunk):
        w_copies[i].wait()
        d = jnp.dot(x_in[:, i * step:(i + 1) * step], wq[i * step:(i + 1) * step], preferred_element_type=F32)
        acc = d if acc is None else acc + d
    qkv[...] = (acc + bq_ref[layer:layer + 1].astype(F32)).astype(BF16).astype(F32)

    scale = 1.0 / math.sqrt(head_dim)
    rows = n_local * GROUP
    head0 = lax.axis_index('tp') * n_local

    def group(g, carry):
        if first:
            in_copy(0, g).wait()
            in_copy(1, g).wait()
        base = pl.multiple_of(g * GROUP, GROUP)
        row16 = lax.broadcasted_iota(jnp.int32, (16, head_dim), 0)
        fresh = qkv[pl.ds(base, GROUP), :]
        row8 = lax.broadcasted_iota(jnp.int32, (GROUP, n_cols), 0)
        slots = jnp.zeros((GROUP, n_cols), jnp.int32)
        for b in range(GROUP):
            slot = slot_smem[g * GROUP + b]
            slots = jnp.where(row8 == b, slot, slots)
            first_row = slot * n_local
            start = pl.multiple_of((first_row // 16) * 16, 16)
            off = first_row - start
            for which, buf in ((1, kbuf), (2, vbuf)):
                block = buf[base + b, pl.ds(start, 16), :].astype(F32)
                for h in range(n_local):
                    new = fresh[b:b + 1, (3 * h + which) * head_dim:(3 * h + which + 1) * head_dim]
                    block = jnp.where(row16 == off + h, new, block)
                buf[base + b, pl.ds(start, 16), :] = block.astype(BF16)
        col = lax.broadcasted_iota(jnp.int32, (GROUP, n_cols), 1)
        allowed = jnp.logical_or(bias[1, pl.ds(base, GROUP)] > 0.5, col // n_local == slots)
        pos_g = bias[0, pl.ds(base, GROUP)]
        parts = []
        for h in range(n_local):
            num = (jnp.full((GROUP, n_cols), 1 + h, jnp.int32) + head0).astype(F32)
            slope = jnp.exp2(-8.0 * num / n_heads)
            parts.append(jnp.where(jnp.logical_and(allowed, col % n_local == h), slope * pos_g, -jnp.inf))
        q16 = jnp.concatenate(
            [fresh[:, 3 * h * head_dim:(3 * h + 1) * head_dim] for h in range(n_local)], axis=0
        ).astype(BF16)
        row_s = lax.broadcasted_iota(jnp.int32, (rows, n_cols), 0) % GROUP
        s = None
        for b in range(GROUP):
            sb = lax.dot_general(q16, kbuf[base + b], (((1,), (1,)), ((), ())), preferred_element_type=F32)
            s = sb if s is None else jnp.where(row_s == b, sb, s)
        s = s * scale + jnp.concatenate(parts, axis=0)
        top = jnp.max(s, axis=-1, keepdims=True)
        e = jnp.exp(s - top)
        p = (e * (1.0 / jnp.sum(e, axis=-1, keepdims=True))).astype(BF16)
        row_o = lax.broadcasted_iota(jnp.int32, (rows, head_dim), 0) % GROUP
        o = None
        for b in range(GROUP):
            ob = jnp.dot(p, vbuf[base + b], preferred_element_type=F32)
            o = ob if o is None else jnp.where(row_o == b, ob, o)
        for h in range(n_local):
            attn[pl.ds(base, GROUP), h * head_dim:(h + 1) * head_dim] = o[h * GROUP:(h + 1) * GROUP]
        if not first:
            out_copy(0, g).start()
            out_copy(1, g).start()
        return carry

    lax.fori_loop(0, n_groups, group, 0)
    wo_copy.wait()
    part_ref[...] = jnp.dot(attn[...].astype(BF16), wo[...], preferred_element_type=F32)
    if not first:
        for c in old:
            c.wait()
        for g in range(n_groups):
            out_copy(0, g).wait()
            out_copy(1, g).wait()


def reduce_kernel(layer, n_tp, last, *refs):
    if last:
        part_ref, res_ref, gain_ref, shift_ref, bo_ref, wu_hbm, bu_ref, wd_hbm, bd_ref, out_ref = refs[:10]
        rest = refs[10:]
    else:
        (part_ref, res_ref, gain_ref, shift_ref, bo_ref, wu_hbm, bu_ref, wd_hbm, bd_ref, k_hbm, v_hbm, k_raw, v_raw,
         out_ref, own_ref, kall, vall) = refs[:17]
        rest = refs[17:]
    (wu, wd, part2, d2d, mid, got, gath, gath2, sem_w, pair_s, pair_r, chip_s, chip_r, ag_s, ag_r, agp_s, agp_r) = rest
    n_batch, width = part_ref.shape
    n_chip = n_tp // 2
    blk = n_batch // n_tp
    me = lax.axis_index('tp')
    x = me // 2
    c = me % 2
    partner = x * 2 + (1 - c)

    def chip(d):
        return lax.rem(x + d, n_chip)

    w_copies = [pltpu.make_async_copy(wu_hbm.at[layer], wu, sem_w.at[0]), pltpu.make_async_copy(wd_hbm.at[layer], wd, sem_w.at[1])]
    if not last:
        w_copies.append(pltpu.make_async_copy(k_hbm.at[layer + 1], kall.at[layer + 1], sem_w.at[2]))
        w_copies.append(pltpu.make_async_copy(v_hbm.at[layer + 1], vall.at[layer + 1], sem_w.at[3]))
    for w in w_copies:
        w.start()
    barrier = pltpu.get_barrier_semaphore()
    peers = [partner] + [chip(d) * 2 + c for d in range(1, n_chip)]
    for peer in peers:
        pl.semaphore_signal(barrier, inc=1, device_id={'tp': peer}, device_id_type=MESH)
    pl.semaphore_wait(barrier, len(peers))

    order = [2, 1, 3, 0] if n_chip == 4 else list(range(1, n_chip)) + [0]

    def rows_of(core, d):
        return pl.ds(pl.multiple_of((core * n_chip + chip(d)) * blk, blk), blk)

    def reduce_scatter(phase, src):
        pair = {
            d: pltpu.make_async_remote_copy(
                src_ref=src.at[rows_of(1 - c, d)], dst_ref=d2d.at[phase, d], send_sem=pair_s.at[phase, d],
                recv_sem=pair_r.at[phase, d], device_id={'tp': partner}, device_id_type=MESH)
            for d in order
        }
        for d in order:
            pair[d].start()
        hops = {}
        acc = None
        for d in order:
            pair[d].wait_recv()
            both = src[rows_of(c, d), :] + d2d[phase, d]
            if d == 0:
                acc = both
            else:
                mid[phase, d] = both
                hops[d] = pltpu.make_async_remote_copy(
                    src_ref=mid.at[phase, d], dst_ref=got.at[phase, d], send_sem=chip_s.at[phase, d],
                    recv_sem=chip_r.at[phase, d], device_id={'tp': chip(d) * 2 + c}, device_id_type=MESH)
                hops[d].start()
        for d in sorted(hops, key=lambda d: min(d, n_chip - d)):
            hops[d].wait_recv()
            acc = acc + got[phase, d]
        for d in order:
            pair[d].wait_send()
            if d:
                hops[d].wait_send()
        return acc

    def all_gather(phase, buf, value):
        buf[c, x] = value
        hops = {}
        for d in order[:-1]:
            hops[d] = pltpu.make_async_remote_copy(
                src_ref=buf.at[c, x], dst_ref=buf.at[c, x], send_sem=ag_s.at[phase, d], recv_sem=ag_r.at[phase, d],
                device_id={'tp': chip(d) * 2 + c}, device_id_type=MESH)
            hops[d].start()

        def pass_on(d):
            slot = lax.rem(x + n_chip - d, n_chip)
            cp = pltpu.make_async_remote_copy(
                src_ref=buf.at[c, slot], dst_ref=buf.at[c, slot], send_sem=agp_s.at[phase, d], recv_sem=agp_r.at[phase, d],
                device_id={'tp': partner}, device_id_type=MESH)
            cp.start()
            return cp

        passed = [pass_on(0)]
        for d in sorted(hops, key=lambda d: min(d, n_chip - d)):
            hops[d].wait_recv()
            passed.append(pass_on(d))
        for cp in passed:
            cp.wait()
        for d in hops:
            hops[d].wait_send()
        return buf[...].astype(F32).reshape(n_batch, width)

    if last:
        res = res_ref[...].astype(F32)
    else:
        res = res_ref[rows_of(c, 0), :].astype(F32)
    total = reduce_scatter(0, part_ref)
    x_mid = (res + total + bo_ref[layer:layer + 1].astype(F32)).astype(BF16).astype(F32)
    normed = all_gather(0, gath, layer_norm_f32(x_mid, gain_ref[layer, 1:2], shift_ref[layer, 1:2])).astype(BF16)
    w_copies[0].wait()
    up = jnp.dot(normed, wu[...], preferred_element_type=F32) + bu_ref[layer:layer + 1].astype(F32)
    act = jax.nn.gelu(up, approximate=True).astype(BF16)
    w_copies[1].wait()
    part2[...] = jnp.dot(act, wd[...], preferred_element_type=F32)
    total = reduce_scatter(1, part2)
    x_next = (x_mid + total + bd_ref[layer:layer + 1].astype(F32)).astype(BF16)
    if last:
        out_ref[...] = all_gather(1, gath2, x_next).astype(BF16)
    else:
        own_ref[...] = x_next
        nxt = layer_norm_f32(x_next.astype(F32), gain_ref[layer + 1, 0:1], shift_ref[layer + 1, 0:1])
        out_ref[...] = all_gather(1, gath2, nxt).astype(BF16)
        w_copies[2].wait()
        w_copies[3].wait()


def solution(mesh):
    tp_size = mesh.shape['tp']
    vm = pl.BlockSpec(memory_space=pltpu.VMEM)
    sm = pl.BlockSpec(memory_space=pltpu.SMEM)
    hbm = pl.BlockSpec(memory_space=pltpu.HBM)

    def device_step(hidden, ln_gain, ln_shift, w_qkv, b_qkv, w_out, b_out, w_up, b_up, w_down, b_down, k_cache, v_cache, write_slot, key_pos, key_valid):
        n_layers, n_batch, cache_len, n_local, head_dim = k_cache.shape
        width = hidden.shape[-1]
        n_cols = cache_len * n_local
        flat = (n_layers, n_batch, n_cols, head_dim)
        in_hbm = functools.partial(pltpu.with_memory_space_constraint, memory_space=pltpu.HBM)
        k_in, v_in = in_hbm(k_cache.reshape(flat)), in_hbm(v_cache.reshape(flat))
        w_qkv, w_out, w_up, w_down = map(in_hbm, (w_qkv, w_out, w_up, w_down))
        x0 = hidden.reshape(n_batch, width)
        n_groups = n_batch // GROUP
        blk = n_batch // tp_size
        n_chip = tp_size // 2
        shape = jax.ShapeDtypeStruct(flat, BF16)
        held = pltpu.VMEM(flat, BF16)
        shared = [in_hbm(a) for a in (b_qkv, w_qkv, w_out, write_slot, key_pos, key_valid)]

        def attn(layer, x_in, caches):
            first = layer == 0
            small = [pltpu.VMEM(b_qkv.shape, BF16), pltpu.VMEM(key_pos.shape, jnp.int32), pltpu.VMEM(key_valid.shape, jnp.int32), pltpu.SMEM(write_slot.shape, jnp.int32)]
            alias = {}
            part = jax.ShapeDtypeStruct((n_batch, width), F32)
            if first:
                ins = [in_hbm(x_in), in_hbm(ln_gain), in_hbm(ln_shift)] + shared + [k_in, v_in]
                specs = [hbm] * len(ins)
                small = [pltpu.VMEM(x_in.shape, BF16), pltpu.VMEM(ln_gain.shape, BF16), pltpu.VMEM(ln_shift.shape, BF16)] + small
                outs, out_specs = (part, held, held), (vm, vm, vm)
            else:
                ins = [x_in] + shared + list(caches)
                specs = [vm] + [hbm] * len(shared) + [vm] * 2
                outs, out_specs = (part, shape, shape, held, held), (vm, hbm, hbm, vm, vm)
                alias = {len(ins) - 2: 3, len(ins) - 1: 4}
            return pl.pallas_call(
                functools.partial(attn_kernel, layer, n_local * tp_size, first),
                out_shape=outs,
                in_specs=specs,
                out_specs=out_specs,
                scratch_shapes=small + [
                    pltpu.VMEM(w_qkv.shape[1:], BF16),
                    pltpu.VMEM(w_out.shape[1:], BF16),
                    pltpu.VMEM((n_batch, b_qkv.shape[1]), F32),
                    pltpu.VMEM((2, n_batch, n_cols), F32),
                    pltpu.VMEM((n_batch, n_local * head_dim), F32),
                    pltpu.SemaphoreType.DMA((5,)),
                    pltpu.SemaphoreType.DMA((7,)),
                    pltpu.SemaphoreType.DMA((2, n_groups) if first else (4,)),
                ],
                input_output_aliases=alias,
                compiler_params=pltpu.CompilerParams(vmem_limit_bytes=14 * MIB),
                name=f'attn_{layer}',
            )(*ins)

        def reduce(layer, part, res, caches=()):
            last = layer == n_layers - 1
            ins = [part, res, ln_gain, ln_shift, b_out, w_up, b_up, w_down, b_down]
            specs = [vm, vm, vm, vm, vm, hbm, vm, hbm, vm]
            outs = [jax.ShapeDtypeStruct((n_batch, width), BF16)]
            if not last:
                ins += [k_in, v_in, *caches]
                specs += [hbm, hbm, vm, vm]
                outs += [jax.ShapeDtypeStruct((blk, width), BF16), held, held]
            dma = pltpu.SemaphoreType.DMA((2, n_chip))
            return pl.pallas_call(
                functools.partial(reduce_kernel, layer, tp_size, last),
                out_shape=tuple(outs),
                in_specs=specs,
                out_specs=tuple([vm] * len(outs)),
                scratch_shapes=[
                    pltpu.VMEM(w_up.shape[1:], BF16),
                    pltpu.VMEM(w_down.shape[1:], BF16),
                    pltpu.VMEM((n_batch, width), F32),
                    pltpu.VMEM((2, n_chip, blk, width), F32),
                    pltpu.VMEM((2, n_chip, blk, width), F32),
                    pltpu.VMEM((2, n_chip, blk, width), F32),
                    pltpu.VMEM((2, n_chip, blk, width), BF16),
                    pltpu.VMEM((2, n_chip, blk, width), BF16),
                    pltpu.SemaphoreType.DMA((4,)),
                ] + [dma] * 8,
                input_output_aliases={} if last else {len(ins) - 2: 2, len(ins) - 1: 3},
                compiler_params=pltpu.CompilerParams(vmem_limit_bytes=14 * MIB, collective_id=layer, has_side_effects=True),
                name=f'reduce_{layer}',
            )(*ins)

        part, k_held, v_held = attn(0, x0, None)
        h1, x1, k_held, v_held = reduce(0, part, x0, (k_held, v_held))
        part, k_new, v_new = attn(1, h1, (k_held, v_held))[:3]
        (x_last,) = reduce(1, part, x1)
        return x_last[:, None, :], k_new.reshape(k_cache.shape), v_new.reshape(v_cache.shape)

    cache_spec = P(None, 'dp', None, 'tp', None)
    in_specs = (P('dp', None, None), P(), P(), P(None, None, 'tp'), P(None, 'tp'), P(None, 'tp', None), P(), P(None, None, 'tp'), P(None, 'tp'), P(None, 'tp', None), P(), cache_spec, cache_spec, P('dp'), P('dp', None), P('dp', None))
    out_specs = (P('dp', None, None), cache_spec, cache_spec)
    return jax.shard_map(device_step, mesh=mesh, in_specs=in_specs, out_specs=out_specs, check_vma=False)
```

```python
import functools
import math

import jax
import jax.numpy as jnp
from jax import lax
from jax.experimental import pallas as pl
from jax.experimental.pallas import tpu as pltpu
from jax.sharding import PartitionSpec as P

LN_EPS = 1e-5
MESH = pl.DeviceIdType.MESH
F32 = jnp.float32
BF16 = jnp.bfloat16
GROUP = 8
AHEAD = 3
MIB = 2 ** 20


def layer_norm_f32(x_f32, gain, shift):
    mean_val = jnp.mean(x_f32, axis=-1, keepdims=True)
    centered = x_f32 - mean_val
    var_val = jnp.mean(centered * centered, axis=-1, keepdims=True)
    normed = centered * lax.rsqrt(var_val + LN_EPS)
    return (normed * gain.astype(F32) + shift.astype(F32)).astype(BF16)


def attn_kernel(layer, n_heads, first, *refs):
    if first:
        (x_in_ref, gain_in, shift_in, bq_in, wq_hbm, slot_hbm, pos_in, valid_in, k_hbm, v_hbm,
         attn_ref, kall, vall,
         x_ref, gain_ref, shift_ref, bq_ref, pos_ref, valid_ref, slot_smem,
         wq, qkv, bias, attn, sem_w, sem_s, sem_in) = refs
    else:
        (x_ref, bq_in, wq_hbm, slot_hbm, pos_in, valid_in, k_raw, v_raw,
         attn_ref, k_out, v_out, kall, vall,
         bq_ref, pos_ref, valid_ref, slot_smem,
         wq, qkv, bias, attn, sem_w, sem_s, sem_out) = refs
    kbuf, vbuf = kall.at[layer], vall.at[layer]
    n_batch, n_cols, head_dim = kbuf.shape
    n_groups = n_batch // GROUP
    n_local = attn.shape[1] // head_dim
    width = x_ref.shape[1]
    cache_len = n_cols // n_local
    n_chunk = 4
    step = width // n_chunk
    pairs = [(slot_hbm, slot_smem), (pos_in, pos_ref), (valid_in, valid_ref), (bq_in, bq_ref)]
    if first:
        pairs = [(x_in_ref, x_ref), (gain_in, gain_ref), (shift_in, shift_ref)] + pairs
    small = [pltpu.make_async_copy(src, dst, sem_s.at[i]) for i, (src, dst) in enumerate(pairs)]
    for c in small:
        c.start()
    w_copies = [
        pltpu.make_async_copy(wq_hbm.at[layer, pl.ds(i * step, step)], wq.at[pl.ds(i * step, step)], sem_w.at[i])
        for i in range(n_chunk)
    ]
    for c in w_copies:
        c.start()

    def in_copy(which, g):
        src, dst = ((k_hbm, kbuf), (v_hbm, vbuf))[which]
        return pltpu.make_async_copy(src.at[layer, pl.ds(g * GROUP, GROUP)], dst.at[pl.ds(g * GROUP, GROUP)], sem_in.at[which, g])

    def out_copy(which, g):
        src, dst = ((kbuf, k_out), (vbuf, v_out))[which]
        return pltpu.make_async_copy(src.at[pl.ds(g * GROUP, GROUP)], dst.at[layer, pl.ds(g * GROUP, GROUP)], sem_out.at[which])

    if first:
        for g in range(AHEAD):
            in_copy(0, g).start()
            in_copy(1, g).start()
    else:
        old = [
            pltpu.make_async_copy(src.at[layer - 1, pl.ds(g * GROUP, GROUP)], dst.at[layer - 1, pl.ds(g * GROUP, GROUP)], sem_out.at[2 + i])
            for g in range(n_groups) for i, (src, dst) in enumerate(((kall, k_out), (vall, v_out)))
        ]
        for c in old:
            c.start()

    t_row = lax.broadcasted_iota(jnp.int32, (cache_len, n_cols), 0)
    t_col = lax.broadcasted_iota(jnp.int32, (cache_len, n_cols), 1) // n_local
    spread = (t_row == t_col).astype(BF16)
    for c in small:
        c.wait()
    pos = jnp.dot(pos_ref[...].astype(F32).astype(BF16), spread, preferred_element_type=F32)
    valid = jnp.dot(valid_ref[...].astype(F32).astype(BF16), spread, preferred_element_type=F32)
    bias[0] = pos
    bias[1] = valid

    if first:
        x_in = layer_norm_f32(x_ref[...].astype(F32), gain_ref[layer, 0:1], shift_ref[layer, 0:1])
    else:
        x_in = x_ref[...]
    acc = None
    for i in range(n_chunk):
        w_copies[i].wait()
        d = jnp.dot(x_in[:, i * step:(i + 1) * step], wq[i * step:(i + 1) * step], preferred_element_type=F32)
        acc = d if acc is None else acc + d
    qkv[...] = (acc + bq_ref[layer:layer + 1].astype(F32)).astype(BF16).astype(F32)

    scale = 1.0 / math.sqrt(head_dim)
    rows = n_local * GROUP
    head0 = lax.axis_index('tp') * n_local

    def group(g, carry):
        if first:
            in_copy(0, g).wait()
            in_copy(1, g).wait()

            @pl.when(g + AHEAD < n_groups)
            def _():
                in_copy(0, g + AHEAD).start()
                in_copy(1, g + AHEAD).start()
        base = pl.multiple_of(g * GROUP, GROUP)
        row16 = lax.broadcasted_iota(jnp.int32, (16, head_dim), 0)
        fresh = qkv[pl.ds(base, GROUP), :]
        row8 = lax.broadcasted_iota(jnp.int32, (GROUP, n_cols), 0)
        slots = jnp.zeros((GROUP, n_cols), jnp.int32)
        for b in range(GROUP):
            slot = slot_smem[g * GROUP + b]
            slots = jnp.where(row8 == b, slot, slots)
            first_row = slot * n_local
            start = pl.multiple_of((first_row // 16) * 16, 16)
            off = first_row - start
            for which, buf in ((1, kbuf), (2, vbuf)):
                block = buf[base + b, pl.ds(start, 16), :].astype(F32)
                for h in range(n_local):
                    new = fresh[b:b + 1, (3 * h + which) * head_dim:(3 * h + which + 1) * head_dim]
                    block = jnp.where(row16 == off + h, new, block)
                buf[base + b, pl.ds(start, 16), :] = block.astype(BF16)
        col = lax.broadcasted_iota(jnp.int32, (GROUP, n_cols), 1)
        allowed = jnp.logical_or(bias[1, pl.ds(base, GROUP)] > 0.5, col // n_local == slots)
        pos_g = bias[0, pl.ds(base, GROUP)]
        parts = []
        for h in range(n_local):
            num = (jnp.full((GROUP, n_cols), 1 + h, jnp.int32) + head0).astype(F32)
            slope = jnp.exp2(-8.0 * num / n_heads)
            parts.append(jnp.where(jnp.logical_and(allowed, col % n_local == h), slope * pos_g, -jnp.inf))
        queries = jnp.concatenate([fresh[:, 3 * h * head_dim:(3 * h + 1) * head_dim] for h in range(n_local)], axis=0)
        odd = lax.broadcasted_iota(jnp.int32, (rows, head_dim), 0) % 2 == 1
        q_pair = jnp.concatenate([jnp.where(odd, 0.0, queries), jnp.where(odd, queries, 0.0)], axis=1).astype(BF16)
        row_s = lax.broadcasted_iota(jnp.int32, (rows, n_cols), 0) % GROUP // 2
        s = None
        for b in range(0, GROUP, 2):
            keys = jnp.concatenate([kbuf[base + b], kbuf[base + b + 1]], axis=1)
            sb = lax.dot_general(q_pair, keys, (((1,), (1,)), ((), ())), preferred_element_type=F32)
            s = sb if s is None else jnp.where(row_s == b // 2, sb, s)
        s = s * scale + jnp.concatenate(parts, axis=0)
        top = jnp.max(s, axis=-1, keepdims=True)
        e = jnp.exp(s - top)
        p = (e * (1.0 / jnp.sum(e, axis=-1, keepdims=True))).astype(BF16)
        row_o = lax.broadcasted_iota(jnp.int32, (rows, head_dim), 0) % GROUP
        o = None
        for b in range(0, GROUP, 2):
            values = jnp.concatenate([vbuf[base + b], vbuf[base + b + 1]], axis=1)
            ob = jnp.dot(p, values, preferred_element_type=F32)
            for i in range(2):
                oi = ob[:, i * head_dim:(i + 1) * head_dim]
                o = oi if o is None else jnp.where(row_o == b + i, oi, o)
        for h in range(n_local):
            attn[pl.ds(base, GROUP), h * head_dim:(h + 1) * head_dim] = o[h * GROUP:(h + 1) * GROUP]
        if not first:
            out_copy(0, g).start()
            out_copy(1, g).start()
        return carry

    lax.fori_loop(0, n_groups, group, 0)
    attn_ref[...] = attn[...].astype(BF16)
    if not first:
        for c in old:
            c.wait()
        for g in range(n_groups):
            out_copy(0, g).wait()
            out_copy(1, g).wait()


def reduce_kernel(layer, n_tp, last, *refs):
    (attn_ref, wo_hbm, res_ref, gain_ref, shift_ref, bo_ref, wu_hbm, bu_ref, wd_hbm, bd_ref) = refs[:10]
    if last:
        out_ref, rest = refs[10], refs[11:]
    else:
        (k_hbm, v_hbm, k_raw, v_raw, out_ref, own_ref, kall, vall) = refs[10:18]
        rest = refs[18:]
    (wo, wu, wd, part_ref, part2, d2d, mid, got, gath, gath2, sem_w,
     pair_s, pair_r, chip_s, chip_r, ag_s, ag_r, agp_s, agp_r) = rest
    n_batch, width = part_ref.shape
    n_chip = n_tp // 2
    blk = n_batch // n_tp
    me = lax.axis_index('tp')
    x = me // 2
    c = me % 2
    partner = x * 2 + (1 - c)

    def chip(d):
        return lax.rem(x + d, n_chip)

    wo_copy = pltpu.make_async_copy(wo_hbm.at[layer], wo, sem_w.at[4])
    wo_copy.start()
    w_copies = [pltpu.make_async_copy(wu_hbm.at[layer], wu, sem_w.at[0]), pltpu.make_async_copy(wd_hbm.at[layer], wd, sem_w.at[1])]
    if not last:
        w_copies.append(pltpu.make_async_copy(k_hbm.at[layer + 1], kall.at[layer + 1], sem_w.at[2]))
        w_copies.append(pltpu.make_async_copy(v_hbm.at[layer + 1], vall.at[layer + 1], sem_w.at[3]))
    for w in w_copies:
        w.start()
    barrier = pltpu.get_barrier_semaphore()
    peers = [partner] + [chip(d) * 2 + 1 - c for d in range(1, n_chip)]
    for peer in peers:
        pl.semaphore_signal(barrier, inc=1, device_id={'tp': peer}, device_id_type=MESH)
    wo_copy.wait()
    part_ref[...] = jnp.dot(attn_ref[...], wo[...], preferred_element_type=F32)
    pl.semaphore_wait(barrier, len(peers))

    order = [2, 1, 3, 0] if n_chip == 4 else list(range(1, n_chip)) + [0]

    def rows_of(core, d):
        return pl.ds(pl.multiple_of((core * n_chip + chip(d)) * blk, blk), blk)

    def reduce_scatter(phase, src):
        pair = {
            d: pltpu.make_async_remote_copy(
                src_ref=src.at[rows_of(1 - c, d)], dst_ref=d2d.at[phase, d], send_sem=pair_s.at[phase, d],
                recv_sem=pair_r.at[phase, d], device_id={'tp': partner}, device_id_type=MESH)
            for d in order
        }
        for d in order:
            pair[d].start()
        hops = {}
        for d in order:
            pair[d].wait_recv()
            mid[phase, d] = src[rows_of(c, d), :] + d2d[phase, d]
            hops[d] = pltpu.make_async_remote_copy(
                src_ref=mid.at[phase, d], dst_ref=got.at[phase, d], send_sem=chip_s.at[phase, d],
                recv_sem=chip_r.at[phase, d], device_id={'tp': chip(d) * 2 + 1 - c}, device_id_type=MESH)
            hops[d].start()
        acc = None
        for d in sorted(hops, key=lambda d: min(d, n_chip - d)):
            hops[d].wait_recv()
            acc = got[phase, d] if acc is None else acc + got[phase, d]
        for d in order:
            pair[d].wait_send()
            hops[d].wait_send()
        return acc

    def all_gather(phase, buf, value):
        buf[1 - c, x] = value
        hops = {}
        for d in order[:-1]:
            hops[d] = pltpu.make_async_remote_copy(
                src_ref=buf.at[1 - c, x], dst_ref=buf.at[1 - c, x], send_sem=ag_s.at[phase, d], recv_sem=ag_r.at[phase, d],
                device_id={'tp': chip(d) * 2 + 1 - c}, device_id_type=MESH)
            hops[d].start()

        def pass_on(d):
            slot = lax.rem(x + n_chip - d, n_chip)
            half = 1 - c if d == 0 else c
            cp = pltpu.make_async_remote_copy(
                src_ref=buf.at[half, slot], dst_ref=buf.at[half, slot], send_sem=agp_s.at[phase, d], recv_sem=agp_r.at[phase, d],
                device_id={'tp': partner}, device_id_type=MESH)
            cp.start()
            return cp

        passed = [pass_on(0)]
        for d in sorted(hops, key=lambda d: min(d, n_chip - d)):
            hops[d].wait_recv()
            passed.append(pass_on(d))
        for cp in passed:
            cp.wait()
        for d in hops:
            hops[d].wait_send()
        return buf[...].astype(F32).reshape(n_batch, width)

    if last:
        res = res_ref[...].astype(F32)
    else:
        res = res_ref[rows_of(1 - c, 0), :].astype(F32)
    total = reduce_scatter(0, part_ref)
    x_mid = (res + total + bo_ref[layer:layer + 1].astype(F32)).astype(BF16).astype(F32)
    normed = all_gather(0, gath, layer_norm_f32(x_mid, gain_ref[layer, 1:2], shift_ref[layer, 1:2])).astype(BF16)
    w_copies[0].wait()
    up = jnp.dot(normed, wu[...], preferred_element_type=F32) + bu_ref[layer:layer + 1].astype(F32)
    act = jax.nn.gelu(up, approximate=True).astype(BF16)
    w_copies[1].wait()
    part2[...] = jnp.dot(act, wd[...], preferred_element_type=F32)
    total = reduce_scatter(1, part2)
    x_next = (x_mid + total + bd_ref[layer:layer + 1].astype(F32)).astype(BF16)
    if last:
        out_ref[...] = all_gather(1, gath2, x_next).astype(BF16)
    else:
        own_ref[...] = x_next
        nxt = layer_norm_f32(x_next.astype(F32), gain_ref[layer + 1, 0:1], shift_ref[layer + 1, 0:1])
        out_ref[...] = all_gather(1, gath2, nxt).astype(BF16)
        for w in w_copies[2:]:
            w.wait()


def solution(mesh):
    tp_size = mesh.shape['tp']
    vm = pl.BlockSpec(memory_space=pltpu.VMEM)
    sm = pl.BlockSpec(memory_space=pltpu.SMEM)
    hbm = pl.BlockSpec(memory_space=pltpu.HBM)

    def device_step(hidden, ln_gain, ln_shift, w_qkv, b_qkv, w_out, b_out, w_up, b_up, w_down, b_down, k_cache, v_cache, write_slot, key_pos, key_valid):
        n_layers, n_batch, cache_len, n_local, head_dim = k_cache.shape
        width = hidden.shape[-1]
        n_cols = cache_len * n_local
        flat = (n_layers, n_batch, n_cols, head_dim)
        in_hbm = functools.partial(pltpu.with_memory_space_constraint, memory_space=pltpu.HBM)
        k_in, v_in = in_hbm(k_cache.reshape(flat)), in_hbm(v_cache.reshape(flat))
        w_qkv, w_out, w_up, w_down = map(in_hbm, (w_qkv, w_out, w_up, w_down))
        x0 = hidden.reshape(n_batch, width)
        n_groups = n_batch // GROUP
        blk = n_batch // tp_size
        n_chip = tp_size // 2
        shape = jax.ShapeDtypeStruct(flat, BF16)
        held = pltpu.VMEM(flat, BF16)
        shared = [in_hbm(a) for a in (write_slot, key_pos, key_valid)]

        def attn(layer, x_in, caches):
            first = layer == 0
            small = [pltpu.VMEM(b_qkv.shape, BF16), pltpu.VMEM(key_pos.shape, jnp.int32), pltpu.VMEM(key_valid.shape, jnp.int32), pltpu.SMEM(write_slot.shape, jnp.int32)]
            work = [
                pltpu.VMEM(w_qkv.shape[1:], BF16),
                pltpu.VMEM((n_batch, b_qkv.shape[1]), F32),
                pltpu.VMEM((2, n_batch, n_cols), F32),
                pltpu.VMEM((n_batch, n_local * head_dim), F32),
            ]
            alias = {}
            mixed = jax.ShapeDtypeStruct((n_batch, n_local * head_dim), BF16)
            if first:
                ins = [in_hbm(x_in), in_hbm(ln_gain), in_hbm(ln_shift), in_hbm(b_qkv), w_qkv] + shared + [k_in, v_in]
                specs = [hbm] * len(ins)
                small = [pltpu.VMEM(x_in.shape, BF16), pltpu.VMEM(ln_gain.shape, BF16), pltpu.VMEM(ln_shift.shape, BF16)] + small
                outs, out_specs = (mixed, held, held), (vm, vm, vm)
                scratch = small + work + [pltpu.SemaphoreType.DMA((5,)), pltpu.SemaphoreType.DMA((7,)), pltpu.SemaphoreType.DMA((2, n_groups))]
            else:
                ins = [x_in, in_hbm(b_qkv), w_qkv] + shared + list(caches)
                specs = [vm, hbm, hbm] + [hbm] * len(shared) + [vm] * 2
                outs, out_specs = (mixed, shape, shape, held, held), (vm, hbm, hbm, vm, vm)
                alias = {len(ins) - 2: 3, len(ins) - 1: 4}
                scratch = small + work + [pltpu.SemaphoreType.DMA((5,)), pltpu.SemaphoreType.DMA((7,)), pltpu.SemaphoreType.DMA((4,))]
            return pl.pallas_call(
                functools.partial(attn_kernel, layer, n_local * tp_size, first),
                out_shape=outs,
                in_specs=specs,
                out_specs=out_specs,
                scratch_shapes=scratch,
                input_output_aliases=alias,
                compiler_params=pltpu.CompilerParams(vmem_limit_bytes=14 * MIB),
                name=f'attn_{layer}',
            )(*ins)

        def reduce(layer, mixed, res, caches=()):
            last = layer == n_layers - 1
            ins = [mixed, w_out, res, ln_gain, ln_shift, b_out, w_up, b_up, w_down, b_down]
            specs = [vm, hbm, vm, vm, vm, vm, hbm, vm, hbm, vm]
            outs = [jax.ShapeDtypeStruct((n_batch, width), BF16)]
            if not last:
                ins += [k_in, v_in, *caches]
                specs += [hbm, hbm, vm, vm]
                outs += [jax.ShapeDtypeStruct((blk, width), BF16), held, held]
            dma = pltpu.SemaphoreType.DMA((2, n_chip))
            return pl.pallas_call(
                functools.partial(reduce_kernel, layer, tp_size, last),
                out_shape=tuple(outs),
                in_specs=specs,
                out_specs=tuple([vm] * len(outs)),
                scratch_shapes=[
                    pltpu.VMEM(w_out.shape[1:], BF16),
                    pltpu.VMEM(w_up.shape[1:], BF16),
                    pltpu.VMEM(w_down.shape[1:], BF16),
                    pltpu.VMEM((n_batch, width), F32),
                    pltpu.VMEM((n_batch, width), F32),
                    pltpu.VMEM((2, n_chip, blk, width), F32),
                    pltpu.VMEM((2, n_chip, blk, width), F32),
                    pltpu.VMEM((2, n_chip, blk, width), F32),
                    pltpu.VMEM((2, n_chip, blk, width), BF16),
                    pltpu.VMEM((2, n_chip, blk, width), BF16),
                    pltpu.SemaphoreType.DMA((6,)),
                ] + [dma] * 8,
                input_output_aliases={} if last else {len(ins) - 2: 2, len(ins) - 1: 3},
                compiler_params=pltpu.CompilerParams(vmem_limit_bytes=14 * MIB, collective_id=layer, has_side_effects=True),
                name=f'reduce_{layer}',
            )(*ins)

        mixed, k_held, v_held = attn(0, x0, None)
        h1, x1, k_held, v_held = reduce(0, mixed, x0, (k_held, v_held))
        mixed, k_new, v_new = attn(1, h1, (k_held, v_held))[:3]
        (x_last,) = reduce(1, mixed, x1)
        return x_last[:, None, :], k_new.reshape(k_cache.shape), v_new.reshape(v_cache.shape)

    cache_spec = P(None, 'dp', None, 'tp', None)
    in_specs = (P('dp', None, None), P(), P(), P(None, None, 'tp'), P(None, 'tp'), P(None, 'tp', None), P(), P(None, None, 'tp'), P(None, 'tp'), P(None, 'tp', None), P(), cache_spec, cache_spec, P('dp'), P('dp', None), P('dp', None))
    out_specs = (P('dp', None, None), cache_spec, cache_spec)
    return jax.shard_map(device_step, mesh=mesh, in_specs=in_specs, out_specs=out_specs, check_vma=False)
```

```python
import functools
import math

import jax
import jax.numpy as jnp
from jax import lax
from jax.experimental import pallas as pl
from jax.experimental.pallas import tpu as pltpu
from jax.sharding import PartitionSpec as P

LN_EPS = 1e-5
MESH = pl.DeviceIdType.MESH
F32 = jnp.float32
BF16 = jnp.bfloat16
GROUP = 8
AHEAD = 6
MIB = 2 ** 20


def layer_norm_f32(x_f32, gain, shift):
    mean_val = jnp.mean(x_f32, axis=-1, keepdims=True)
    centered = x_f32 - mean_val
    var_val = jnp.mean(centered * centered, axis=-1, keepdims=True)
    normed = centered * lax.rsqrt(var_val + LN_EPS)
    return (normed * gain.astype(F32) + shift.astype(F32)).astype(BF16)


def attn_kernel(layer, n_heads, first, *refs):
    if first:
        (x_in_ref, gain_in, shift_in, bq_in, wq_hbm, wo_hbm, slot_hbm, pos_in, valid_in, k_hbm, v_hbm,
         part_ref, kall, vall,
         pos_ref, valid_ref, slot_smem, wo, bias, attn, sem_w, sem_s,
         x_ref, gain_ref, shift_ref, bq_ref, wq, qkv, sem_in) = refs
    else:
        (qkv, wo_hbm, slot_hbm, pos_in, valid_in, k_raw, v_raw,
         part_ref, k_out, v_out, kall, vall,
         pos_ref, valid_ref, slot_smem, wo, bias, attn, sem_w, sem_s, sem_out) = refs
    kbuf, vbuf = kall.at[layer], vall.at[layer]
    n_batch, n_cols, head_dim = kbuf.shape
    n_groups = n_batch // GROUP
    n_local = attn.shape[1] // head_dim
    cache_len = n_cols // n_local
    n_chunk = 4
    pairs = [(slot_hbm, slot_smem), (pos_in, pos_ref), (valid_in, valid_ref)]
    if first:
        pairs = [(x_in_ref, x_ref), (gain_in, gain_ref), (shift_in, shift_ref), (bq_in, bq_ref)] + pairs
    small = [pltpu.make_async_copy(src, dst, sem_s.at[i]) for i, (src, dst) in enumerate(pairs)]
    for c in small:
        c.start()
    wo_copy = pltpu.make_async_copy(wo_hbm.at[layer], wo, sem_w.at[n_chunk])
    if first:
        step = x_ref.shape[1] // n_chunk
        w_copies = [
            pltpu.make_async_copy(wq_hbm.at[layer, pl.ds(i * step, step)], wq.at[pl.ds(i * step, step)], sem_w.at[i])
            for i in range(n_chunk)
        ]
        for c in w_copies:
            c.start()

    def in_copy(which, g):
        src, dst = ((k_hbm, kbuf), (v_hbm, vbuf))[which]
        return pltpu.make_async_copy(src.at[layer, pl.ds(g * GROUP, GROUP)], dst.at[pl.ds(g * GROUP, GROUP)], sem_in.at[which, g])

    def out_copy(which, g):
        src, dst = ((kbuf, k_out), (vbuf, v_out))[which]
        return pltpu.make_async_copy(src.at[pl.ds(g * GROUP, GROUP)], dst.at[layer, pl.ds(g * GROUP, GROUP)], sem_out.at[which])

    if first:
        for g in range(AHEAD - n_chunk):
            in_copy(0, g).start()
            in_copy(1, g).start()
    else:
        wo_copy.start()
        old = [
            pltpu.make_async_copy(src.at[layer - 1, pl.ds(g * GROUP, GROUP)], dst.at[layer - 1, pl.ds(g * GROUP, GROUP)], sem_out.at[2 + i])
            for g in range(n_groups) for i, (src, dst) in enumerate(((kall, k_out), (vall, v_out)))
        ]
        for c in old:
            c.start()

    t_row = lax.broadcasted_iota(jnp.int32, (cache_len, n_cols), 0)
    t_col = lax.broadcasted_iota(jnp.int32, (cache_len, n_cols), 1) // n_local
    spread = (t_row == t_col).astype(BF16)
    for c in small:
        c.wait()
    pos = jnp.dot(pos_ref[...].astype(F32).astype(BF16), spread, preferred_element_type=F32)
    valid = jnp.dot(valid_ref[...].astype(F32).astype(BF16), spread, preferred_element_type=F32)
    bias[0] = pos
    bias[1] = valid

    if first:
        x_in = layer_norm_f32(x_ref[...].astype(F32), gain_ref[layer, 0:1], shift_ref[layer, 0:1])
        acc = None
        for i in range(n_chunk):
            w_copies[i].wait()
            in_copy(0, AHEAD - n_chunk + i).start()
            in_copy(1, AHEAD - n_chunk + i).start()
            d = jnp.dot(x_in[:, i * step:(i + 1) * step], wq[i * step:(i + 1) * step], preferred_element_type=F32)
            acc = d if acc is None else acc + d
        qkv[...] = (acc + bq_ref[layer:layer + 1].astype(F32)).astype(BF16).astype(F32)

    scale = 1.0 / math.sqrt(head_dim)
    rows = n_local * GROUP
    head0 = lax.axis_index('tp') * n_local

    def group(g, carry):
        if first:
            in_copy(0, g).wait()
            in_copy(1, g).wait()

            @pl.when(g + AHEAD < n_groups)
            def _():
                in_copy(0, g + AHEAD).start()
                in_copy(1, g + AHEAD).start()

            @pl.when(g + AHEAD == n_groups)
            def _():
                wo_copy.start()
        base = pl.multiple_of(g * GROUP, GROUP)
        row16 = lax.broadcasted_iota(jnp.int32, (16, head_dim), 0)
        fresh = qkv[pl.ds(base, GROUP), :]
        row8 = lax.broadcasted_iota(jnp.int32, (GROUP, n_cols), 0)
        slots = jnp.zeros((GROUP, n_cols), jnp.int32)
        for b in range(GROUP):
            slot = slot_smem[g * GROUP + b]
            slots = jnp.where(row8 == b, slot, slots)
            first_row = slot * n_local
            start = pl.multiple_of((first_row // 16) * 16, 16)
            off = first_row - start
            for which, buf in ((1, kbuf), (2, vbuf)):
                block = buf[base + b, pl.ds(start, 16), :].astype(F32)
                for h in range(n_local):
                    new = fresh[b:b + 1, (3 * h + which) * head_dim:(3 * h + which + 1) * head_dim]
                    block = jnp.where(row16 == off + h, new, block)
                buf[base + b, pl.ds(start, 16), :] = block.astype(BF16)
        col = lax.broadcasted_iota(jnp.int32, (GROUP, n_cols), 1)
        allowed = jnp.logical_or(bias[1, pl.ds(base, GROUP)] > 0.5, col // n_local == slots)
        pos_g = bias[0, pl.ds(base, GROUP)]
        parts = []
        for h in range(n_local):
            num = (jnp.full((GROUP, n_cols), 1 + h, jnp.int32) + head0).astype(F32)
            slope = jnp.exp2(-8.0 * num / n_heads)
            parts.append(jnp.where(jnp.logical_and(allowed, col % n_local == h), slope * pos_g, -jnp.inf))
        queries = jnp.concatenate([fresh[:, 3 * h * head_dim:(3 * h + 1) * head_dim] for h in range(n_local)], axis=0)
        odd = lax.broadcasted_iota(jnp.int32, (rows, head_dim), 0) % 2 == 1
        q_pair = jnp.concatenate([jnp.where(odd, 0.0, queries), jnp.where(odd, queries, 0.0)], axis=1).astype(BF16)
        row_s = lax.broadcasted_iota(jnp.int32, (rows, n_cols), 0) % GROUP // 2
        s = None
        for b in range(0, GROUP, 2):
            keys = jnp.concatenate([kbuf[base + b], kbuf[base + b + 1]], axis=1)
            sb = lax.dot_general(q_pair, keys, (((1,), (1,)), ((), ())), preferred_element_type=F32)
            s = sb if s is None else jnp.where(row_s == b // 2, sb, s)
        s = s * scale + jnp.concatenate(parts, axis=0)
        top = jnp.max(s, axis=-1, keepdims=True)
        e = jnp.exp(s - top)
        p = (e * (1.0 / jnp.sum(e, axis=-1, keepdims=True))).astype(BF16)
        row_o = lax.broadcasted_iota(jnp.int32, (rows, head_dim), 0) % GROUP
        o = None
        for b in range(0, GROUP, 2):
            values = jnp.concatenate([vbuf[base + b], vbuf[base + b + 1]], axis=1)
            ob = jnp.dot(p, values, preferred_element_type=F32)
            for i in range(2):
                oi = ob[:, i * head_dim:(i + 1) * head_dim]
                o = oi if o is None else jnp.where(row_o == b + i, oi, o)
        for h in range(n_local):
            attn[pl.ds(base, GROUP), h * head_dim:(h + 1) * head_dim] = o[h * GROUP:(h + 1) * GROUP]
        if not first:
            out_copy(0, g).start()
            out_copy(1, g).start()
        return carry

    lax.fori_loop(0, n_groups, group, 0)
    wo_copy.wait()
    part_ref[...] = jnp.dot(attn[...].astype(BF16), wo[...], preferred_element_type=F32)
    if not first:
        for c in old:
            c.wait()
        for g in range(n_groups):
            out_copy(0, g).wait()
            out_copy(1, g).wait()


def reduce_kernel(layer, n_tp, last, *refs):
    (part_ref, res_ref, gain_ref, shift_ref, bo_ref, wu_hbm, bu_ref, wd_hbm, bd_ref) = refs[:9]
    if last:
        out_ref, rest = refs[9], refs[10:]
    else:
        (k_hbm, v_hbm, wq_hbm, bq_ref, k_raw, v_raw, out_ref, own_ref, kall, vall) = refs[9:19]
        rest = refs[19:]
    (wu, wd, part2, d2d, mid, got, gath, gath2, sem_w,
     pair_s, pair_r, chip_s, chip_r, ag_s, ag_r, agp_s, agp_r) = rest
    n_batch, width = part_ref.shape
    n_chip = n_tp // 2
    blk = n_batch // n_tp
    me = lax.axis_index('tp')
    x = me // 2
    c = me % 2
    partner = x * 2 + (1 - c)

    def chip(d):
        return lax.rem(x + d, n_chip)

    w_copies = [pltpu.make_async_copy(wu_hbm.at[layer], wu, sem_w.at[0]), pltpu.make_async_copy(wd_hbm.at[layer], wd, sem_w.at[1])]
    if not last:
        w_copies.append(pltpu.make_async_copy(k_hbm.at[layer + 1], kall.at[layer + 1], sem_w.at[2]))
        w_copies.append(pltpu.make_async_copy(v_hbm.at[layer + 1], vall.at[layer + 1], sem_w.at[3]))
        n_qkv = bq_ref.shape[1]
        wq = wu.at[:, pl.ds(0, n_qkv)]
        wq_copy = pltpu.make_async_copy(wq_hbm.at[layer + 1], wq, sem_w.at[4])
    barrier = pltpu.get_barrier_semaphore()
    peers = [partner] + [chip(d) * 2 + 1 - c for d in range(1, n_chip)]
    for peer in peers:
        pl.semaphore_signal(barrier, inc=1, device_id={'tp': peer}, device_id_type=MESH)
    for w in w_copies:
        w.start()
    pl.semaphore_wait(barrier, len(peers))

    order = [2, 1, 3, 0] if n_chip == 4 else list(range(1, n_chip)) + [0]

    def rows_of(core, d):
        return pl.ds(pl.multiple_of((core * n_chip + chip(d)) * blk, blk), blk)

    def reduce_scatter(phase, src):
        pair = {
            d: pltpu.make_async_remote_copy(
                src_ref=src.at[rows_of(1 - c, d)], dst_ref=d2d.at[phase, d], send_sem=pair_s.at[phase, d],
                recv_sem=pair_r.at[phase, d], device_id={'tp': partner}, device_id_type=MESH)
            for d in order
        }
        for d in order:
            pair[d].start()
        hops = {}
        for d in order:
            pair[d].wait_recv()
            mid[phase, d] = src[rows_of(c, d), :] + d2d[phase, d]
            hops[d] = pltpu.make_async_remote_copy(
                src_ref=mid.at[phase, d], dst_ref=got.at[phase, d], send_sem=chip_s.at[phase, d],
                recv_sem=chip_r.at[phase, d], device_id={'tp': chip(d) * 2 + 1 - c}, device_id_type=MESH)
            hops[d].start()
        acc = None
        for d in sorted(hops, key=lambda d: min(d, n_chip - d)):
            hops[d].wait_recv()
            acc = got[phase, d] if acc is None else acc + got[phase, d]
        for d in order:
            pair[d].wait_send()
            hops[d].wait_send()
        return acc

    def all_gather(phase, buf, value):
        buf[1 - c, x] = value
        hops = {}
        for d in order[:-1]:
            hops[d] = pltpu.make_async_remote_copy(
                src_ref=buf.at[1 - c, x], dst_ref=buf.at[1 - c, x], send_sem=ag_s.at[phase, d], recv_sem=ag_r.at[phase, d],
                device_id={'tp': chip(d) * 2 + 1 - c}, device_id_type=MESH)
            hops[d].start()

        def pass_on(d):
            slot = lax.rem(x + n_chip - d, n_chip)
            half = 1 - c if d == 0 else c
            cp = pltpu.make_async_remote_copy(
                src_ref=buf.at[half, slot], dst_ref=buf.at[half, slot], send_sem=agp_s.at[phase, d], recv_sem=agp_r.at[phase, d],
                device_id={'tp': partner}, device_id_type=MESH)
            cp.start()
            return cp

        passed = [pass_on(0)]
        for d in sorted(hops, key=lambda d: min(d, n_chip - d)):
            hops[d].wait_recv()
            passed.append(pass_on(d))
        for cp in passed:
            cp.wait()
        for d in hops:
            hops[d].wait_send()
        return buf[...].astype(F32).reshape(n_batch, width)

    if last:
        res = res_ref[...].astype(F32)
    else:
        res = res_ref[rows_of(1 - c, 0), :].astype(F32)
    total = reduce_scatter(0, part_ref)
    x_mid = (res + total + bo_ref[layer:layer + 1].astype(F32)).astype(BF16).astype(F32)
    normed = all_gather(0, gath, layer_norm_f32(x_mid, gain_ref[layer, 1:2], shift_ref[layer, 1:2])).astype(BF16)
    w_copies[0].wait()
    up = jnp.dot(normed, wu[...], preferred_element_type=F32) + bu_ref[layer:layer + 1].astype(F32)
    act = jax.nn.gelu(up, approximate=True).astype(BF16)
    if not last:
        wq_copy.start()
    w_copies[1].wait()
    part2[...] = jnp.dot(act, wd[...], preferred_element_type=F32)
    total = reduce_scatter(1, part2)
    x_next = (x_mid + total + bd_ref[layer:layer + 1].astype(F32)).astype(BF16)
    if last:
        out_ref[...] = all_gather(1, gath2, x_next).astype(BF16)
    else:
        own_ref[...] = x_next
        nxt = layer_norm_f32(x_next.astype(F32), gain_ref[layer + 1, 0:1], shift_ref[layer + 1, 0:1])
        normed = all_gather(1, gath2, nxt).astype(BF16)
        wq_copy.wait()
        qkv = jnp.dot(normed, wu[:, :n_qkv], preferred_element_type=F32) + bq_ref[layer + 1:layer + 2].astype(F32)
        out_ref[...] = qkv.astype(BF16).astype(F32)
        for w in w_copies[2:]:
            w.wait()


def solution(mesh):
    tp_size = mesh.shape['tp']
    vm = pl.BlockSpec(memory_space=pltpu.VMEM)
    sm = pl.BlockSpec(memory_space=pltpu.SMEM)
    hbm = pl.BlockSpec(memory_space=pltpu.HBM)

    def device_step(hidden, ln_gain, ln_shift, w_qkv, b_qkv, w_out, b_out, w_up, b_up, w_down, b_down, k_cache, v_cache, write_slot, key_pos, key_valid):
        n_layers, n_batch, cache_len, n_local, head_dim = k_cache.shape
        width = hidden.shape[-1]
        n_cols = cache_len * n_local
        flat = (n_layers, n_batch, n_cols, head_dim)
        in_hbm = functools.partial(pltpu.with_memory_space_constraint, memory_space=pltpu.HBM)
        k_in, v_in = in_hbm(k_cache.reshape(flat)), in_hbm(v_cache.reshape(flat))
        w_qkv, w_out, w_up, w_down = map(in_hbm, (w_qkv, w_out, w_up, w_down))
        x0 = hidden.reshape(n_batch, width)
        n_groups = n_batch // GROUP
        blk = n_batch // tp_size
        n_chip = tp_size // 2
        shape = jax.ShapeDtypeStruct(flat, BF16)
        held = pltpu.VMEM(flat, BF16)
        shared = [in_hbm(a) for a in (write_slot, key_pos, key_valid)]

        def attn(layer, x_in, caches):
            first = layer == 0
            n_qkv = b_qkv.shape[1]
            scratch = [
                pltpu.VMEM(key_pos.shape, jnp.int32),
                pltpu.VMEM(key_valid.shape, jnp.int32),
                pltpu.SMEM(write_slot.shape, jnp.int32),
                pltpu.VMEM(w_out.shape[1:], BF16),
                pltpu.VMEM((2, n_batch, n_cols), F32),
                pltpu.VMEM((n_batch, n_local * head_dim), F32),
                pltpu.SemaphoreType.DMA((5,)),
                pltpu.SemaphoreType.DMA((7,)),
            ]
            alias = {}
            part = jax.ShapeDtypeStruct((n_batch, width), F32)
            if first:
                ins = [in_hbm(a) for a in (x_in, ln_gain, ln_shift, b_qkv)] + [w_qkv, w_out] + shared + [k_in, v_in]
                specs = [hbm] * len(ins)
                outs, out_specs = (part, held, held), (vm, vm, vm)
                scratch += [
                    pltpu.VMEM(x_in.shape, BF16),
                    pltpu.VMEM(ln_gain.shape, BF16),
                    pltpu.VMEM(ln_shift.shape, BF16),
                    pltpu.VMEM(b_qkv.shape, BF16),
                    pltpu.VMEM(w_qkv.shape[1:], BF16),
                    pltpu.VMEM((n_batch, n_qkv), F32),
                    pltpu.SemaphoreType.DMA((2, n_groups)),
                ]
            else:
                ins = [x_in, w_out] + shared + list(caches)
                specs = [vm, hbm] + [hbm] * len(shared) + [vm] * 2
                outs, out_specs = (part, shape, shape, held, held), (vm, hbm, hbm, vm, vm)
                alias = {len(ins) - 2: 3, len(ins) - 1: 4}
                scratch += [pltpu.SemaphoreType.DMA((4,))]
            return pl.pallas_call(
                functools.partial(attn_kernel, layer, n_local * tp_size, first),
                out_shape=outs,
                in_specs=specs,
                out_specs=out_specs,
                scratch_shapes=scratch,
                input_output_aliases=alias,
                compiler_params=pltpu.CompilerParams(vmem_limit_bytes=13 * MIB),
                name=f'attn_{layer}',
            )(*ins)

        def reduce(layer, part, res, caches=()):
            last = layer == n_layers - 1
            ins = [part, res, ln_gain, ln_shift, b_out, w_up, b_up, w_down, b_down]
            specs = [vm, vm, vm, vm, vm, hbm, vm, hbm, vm]
            outs = [jax.ShapeDtypeStruct((n_batch, width), BF16)]
            if not last:
                ins += [k_in, v_in, w_qkv, b_qkv, *caches]
                specs += [hbm, hbm, hbm, vm, vm, vm]
                outs = [jax.ShapeDtypeStruct((n_batch, b_qkv.shape[1]), F32)]
                outs += [jax.ShapeDtypeStruct((blk, width), BF16), held, held]
            dma = pltpu.SemaphoreType.DMA((2, n_chip))
            return pl.pallas_call(
                functools.partial(reduce_kernel, layer, tp_size, last),
                out_shape=tuple(outs),
                in_specs=specs,
                out_specs=tuple([vm] * len(outs)),
                scratch_shapes=[
                    pltpu.VMEM(w_up.shape[1:], BF16),
                    pltpu.VMEM(w_down.shape[1:], BF16),
                    pltpu.VMEM((n_batch, width), F32),
                    pltpu.VMEM((2, n_chip, blk, width), F32),
                    pltpu.VMEM((2, n_chip, blk, width), F32),
                    pltpu.VMEM((2, n_chip, blk, width), F32),
                    pltpu.VMEM((2, n_chip, blk, width), BF16),
                    pltpu.VMEM((2, n_chip, blk, width), BF16),
                    pltpu.SemaphoreType.DMA((6,)),
                ] + [dma] * 8,
                input_output_aliases={} if last else {len(ins) - 2: 2, len(ins) - 1: 3},
                compiler_params=pltpu.CompilerParams(vmem_limit_bytes=13 * MIB, collective_id=layer, has_side_effects=True),
                name=f'reduce_{layer}',
            )(*ins)

        part, k_held, v_held = attn(0, x0, None)
        qkv, x1, k_held, v_held = reduce(0, part, x0, (k_held, v_held))
        part, k_new, v_new = attn(1, qkv, (k_held, v_held))[:3]
        (x_last,) = reduce(1, part, x1)
        return x_last[:, None, :], k_new.reshape(k_cache.shape), v_new.reshape(v_cache.shape)

    cache_spec = P(None, 'dp', None, 'tp', None)
    in_specs = (P('dp', None, None), P(), P(), P(None, None, 'tp'), P(None, 'tp'), P(None, 'tp', None), P(), P(None, None, 'tp'), P(None, 'tp'), P(None, 'tp', None), P(), cache_spec, cache_spec, P('dp'), P('dp', None), P('dp', None))
    out_specs = (P('dp', None, None), cache_spec, cache_spec)
    return jax.shard_map(device_step, mesh=mesh, in_specs=in_specs, out_specs=out_specs, check_vma=False)
```

```python
import functools
import math

import jax
import jax.numpy as jnp
from jax import lax
from jax.experimental import pallas as pl
from jax.experimental.pallas import tpu as pltpu
from jax.sharding import PartitionSpec as P

LN_EPS = 1e-5
MESH = pl.DeviceIdType.MESH
F32 = jnp.float32
BF16 = jnp.bfloat16
GROUP = 8
AHEAD = 6
SUB = 2
EARLY = 2
MIB = 2 ** 20


def layer_norm_f32(x_f32, gain, shift):
    mean_val = jnp.mean(x_f32, axis=-1, keepdims=True)
    centered = x_f32 - mean_val
    var_val = jnp.mean(centered * centered, axis=-1, keepdims=True)
    normed = centered * lax.rsqrt(var_val + LN_EPS)
    return (normed * gain.astype(F32) + shift.astype(F32)).astype(BF16)


def attn_kernel(layer, n_heads, first, *refs):
    if first:
        (x_in_ref, gain_in, shift_in, bq_in, wq_hbm, wo_hbm, slot_hbm, pos_in, valid_in, k_hbm, v_hbm,
         part_ref, k_out, v_out, kall, vall,
         pos_ref, valid_ref, slot_smem, wo, bias, attn, sem_w, sem_s, sem_out,
         x_ref, gain_ref, shift_ref, bq_ref, wq, qkv, sem_in) = refs
        old = []
    else:
        (qkv, wo_hbm, slot_hbm, pos_in, valid_in, k_part, v_part, k_raw, v_raw,
         part_ref, k_out, v_out, kall, vall,
         pos_ref, valid_ref, slot_smem, wo, bias, attn, sem_w, sem_s, sem_out) = refs
    kbuf, vbuf = kall.at[layer], vall.at[layer]
    n_batch, n_cols, head_dim = kbuf.shape
    n_groups = n_batch // GROUP
    n_local = attn.shape[1] // head_dim
    cache_len = n_cols // n_local
    n_chunk = 4
    pairs = [(slot_hbm, slot_smem), (pos_in, pos_ref), (valid_in, valid_ref)]
    if first:
        pairs = [(x_in_ref, x_ref), (gain_in, gain_ref), (shift_in, shift_ref), (bq_in, bq_ref)] + pairs
    small = [pltpu.make_async_copy(src, dst, sem_s.at[i]) for i, (src, dst) in enumerate(pairs)]
    for c in small:
        c.start()
    wo_copy = pltpu.make_async_copy(wo_hbm.at[layer], wo, sem_w.at[n_chunk])
    if first:
        step = x_ref.shape[1] // n_chunk
        w_copies = [
            pltpu.make_async_copy(wq_hbm.at[layer, pl.ds(i * step, step)], wq.at[pl.ds(i * step, step)], sem_w.at[i])
            for i in range(n_chunk)
        ]
        for c in w_copies:
            c.start()

    def in_copy(which, g):
        src, dst = ((k_hbm, kbuf), (v_hbm, vbuf))[which]
        return pltpu.make_async_copy(src.at[layer, pl.ds(g * GROUP, GROUP)], dst.at[pl.ds(g * GROUP, GROUP)], sem_in.at[which, g])

    def out_copy(which, g):
        src, dst = ((kbuf, k_out), (vbuf, v_out))[which]
        return pltpu.make_async_copy(src.at[pl.ds(g * GROUP, GROUP)], dst.at[layer, pl.ds(g * GROUP, GROUP)], sem_out.at[which])

    if first:
        for g in range(AHEAD - n_chunk):
            in_copy(0, g).start()
            in_copy(1, g).start()
    else:
        wo_copy.start()
        old = [
            pltpu.make_async_copy(src.at[layer - 1, pl.ds(g * GROUP, GROUP)], dst.at[layer - 1, pl.ds(g * GROUP, GROUP)], sem_out.at[2 + i])
            for g in range(EARLY, n_groups) for i, (src, dst) in enumerate(((kall, k_out), (vall, v_out)))
        ]
        for c in old:
            c.start()

    t_row = lax.broadcasted_iota(jnp.int32, (cache_len, n_cols), 0)
    t_col = lax.broadcasted_iota(jnp.int32, (cache_len, n_cols), 1) // n_local
    spread = (t_row == t_col).astype(BF16)
    for c in small:
        c.wait()
    pos = jnp.dot(pos_ref[...].astype(F32).astype(BF16), spread, preferred_element_type=F32)
    valid = jnp.dot(valid_ref[...].astype(F32).astype(BF16), spread, preferred_element_type=F32)
    bias[0] = pos
    bias[1] = valid

    if first:
        x_in = layer_norm_f32(x_ref[...].astype(F32), gain_ref[layer, 0:1], shift_ref[layer, 0:1])
        acc = None
        for i in range(n_chunk):
            w_copies[i].wait()
            in_copy(0, AHEAD - n_chunk + i).start()
            in_copy(1, AHEAD - n_chunk + i).start()
            d = jnp.dot(x_in[:, i * step:(i + 1) * step], wq[i * step:(i + 1) * step], preferred_element_type=F32)
            acc = d if acc is None else acc + d
        qkv[...] = (acc + bq_ref[layer:layer + 1].astype(F32)).astype(BF16).astype(F32)

    scale = 1.0 / math.sqrt(head_dim)
    rows = n_local * GROUP
    head0 = lax.axis_index('tp') * n_local

    def update(g):
        base = pl.multiple_of(g * GROUP, GROUP)
        row16 = lax.broadcasted_iota(jnp.int32, (16, head_dim), 0)
        fresh = qkv[pl.ds(base, GROUP), :]
        row8 = lax.broadcasted_iota(jnp.int32, (GROUP, n_cols), 0)
        slots = jnp.zeros((GROUP, n_cols), jnp.int32)
        for b in range(GROUP):
            slot = slot_smem[g * GROUP + b]
            slots = jnp.where(row8 == b, slot, slots)
            first_row = slot * n_local
            start = pl.multiple_of((first_row // 16) * 16, 16)
            off = first_row - start
            for which, buf in ((1, kbuf), (2, vbuf)):
                block = buf[base + b, pl.ds(start, 16), :].astype(F32)
                for h in range(n_local):
                    new = fresh[b:b + 1, (3 * h + which) * head_dim:(3 * h + which + 1) * head_dim]
                    block = jnp.where(row16 == off + h, new, block)
                buf[base + b, pl.ds(start, 16), :] = block.astype(BF16)
        col = lax.broadcasted_iota(jnp.int32, (GROUP, n_cols), 1)
        allowed = jnp.logical_or(bias[1, pl.ds(base, GROUP)] > 0.5, col // n_local == slots)
        pos_g = bias[0, pl.ds(base, GROUP)]
        parts = []
        for h in range(n_local):
            num = (jnp.full((GROUP, n_cols), 1 + h, jnp.int32) + head0).astype(F32)
            slope = jnp.exp2(-8.0 * num / n_heads)
            parts.append(jnp.where(jnp.logical_and(allowed, col % n_local == h), slope * pos_g, -jnp.inf))
        queries = jnp.concatenate([fresh[:, 3 * h * head_dim:(3 * h + 1) * head_dim] for h in range(n_local)], axis=0)
        odd = lax.broadcasted_iota(jnp.int32, (rows, head_dim), 0) % 2 == 1
        q_pair = jnp.concatenate([jnp.where(odd, 0.0, queries), jnp.where(odd, queries, 0.0)], axis=1).astype(BF16)
        return base, q_pair, jnp.concatenate(parts, axis=0)

    def scores(base, q_pair, add):
        row_s = lax.broadcasted_iota(jnp.int32, (rows, n_cols), 0) % GROUP // 2
        s = None
        for b in range(0, GROUP, 2):
            keys = jnp.concatenate([kbuf[base + b], kbuf[base + b + 1]], axis=1)
            sb = lax.dot_general(q_pair, keys, (((1,), (1,)), ((), ())), preferred_element_type=F32)
            s = sb if s is None else jnp.where(row_s == b // 2, sb, s)
        return s * scale + add

    def softmax(s):
        top = jnp.max(s, axis=-1, keepdims=True)
        e = jnp.exp(s - top)
        return (e * (1.0 / jnp.sum(e, axis=-1, keepdims=True))).astype(BF16)

    def mix(base, p):
        row_o = lax.broadcasted_iota(jnp.int32, (rows, head_dim), 0) % GROUP
        o = None
        for b in range(0, GROUP, 2):
            values = jnp.concatenate([vbuf[base + b], vbuf[base + b + 1]], axis=1)
            ob = jnp.dot(p, values, preferred_element_type=F32)
            for i in range(2):
                oi = ob[:, i * head_dim:(i + 1) * head_dim]
                o = oi if o is None else jnp.where(row_o == b + i, oi, o)
        for h in range(n_local):
            attn[pl.ds(base, GROUP), h * head_dim:(h + 1) * head_dim] = o[h * GROUP:(h + 1) * GROUP]

    def groups(i, carry):
        todo = [i * SUB + j for j in range(SUB)]
        if first:
            for g in todo:
                in_copy(0, g).wait()
                in_copy(1, g).wait()

            @pl.when(todo[-1] + AHEAD < n_groups)
            def _():
                for g in todo:
                    in_copy(0, g + AHEAD).start()
                    in_copy(1, g + AHEAD).start()

            @pl.when(i == n_groups // SUB - 2)
            def _():
                wo_copy.start()

            @pl.when(i == n_groups // SUB - 1)
            def _():
                for g in range(EARLY):
                    out_copy(0, g).start()
                    out_copy(1, g).start()
        state = [update(g) for g in todo]
        probs = [scores(*st) for st in state]
        for (base, _, _), s in zip(state, probs):
            mix(base, softmax(s))
        if not first:
            for g in todo:
                out_copy(0, g).start()
                out_copy(1, g).start()
        return carry

    lax.fori_loop(0, n_groups // SUB, groups, 0)
    wo_copy.wait()
    part_ref[...] = jnp.dot(attn[...].astype(BF16), wo[...], preferred_element_type=F32)
    for c in old:
        c.wait()
    for g in range(EARLY if first else n_groups):
        out_copy(0, g).wait()
        out_copy(1, g).wait()


def reduce_kernel(layer, n_tp, last, *refs):
    (part_ref, res_ref, gain_ref, shift_ref, bo_ref, wu_hbm, bu_ref, wd_hbm, bd_ref) = refs[:9]
    if last:
        out_ref, rest = refs[9], refs[10:]
    else:
        (k_hbm, v_hbm, wq_hbm, bq_ref, k_raw, v_raw, out_ref, own_ref, kall, vall) = refs[9:19]
        rest = refs[19:]
    (wu, wd, part2, d2d, mid, got, gath, gath2, sem_w,
     pair_s, pair_r, chip_s, chip_r, ag_s, ag_r, agp_s, agp_r) = rest
    n_batch, width = part_ref.shape
    n_chip = n_tp // 2
    blk = n_batch // n_tp
    me = lax.axis_index('tp')
    x = me // 2
    c = me % 2
    partner = x * 2 + (1 - c)

    def chip(d):
        return lax.rem(x + d, n_chip)

    w_copies = [pltpu.make_async_copy(wu_hbm.at[layer], wu, sem_w.at[0]), pltpu.make_async_copy(wd_hbm.at[layer], wd, sem_w.at[1])]
    if not last:
        w_copies.append(pltpu.make_async_copy(k_hbm.at[layer + 1], kall.at[layer + 1], sem_w.at[2]))
        w_copies.append(pltpu.make_async_copy(v_hbm.at[layer + 1], vall.at[layer + 1], sem_w.at[3]))
        n_qkv = bq_ref.shape[1]
        wq = wu.at[:, pl.ds(0, n_qkv)]
        wq_copy = pltpu.make_async_copy(wq_hbm.at[layer + 1], wq, sem_w.at[4])
    barrier = pltpu.get_barrier_semaphore()
    peers = [partner] + [chip(d) * 2 + 1 - c for d in range(1, n_chip)]
    for peer in peers:
        pl.semaphore_signal(barrier, inc=1, device_id={'tp': peer}, device_id_type=MESH)
    for w in w_copies:
        w.start()
    pl.semaphore_wait(barrier, len(peers))

    order = [2, 1, 3, 0] if n_chip == 4 else list(range(1, n_chip)) + [0]

    def rows_of(core, d):
        return pl.ds(pl.multiple_of((core * n_chip + chip(d)) * blk, blk), blk)

    def reduce_scatter(phase, src):
        pair = {
            d: pltpu.make_async_remote_copy(
                src_ref=src.at[rows_of(1 - c, d)], dst_ref=d2d.at[phase, d], send_sem=pair_s.at[phase, d],
                recv_sem=pair_r.at[phase, d], device_id={'tp': partner}, device_id_type=MESH)
            for d in order
        }
        for d in order:
            pair[d].start()
        hops = {}
        for d in order:
            pair[d].wait_recv()
            mid[phase, d] = src[rows_of(c, d), :] + d2d[phase, d]
            hops[d] = pltpu.make_async_remote_copy(
                src_ref=mid.at[phase, d], dst_ref=got.at[phase, d], send_sem=chip_s.at[phase, d],
                recv_sem=chip_r.at[phase, d], device_id={'tp': chip(d) * 2 + 1 - c}, device_id_type=MESH)
            hops[d].start()
        acc = None
        for d in sorted(hops, key=lambda d: min(d, n_chip - d)):
            hops[d].wait_recv()
            acc = got[phase, d] if acc is None else acc + got[phase, d]
        for d in order:
            pair[d].wait_send()
            hops[d].wait_send()
        return acc

    def all_gather(phase, buf, value):
        buf[1 - c, x] = value
        hops = {}
        for d in order[:-1]:
            hops[d] = pltpu.make_async_remote_copy(
                src_ref=buf.at[1 - c, x], dst_ref=buf.at[1 - c, x], send_sem=ag_s.at[phase, d], recv_sem=ag_r.at[phase, d],
                device_id={'tp': chip(d) * 2 + 1 - c}, device_id_type=MESH)
            hops[d].start()

        def pass_on(d):
            slot = lax.rem(x + n_chip - d, n_chip)
            half = 1 - c if d == 0 else c
            cp = pltpu.make_async_remote_copy(
                src_ref=buf.at[half, slot], dst_ref=buf.at[half, slot], send_sem=agp_s.at[phase, d], recv_sem=agp_r.at[phase, d],
                device_id={'tp': partner}, device_id_type=MESH)
            cp.start()
            return cp

        passed = [pass_on(0)]
        for d in sorted(hops, key=lambda d: min(d, n_chip - d)):
            hops[d].wait_recv()
            passed.append(pass_on(d))
        for cp in passed:
            cp.wait()
        for d in hops:
            hops[d].wait_send()
        return buf[...].astype(F32).reshape(n_batch, width)

    if last:
        res = res_ref[...].astype(F32)
    else:
        res = res_ref[rows_of(1 - c, 0), :].astype(F32)
    total = reduce_scatter(0, part_ref)
    x_mid = (res + total + bo_ref[layer:layer + 1].astype(F32)).astype(BF16).astype(F32)
    normed = all_gather(0, gath, layer_norm_f32(x_mid, gain_ref[layer, 1:2], shift_ref[layer, 1:2])).astype(BF16)
    w_copies[0].wait()
    up = jnp.dot(normed, wu[...], preferred_element_type=F32) + bu_ref[layer:layer + 1].astype(F32)
    act = jax.nn.gelu(up, approximate=True).astype(BF16)
    if not last:
        wq_copy.start()
    w_copies[1].wait()
    part2[...] = jnp.dot(act, wd[...], preferred_element_type=F32)
    total = reduce_scatter(1, part2)
    x_next = (x_mid + total + bd_ref[layer:layer + 1].astype(F32)).astype(BF16)
    if last:
        out_ref[...] = all_gather(1, gath2, x_next).astype(BF16)
    else:
        own_ref[...] = x_next
        nxt = layer_norm_f32(x_next.astype(F32), gain_ref[layer + 1, 0:1], shift_ref[layer + 1, 0:1])
        normed = all_gather(1, gath2, nxt).astype(BF16)
        wq_copy.wait()
        qkv = jnp.dot(normed, wu[:, :n_qkv], preferred_element_type=F32) + bq_ref[layer + 1:layer + 2].astype(F32)
        out_ref[...] = qkv.astype(BF16).astype(F32)
        for w in w_copies[2:]:
            w.wait()


def solution(mesh):
    tp_size = mesh.shape['tp']
    vm = pl.BlockSpec(memory_space=pltpu.VMEM)
    sm = pl.BlockSpec(memory_space=pltpu.SMEM)
    hbm = pl.BlockSpec(memory_space=pltpu.HBM)

    def device_step(hidden, ln_gain, ln_shift, w_qkv, b_qkv, w_out, b_out, w_up, b_up, w_down, b_down, k_cache, v_cache, write_slot, key_pos, key_valid):
        n_layers, n_batch, cache_len, n_local, head_dim = k_cache.shape
        width = hidden.shape[-1]
        n_cols = cache_len * n_local
        flat = (n_layers, n_batch, n_cols, head_dim)
        in_hbm = functools.partial(pltpu.with_memory_space_constraint, memory_space=pltpu.HBM)
        k_in, v_in = in_hbm(k_cache.reshape(flat)), in_hbm(v_cache.reshape(flat))
        w_qkv, w_out, w_up, w_down = map(in_hbm, (w_qkv, w_out, w_up, w_down))
        x0 = hidden.reshape(n_batch, width)
        n_groups = n_batch // GROUP
        blk = n_batch // tp_size
        n_chip = tp_size // 2
        shape = jax.ShapeDtypeStruct(flat, BF16)
        held = pltpu.VMEM(flat, BF16)
        shared = [in_hbm(a) for a in (write_slot, key_pos, key_valid)]

        def attn(layer, x_in, caches):
            first = layer == 0
            n_qkv = b_qkv.shape[1]
            scratch = [
                pltpu.VMEM(key_pos.shape, jnp.int32),
                pltpu.VMEM(key_valid.shape, jnp.int32),
                pltpu.SMEM(write_slot.shape, jnp.int32),
                pltpu.VMEM(w_out.shape[1:], BF16),
                pltpu.VMEM((2, n_batch, n_cols), F32),
                pltpu.VMEM((n_batch, n_local * head_dim), F32),
                pltpu.SemaphoreType.DMA((5,)),
                pltpu.SemaphoreType.DMA((7,)),
                pltpu.SemaphoreType.DMA((4,)),
            ]
            alias = {}
            part = jax.ShapeDtypeStruct((n_batch, width), F32)
            outs, out_specs = (part, shape, shape, held, held), (vm, hbm, hbm, vm, vm)
            if first:
                ins = [in_hbm(a) for a in (x_in, ln_gain, ln_shift, b_qkv)] + [w_qkv, w_out] + shared + [k_in, v_in]
                specs = [hbm] * len(ins)
                scratch += [
                    pltpu.VMEM(x_in.shape, BF16),
                    pltpu.VMEM(ln_gain.shape, BF16),
                    pltpu.VMEM(ln_shift.shape, BF16),
                    pltpu.VMEM(b_qkv.shape, BF16),
                    pltpu.VMEM(w_qkv.shape[1:], BF16),
                    pltpu.VMEM((n_batch, n_qkv), F32),
                    pltpu.SemaphoreType.DMA((2, n_groups)),
                ]
            else:
                ins = [x_in, w_out] + shared + list(caches)
                specs = [vm, hbm] + [hbm] * len(shared) + [hbm] * 2 + [vm] * 2
                alias = {len(ins) - 4 + i: 1 + i for i in range(4)}
            return pl.pallas_call(
                functools.partial(attn_kernel, layer, n_local * tp_size, first),
                out_shape=outs,
                in_specs=specs,
                out_specs=out_specs,
                scratch_shapes=scratch,
                input_output_aliases=alias,
                compiler_params=pltpu.CompilerParams(vmem_limit_bytes=13 * MIB),
                name=f'attn_{layer}',
            )(*ins)

        def reduce(layer, part, res, caches=()):
            last = layer == n_layers - 1
            ins = [part, res, ln_gain, ln_shift, b_out, w_up, b_up, w_down, b_down]
            specs = [vm, vm, vm, vm, vm, hbm, vm, hbm, vm]
            outs = [jax.ShapeDtypeStruct((n_batch, width), BF16)]
            if not last:
                ins += [k_in, v_in, w_qkv, b_qkv, *caches]
                specs += [hbm, hbm, hbm, vm, vm, vm]
                outs = [jax.ShapeDtypeStruct((n_batch, b_qkv.shape[1]), F32)]
                outs += [jax.ShapeDtypeStruct((blk, width), BF16), held, held]
            dma = pltpu.SemaphoreType.DMA((2, n_chip))
            return pl.pallas_call(
                functools.partial(reduce_kernel, layer, tp_size, last),
                out_shape=tuple(outs),
                in_specs=specs,
                out_specs=tuple([vm] * len(outs)),
                scratch_shapes=[
                    pltpu.VMEM(w_up.shape[1:], BF16),
                    pltpu.VMEM(w_down.shape[1:], BF16),
                    pltpu.VMEM((n_batch, width), F32),
                    pltpu.VMEM((2, n_chip, blk, width), F32),
                    pltpu.VMEM((2, n_chip, blk, width), F32),
                    pltpu.VMEM((2, n_chip, blk, width), F32),
                    pltpu.VMEM((2, n_chip, blk, width), BF16),
                    pltpu.VMEM((2, n_chip, blk, width), BF16),
                    pltpu.SemaphoreType.DMA((6,)),
                ] + [dma] * 8,
                input_output_aliases={} if last else {len(ins) - 2: 2, len(ins) - 1: 3},
                compiler_params=pltpu.CompilerParams(vmem_limit_bytes=13 * MIB, collective_id=layer, has_side_effects=True),
                name=f'reduce_{layer}',
            )(*ins)

        part, k_new, v_new, k_held, v_held = attn(0, x0, None)
        qkv, x1, k_held, v_held = reduce(0, part, x0, (k_held, v_held))
        part, k_new, v_new, _, _ = attn(1, qkv, (k_new, v_new, k_held, v_held))
        (x_last,) = reduce(1, part, x1)
        return x_last[:, None, :], k_new.reshape(k_cache.shape), v_new.reshape(v_cache.shape)

    cache_spec = P(None, 'dp', None, 'tp', None)
    in_specs = (P('dp', None, None), P(), P(), P(None, None, 'tp'), P(None, 'tp'), P(None, 'tp', None), P(), P(None, None, 'tp'), P(None, 'tp'), P(None, 'tp', None), P(), cache_spec, cache_spec, P('dp'), P('dp', None), P('dp', None))
    out_specs = (P('dp', None, None), cache_spec, cache_spec)
    return jax.shard_map(device_step, mesh=mesh, in_specs=in_specs, out_specs=out_specs, check_vma=False)
```

```python
import functools
import math

import jax
import jax.numpy as jnp
from jax import lax
from jax.experimental import pallas as pl
from jax.experimental.pallas import tpu as pltpu
from jax.sharding import PartitionSpec as P

LN_EPS = 1e-5
MESH = pl.DeviceIdType.MESH
F32 = jnp.float32
BF16 = jnp.bfloat16
GROUP = 8
AHEAD = 6
SUB = 2
EARLY = 2
RS_DIRECT = 512
AG_PASSED = 1408
MIB = 2 ** 20


def layer_norm_f32(x_f32, gain, shift):
    mean_val = jnp.mean(x_f32, axis=-1, keepdims=True)
    centered = x_f32 - mean_val
    var_val = jnp.mean(centered * centered, axis=-1, keepdims=True)
    normed = centered * lax.rsqrt(var_val + LN_EPS)
    return (normed * gain.astype(F32) + shift.astype(F32)).astype(BF16)


def attn_kernel(layer, n_heads, first, *refs):
    if first:
        (x_in_ref, gain_in, shift_in, bq_in, wq_hbm, wo_hbm, slot_hbm, pos_in, valid_in, k_hbm, v_hbm,
         part_ref, k_out, v_out, kall, vall,
         pos_ref, valid_ref, slot_smem, wo, bias, attn, sem_w, sem_s, sem_out,
         x_ref, gain_ref, shift_ref, bq_ref, wq, qkv, sem_in) = refs
        old = []
    else:
        (qkv, wo_hbm, slot_hbm, pos_in, valid_in, k_part, v_part, k_raw, v_raw,
         part_ref, k_out, v_out, kall, vall,
         pos_ref, valid_ref, slot_smem, wo, bias, attn, sem_w, sem_s, sem_out) = refs
    kbuf, vbuf = kall.at[layer], vall.at[layer]
    n_batch, n_cols, head_dim = kbuf.shape
    n_groups = n_batch // GROUP
    n_local = attn.shape[1] // head_dim
    cache_len = n_cols // n_local
    n_chunk = 4
    pairs = [(slot_hbm, slot_smem), (pos_in, pos_ref), (valid_in, valid_ref)]
    if first:
        pairs = [(x_in_ref, x_ref), (gain_in, gain_ref), (shift_in, shift_ref), (bq_in, bq_ref)] + pairs
    small = [pltpu.make_async_copy(src, dst, sem_s.at[i]) for i, (src, dst) in enumerate(pairs)]
    for c in small:
        c.start()
    wo_copy = pltpu.make_async_copy(wo_hbm.at[layer], wo, sem_w.at[n_chunk])
    if first:
        step = x_ref.shape[1] // n_chunk
        w_copies = [
            pltpu.make_async_copy(wq_hbm.at[layer, pl.ds(i * step, step)], wq.at[pl.ds(i * step, step)], sem_w.at[i])
            for i in range(n_chunk)
        ]
        for c in w_copies:
            c.start()

    def in_copy(which, g):
        src, dst = ((k_hbm, kbuf), (v_hbm, vbuf))[which]
        return pltpu.make_async_copy(src.at[layer, pl.ds(g * GROUP, GROUP)], dst.at[pl.ds(g * GROUP, GROUP)], sem_in.at[which, g])

    def out_copy(which, g):
        src, dst = ((kbuf, k_out), (vbuf, v_out))[which]
        return pltpu.make_async_copy(src.at[pl.ds(g * GROUP, GROUP)], dst.at[layer, pl.ds(g * GROUP, GROUP)], sem_out.at[which])

    if first:
        for g in range(AHEAD - n_chunk):
            in_copy(0, g).start()
            in_copy(1, g).start()
    else:
        wo_copy.start()
        old = [
            pltpu.make_async_copy(src.at[layer - 1, pl.ds(g * GROUP, GROUP)], dst.at[layer - 1, pl.ds(g * GROUP, GROUP)], sem_out.at[2 + i])
            for g in range(EARLY, n_groups) for i, (src, dst) in enumerate(((kall, k_out), (vall, v_out)))
        ]
        for c in old:
            c.start()

    t_row = lax.broadcasted_iota(jnp.int32, (cache_len, n_cols), 0)
    t_col = lax.broadcasted_iota(jnp.int32, (cache_len, n_cols), 1) // n_local
    spread = (t_row == t_col).astype(BF16)
    for c in small:
        c.wait()
    pos = jnp.dot(pos_ref[...].astype(F32).astype(BF16), spread, preferred_element_type=F32)
    valid = jnp.dot(valid_ref[...].astype(F32).astype(BF16), spread, preferred_element_type=F32)
    bias[0] = pos
    bias[1] = valid

    if first:
        x_in = layer_norm_f32(x_ref[...].astype(F32), gain_ref[layer, 0:1], shift_ref[layer, 0:1])
        acc = None
        for i in range(n_chunk):
            w_copies[i].wait()
            in_copy(0, AHEAD - n_chunk + i).start()
            in_copy(1, AHEAD - n_chunk + i).start()
            d = jnp.dot(x_in[:, i * step:(i + 1) * step], wq[i * step:(i + 1) * step], preferred_element_type=F32)
            acc = d if acc is None else acc + d
        qkv[...] = (acc + bq_ref[layer:layer + 1].astype(F32)).astype(BF16).astype(F32)

    scale = 1.0 / math.sqrt(head_dim)
    rows = n_local * GROUP
    head0 = lax.axis_index('tp') * n_local

    def update(g):
        base = pl.multiple_of(g * GROUP, GROUP)
        row16 = lax.broadcasted_iota(jnp.int32, (16, head_dim), 0)
        fresh = qkv[pl.ds(base, GROUP), :]
        row8 = lax.broadcasted_iota(jnp.int32, (GROUP, n_cols), 0)
        slots = jnp.zeros((GROUP, n_cols), jnp.int32)
        for b in range(GROUP):
            slot = slot_smem[g * GROUP + b]
            slots = jnp.where(row8 == b, slot, slots)
            first_row = slot * n_local
            start = pl.multiple_of((first_row // 16) * 16, 16)
            off = first_row - start
            for which, buf in ((1, kbuf), (2, vbuf)):
                block = buf[base + b, pl.ds(start, 16), :].astype(F32)
                for h in range(n_local):
                    new = fresh[b:b + 1, (3 * h + which) * head_dim:(3 * h + which + 1) * head_dim]
                    block = jnp.where(row16 == off + h, new, block)
                buf[base + b, pl.ds(start, 16), :] = block.astype(BF16)
        col = lax.broadcasted_iota(jnp.int32, (GROUP, n_cols), 1)
        allowed = jnp.logical_or(bias[1, pl.ds(base, GROUP)] > 0.5, col // n_local == slots)
        pos_g = bias[0, pl.ds(base, GROUP)]
        parts = []
        for h in range(n_local):
            num = (jnp.full((GROUP, n_cols), 1 + h, jnp.int32) + head0).astype(F32)
            slope = jnp.exp2(-8.0 * num / n_heads)
            parts.append(jnp.where(jnp.logical_and(allowed, col % n_local == h), slope * pos_g, -jnp.inf))
        queries = jnp.concatenate([fresh[:, 3 * h * head_dim:(3 * h + 1) * head_dim] for h in range(n_local)], axis=0)
        odd = lax.broadcasted_iota(jnp.int32, (rows, head_dim), 0) % 2 == 1
        q_pair = jnp.concatenate([jnp.where(odd, 0.0, queries), jnp.where(odd, queries, 0.0)], axis=1).astype(BF16)
        return base, q_pair, jnp.concatenate(parts, axis=0)

    def scores(base, q_pair, add):
        row_s = lax.broadcasted_iota(jnp.int32, (rows, n_cols), 0) % GROUP // 2
        s = None
        for b in range(0, GROUP, 2):
            keys = jnp.concatenate([kbuf[base + b], kbuf[base + b + 1]], axis=1)
            sb = lax.dot_general(q_pair, keys, (((1,), (1,)), ((), ())), preferred_element_type=F32)
            s = sb if s is None else jnp.where(row_s == b // 2, sb, s)
        return s * scale + add

    def softmax(s):
        top = jnp.max(s, axis=-1, keepdims=True)
        e = jnp.exp(s - top)
        return (e * (1.0 / jnp.sum(e, axis=-1, keepdims=True))).astype(BF16)

    def mix(base, p):
        row_o = lax.broadcasted_iota(jnp.int32, (rows, head_dim), 0) % GROUP
        o = None
        for b in range(0, GROUP, 2):
            values = jnp.concatenate([vbuf[base + b], vbuf[base + b + 1]], axis=1)
            ob = jnp.dot(p, values, preferred_element_type=F32)
            for i in range(2):
                oi = ob[:, i * head_dim:(i + 1) * head_dim]
                o = oi if o is None else jnp.where(row_o == b + i, oi, o)
        for h in range(n_local):
            attn[pl.ds(base, GROUP), h * head_dim:(h + 1) * head_dim] = o[h * GROUP:(h + 1) * GROUP]

    def groups(i, carry):
        todo = [i * SUB + j for j in range(SUB)]
        if first:
            for g in todo:
                in_copy(0, g).wait()
                in_copy(1, g).wait()

            @pl.when(todo[-1] + AHEAD < n_groups)
            def _():
                for g in todo:
                    in_copy(0, g + AHEAD).start()
                    in_copy(1, g + AHEAD).start()

            @pl.when(i == n_groups // SUB - 2)
            def _():
                wo_copy.start()

            @pl.when(i == n_groups // SUB - 1)
            def _():
                for g in range(EARLY):
                    out_copy(0, g).start()
                    out_copy(1, g).start()
        state = [update(g) for g in todo]
        probs = [scores(*st) for st in state]
        for (base, _, _), s in zip(state, probs):
            mix(base, softmax(s))
        if not first:
            for g in todo:
                out_copy(0, g).start()
                out_copy(1, g).start()
        return carry

    lax.fori_loop(0, n_groups // SUB, groups, 0)
    wo_copy.wait()
    part_ref[...] = jnp.dot(attn[...].astype(BF16), wo[...], preferred_element_type=F32)
    for c in old:
        c.wait()
    for g in range(EARLY if first else n_groups):
        out_copy(0, g).wait()
        out_copy(1, g).wait()


def reduce_kernel(layer, n_tp, last, *refs):
    (part_ref, res_ref, gain_ref, shift_ref, bo_ref, wu_hbm, bu_ref, wd_hbm, bd_ref) = refs[:9]
    if last:
        out_ref, rest = refs[9], refs[10:]
    else:
        (k_hbm, v_hbm, wq_hbm, bq_ref, k_raw, v_raw, out_ref, own_ref, kall, vall) = refs[9:19]
        rest = refs[19:]
    (wu, wd, part2, d2d, mid, got, near, gath, gath2, sem_w,
     pair_s, pair_r, chip_s, chip_r, ag_s, ag_r, agp_s, agp_r, dir_s, dir_r, agd_s, agd_r) = rest
    n_batch, width = part_ref.shape
    n_chip = n_tp // 2
    blk = n_batch // n_tp
    me = lax.axis_index('tp')
    x = me // 2
    c = me % 2
    partner = x * 2 + (1 - c)

    def chip(d):
        return lax.rem(x + d, n_chip)

    w_copies = [pltpu.make_async_copy(wu_hbm.at[layer], wu, sem_w.at[0]), pltpu.make_async_copy(wd_hbm.at[layer], wd, sem_w.at[1])]
    if not last:
        w_copies.append(pltpu.make_async_copy(k_hbm.at[layer + 1], kall.at[layer + 1], sem_w.at[2]))
        w_copies.append(pltpu.make_async_copy(v_hbm.at[layer + 1], vall.at[layer + 1], sem_w.at[3]))
        n_qkv = bq_ref.shape[1]
        wq = wu.at[:, pl.ds(0, n_qkv)]
        wq_copy = pltpu.make_async_copy(wq_hbm.at[layer + 1], wq, sem_w.at[4])
    barrier = pltpu.get_barrier_semaphore()
    for d in range(1, n_tp):
        pl.semaphore_signal(barrier, inc=1, device_id={'tp': lax.rem(me + d, n_tp)}, device_id_type=MESH)
    for w in w_copies:
        w.start()
    pl.semaphore_wait(barrier, n_tp - 1)

    order = [2, 1, 3, 0] if n_chip == 4 else list(range(1, n_chip)) + [0]

    def rows_of(core, d):
        return pl.ds(pl.multiple_of((core * n_chip + chip(d)) * blk, blk), blk)

    direct, passed_cols = pl.ds(0, RS_DIRECT), pl.ds(0, AG_PASSED)
    tail, spread = pl.ds(RS_DIRECT, width - RS_DIRECT), pl.ds(AG_PASSED, width - AG_PASSED)
    far = order[:-1]
    by_distance = sorted(order, key=lambda d: min(d, n_chip - d))

    def remote(src, dst, send_sem, recv_sem, to):
        return pltpu.make_async_remote_copy(src_ref=src, dst_ref=dst, send_sem=send_sem, recv_sem=recv_sem, device_id={'tp': to}, device_id_type=MESH)

    def reduce_scatter(phase, src, fill_tail=None):
        def straight(d, half, sender):
            return remote(src.at[rows_of(half, d), direct], near.at[phase, sender, d], dir_s.at[phase, half, d], dir_r.at[phase, sender, d], chip(d) * 2 + 1 - half)

        def paired(d):
            cols = tail if d else pl.ds(0, width)
            return remote(src.at[rows_of(1 - c, d), cols], d2d.at[phase, d, :, cols], pair_s.at[phase, d], pair_r.at[phase, d], partner)

        def onward(d):
            cols = tail if d else pl.ds(0, width)
            return remote(mid.at[phase, d, :, cols], got.at[phase, d, :, cols], chip_s.at[phase, d], chip_r.at[phase, d], chip(d) * 2 + 1 - c)

        for d in far:
            for half in range(2):
                straight(d, half, c).start()
        if fill_tail is not None:
            fill_tail()
        for d in order:
            paired(d).start()
        for d in order:
            paired(d).wait_recv()
            cols = tail if d else pl.ds(0, width)
            mid[phase, d, :, cols] = src[rows_of(c, d), cols] + d2d[phase, d, :, cols]
            onward(d).start()
        head = None
        for d in far:
            for sender in range(2):
                straight(d, 0, sender).wait_recv()
                head = near[phase, sender, d] if head is None else head + near[phase, sender, d]
        acc = None
        for d in by_distance:
            onward(d).wait_recv()
            if d == 0:
                head = head + got[phase, d, :, direct]
            acc = got[phase, d, :, tail] if acc is None else acc + got[phase, d, :, tail]
        for d in order:
            paired(d).wait_send()
            onward(d).wait_send()
        for d in far:
            for half in range(2):
                straight(d, half, c).wait_send()
        return jnp.concatenate([head, acc], axis=1)

    def all_gather(phase, buf, value):
        buf[1 - c, x] = value

        def onward(d):
            return remote(buf.at[1 - c, x, :, passed_cols], buf.at[1 - c, x, :, passed_cols], ag_s.at[phase, d], ag_r.at[phase, d], chip(d) * 2 + 1 - c)

        def straight(d, core, half, slot):
            part = buf.at[half, slot, :, spread]
            return remote(part, part, agd_s.at[phase, core, d], agd_r.at[phase, half, d], chip(d) * 2 + core)

        def pass_on(d):
            slot = lax.rem(x + n_chip - d, n_chip)
            half = c if d else 1 - c
            part = buf.at[half, slot, :, passed_cols] if d else buf.at[half, slot]
            return remote(part, part, agp_s.at[phase, d], agp_r.at[phase, d], partner)

        for d in far:
            onward(d).start()
        pass_on(0).start()
        for d in far:
            for core in range(2):
                straight(d, core, 1 - c, x).start()
        for d in by_distance[1:]:
            onward(d).wait_recv()
            pass_on(d).start()
        for d in far:
            for half in range(2):
                straight(d, 0, half, lax.rem(x + n_chip - d, n_chip)).wait_recv()
        for d in order:
            pass_on(d).wait()
        for d in far:
            onward(d).wait_send()
            for core in range(2):
                straight(d, core, 1 - c, x).wait_send()
        return buf[...].astype(F32).reshape(n_batch, width)

    if last:
        res = res_ref[...].astype(F32)
    else:
        res = res_ref[rows_of(1 - c, 0), :].astype(F32)
    total = reduce_scatter(0, part_ref)
    x_mid = (res + total + bo_ref[layer:layer + 1].astype(F32)).astype(BF16).astype(F32)
    normed = all_gather(0, gath, layer_norm_f32(x_mid, gain_ref[layer, 1:2], shift_ref[layer, 1:2])).astype(BF16)
    w_copies[0].wait()
    up = jnp.dot(normed, wu[...], preferred_element_type=F32) + bu_ref[layer:layer + 1].astype(F32)
    act = jax.nn.gelu(up, approximate=True).astype(BF16)
    if not last:
        wq_copy.start()
    w_copies[1].wait()
    part2[:, :RS_DIRECT] = jnp.dot(act, wd[:, :RS_DIRECT], preferred_element_type=F32)

    def fill_tail():
        part2[:, RS_DIRECT:] = jnp.dot(act, wd[:, RS_DIRECT:], preferred_element_type=F32)

    total = reduce_scatter(1, part2, fill_tail)
    x_next = (x_mid + total + bd_ref[layer:layer + 1].astype(F32)).astype(BF16)
    if last:
        out_ref[...] = all_gather(1, gath2, x_next).astype(BF16)
    else:
        own_ref[...] = x_next
        nxt = layer_norm_f32(x_next.astype(F32), gain_ref[layer + 1, 0:1], shift_ref[layer + 1, 0:1])
        normed = all_gather(1, gath2, nxt).astype(BF16)
        wq_copy.wait()
        qkv = jnp.dot(normed, wu[:, :n_qkv], preferred_element_type=F32) + bq_ref[layer + 1:layer + 2].astype(F32)
        out_ref[...] = qkv.astype(BF16).astype(F32)
        for w in w_copies[2:]:
            w.wait()


def solution(mesh):
    tp_size = mesh.shape['tp']
    vm = pl.BlockSpec(memory_space=pltpu.VMEM)
    sm = pl.BlockSpec(memory_space=pltpu.SMEM)
    hbm = pl.BlockSpec(memory_space=pltpu.HBM)

    def device_step(hidden, ln_gain, ln_shift, w_qkv, b_qkv, w_out, b_out, w_up, b_up, w_down, b_down, k_cache, v_cache, write_slot, key_pos, key_valid):
        n_layers, n_batch, cache_len, n_local, head_dim = k_cache.shape
        width = hidden.shape[-1]
        n_cols = cache_len * n_local
        flat = (n_layers, n_batch, n_cols, head_dim)
        in_hbm = functools.partial(pltpu.with_memory_space_constraint, memory_space=pltpu.HBM)
        k_in, v_in = in_hbm(k_cache.reshape(flat)), in_hbm(v_cache.reshape(flat))
        w_qkv, w_out, w_up, w_down = map(in_hbm, (w_qkv, w_out, w_up, w_down))
        x0 = hidden.reshape(n_batch, width)
        n_groups = n_batch // GROUP
        blk = n_batch // tp_size
        n_chip = tp_size // 2
        shape = jax.ShapeDtypeStruct(flat, BF16)
        held = pltpu.VMEM(flat, BF16)
        shared = [in_hbm(a) for a in (write_slot, key_pos, key_valid)]

        def attn(layer, x_in, caches):
            first = layer == 0
            n_qkv = b_qkv.shape[1]
            scratch = [
                pltpu.VMEM(key_pos.shape, jnp.int32),
                pltpu.VMEM(key_valid.shape, jnp.int32),
                pltpu.SMEM(write_slot.shape, jnp.int32),
                pltpu.VMEM(w_out.shape[1:], BF16),
                pltpu.VMEM((2, n_batch, n_cols), F32),
                pltpu.VMEM((n_batch, n_local * head_dim), F32),
                pltpu.SemaphoreType.DMA((5,)),
                pltpu.SemaphoreType.DMA((7,)),
                pltpu.SemaphoreType.DMA((4,)),
            ]
            alias = {}
            part = jax.ShapeDtypeStruct((n_batch, width), F32)
            outs, out_specs = (part, shape, shape, held, held), (vm, hbm, hbm, vm, vm)
            if first:
                ins = [in_hbm(a) for a in (x_in, ln_gain, ln_shift, b_qkv)] + [w_qkv, w_out] + shared + [k_in, v_in]
                specs = [hbm] * len(ins)
                scratch += [
                    pltpu.VMEM(x_in.shape, BF16),
                    pltpu.VMEM(ln_gain.shape, BF16),
                    pltpu.VMEM(ln_shift.shape, BF16),
                    pltpu.VMEM(b_qkv.shape, BF16),
                    pltpu.VMEM(w_qkv.shape[1:], BF16),
                    pltpu.VMEM((n_batch, n_qkv), F32),
                    pltpu.SemaphoreType.DMA((2, n_groups)),
                ]
            else:
                ins = [x_in, w_out] + shared + list(caches)
                specs = [vm, hbm] + [hbm] * len(shared) + [hbm] * 2 + [vm] * 2
                alias = {len(ins) - 4 + i: 1 + i for i in range(4)}
            return pl.pallas_call(
                functools.partial(attn_kernel, layer, n_local * tp_size, first),
                out_shape=outs,
                in_specs=specs,
                out_specs=out_specs,
                scratch_shapes=scratch,
                input_output_aliases=alias,
                compiler_params=pltpu.CompilerParams(vmem_limit_bytes=13 * MIB),
                name=f'attn_{layer}',
            )(*ins)

        def reduce(layer, part, res, caches=()):
            last = layer == n_layers - 1
            ins = [part, res, ln_gain, ln_shift, b_out, w_up, b_up, w_down, b_down]
            specs = [vm, vm, vm, vm, vm, hbm, vm, hbm, vm]
            outs = [jax.ShapeDtypeStruct((n_batch, width), BF16)]
            if not last:
                ins += [k_in, v_in, w_qkv, b_qkv, *caches]
                specs += [hbm, hbm, hbm, vm, vm, vm]
                outs = [jax.ShapeDtypeStruct((n_batch, b_qkv.shape[1]), F32)]
                outs += [jax.ShapeDtypeStruct((blk, width), BF16), held, held]
            dma = pltpu.SemaphoreType.DMA((2, n_chip))
            dma2 = pltpu.SemaphoreType.DMA((2, 2, n_chip))
            return pl.pallas_call(
                functools.partial(reduce_kernel, layer, tp_size, last),
                out_shape=tuple(outs),
                in_specs=specs,
                out_specs=tuple([vm] * len(outs)),
                scratch_shapes=[
                    pltpu.VMEM(w_up.shape[1:], BF16),
                    pltpu.VMEM(w_down.shape[1:], BF16),
                    pltpu.VMEM((n_batch, width), F32),
                    pltpu.VMEM((2, n_chip, blk, width), F32),
                    pltpu.VMEM((2, n_chip, blk, width), F32),
                    pltpu.VMEM((2, n_chip, blk, width), F32),
                    pltpu.VMEM((2, 2, n_chip, blk, RS_DIRECT), F32),
                    pltpu.VMEM((2, n_chip, blk, width), BF16),
                    pltpu.VMEM((2, n_chip, blk, width), BF16),
                    pltpu.SemaphoreType.DMA((6,)),
                ] + [dma] * 8 + [dma2] * 4,
                input_output_aliases={} if last else {len(ins) - 2: 2, len(ins) - 1: 3},
                compiler_params=pltpu.CompilerParams(vmem_limit_bytes=13 * MIB, collective_id=layer, has_side_effects=True),
                name=f'reduce_{layer}',
            )(*ins)

        part, k_new, v_new, k_held, v_held = attn(0, x0, None)
        qkv, x1, k_held, v_held = reduce(0, part, x0, (k_held, v_held))
        part, k_new, v_new, _, _ = attn(1, qkv, (k_new, v_new, k_held, v_held))
        (x_last,) = reduce(1, part, x1)
        return x_last[:, None, :], k_new.reshape(k_cache.shape), v_new.reshape(v_cache.shape)

    cache_spec = P(None, 'dp', None, 'tp', None)
    in_specs = (P('dp', None, None), P(), P(), P(None, None, 'tp'), P(None, 'tp'), P(None, 'tp', None), P(), P(None, None, 'tp'), P(None, 'tp'), P(None, 'tp', None), P(), cache_spec, cache_spec, P('dp'), P('dp', None), P('dp', None))
    out_specs = (P('dp', None, None), cache_spec, cache_spec)
    return jax.shard_map(device_step, mesh=mesh, in_specs=in_specs, out_specs=out_specs, check_vma=False)
```

```python
import functools
import math

import jax
import jax.numpy as jnp
from jax import lax
from jax.experimental import pallas as pl
from jax.experimental.pallas import tpu as pltpu
from jax.sharding import PartitionSpec as P

LN_EPS = 1e-5
MESH = pl.DeviceIdType.MESH
F32 = jnp.float32
BF16 = jnp.bfloat16
GROUP = 8
AHEAD = 6
SUB = 2
EARLY = 2
MIB = 2 ** 20


def layer_norm_f32(x_f32, gain, shift):
    mean_val = jnp.mean(x_f32, axis=-1, keepdims=True)
    centered = x_f32 - mean_val
    var_val = jnp.mean(centered * centered, axis=-1, keepdims=True)
    normed = centered * lax.rsqrt(var_val + LN_EPS)
    return (normed * gain.astype(F32) + shift.astype(F32)).astype(BF16)


def attn_kernel(layer, n_heads, first, *refs):
    if first:
        (x_in_ref, gain_in, shift_in, bq_in, wq_hbm, slot_hbm, pos_in, valid_in, k_hbm, v_hbm,
         attn_ref, k_out, v_out, kall, vall,
         pos_ref, valid_ref, slot_smem, bias, attn, sem_w, sem_s, sem_out,
         x_ref, gain_ref, shift_ref, bq_ref, wq, qkv, sem_in) = refs
        old = []
    else:
        (qkv, slot_hbm, pos_in, valid_in, k_part, v_part, k_raw, v_raw,
         attn_ref, k_out, v_out, kall, vall,
         pos_ref, valid_ref, slot_smem, bias, attn, sem_w, sem_s, sem_out) = refs
    kbuf, vbuf = kall.at[layer], vall.at[layer]
    n_batch, n_cols, head_dim = kbuf.shape
    n_groups = n_batch // GROUP
    n_local = attn.shape[1] // head_dim
    cache_len = n_cols // n_local
    n_chunk = 4
    pairs = [(slot_hbm, slot_smem), (pos_in, pos_ref), (valid_in, valid_ref)]
    if first:
        pairs = [(x_in_ref, x_ref), (gain_in, gain_ref), (shift_in, shift_ref), (bq_in, bq_ref)] + pairs
    small = [pltpu.make_async_copy(src, dst, sem_s.at[i]) for i, (src, dst) in enumerate(pairs)]
    for c in small:
        c.start()
    if first:
        step = x_ref.shape[1] // n_chunk
        w_copies = [
            pltpu.make_async_copy(wq_hbm.at[layer, pl.ds(i * step, step)], wq.at[pl.ds(i * step, step)], sem_w.at[i])
            for i in range(n_chunk)
        ]
        for c in w_copies:
            c.start()

    def in_copy(which, g):
        src, dst = ((k_hbm, kbuf), (v_hbm, vbuf))[which]
        return pltpu.make_async_copy(src.at[layer, pl.ds(g * GROUP, GROUP)], dst.at[pl.ds(g * GROUP, GROUP)], sem_in.at[which, g])

    def out_copy(which, g):
        src, dst = ((kbuf, k_out), (vbuf, v_out))[which]
        return pltpu.make_async_copy(src.at[pl.ds(g * GROUP, GROUP)], dst.at[layer, pl.ds(g * GROUP, GROUP)], sem_out.at[which])

    if first:
        for g in range(AHEAD - n_chunk):
            in_copy(0, g).start()
            in_copy(1, g).start()
    else:
        old = [
            pltpu.make_async_copy(src.at[layer - 1, pl.ds(g * GROUP, GROUP)], dst.at[layer - 1, pl.ds(g * GROUP, GROUP)], sem_out.at[2 + i])
            for g in range(EARLY, n_groups) for i, (src, dst) in enumerate(((kall, k_out), (vall, v_out)))
        ]
        for c in old:
            c.start()

    t_row = lax.broadcasted_iota(jnp.int32, (cache_len, n_cols), 0)
    t_col = lax.broadcasted_iota(jnp.int32, (cache_len, n_cols), 1) // n_local
    spread = (t_row == t_col).astype(BF16)
    for c in small:
        c.wait()
    pos = jnp.dot(pos_ref[...].astype(F32).astype(BF16), spread, preferred_element_type=F32)
    valid = jnp.dot(valid_ref[...].astype(F32).astype(BF16), spread, preferred_element_type=F32)
    bias[0] = pos
    bias[1] = valid

    if first:
        x_in = layer_norm_f32(x_ref[...].astype(F32), gain_ref[layer, 0:1], shift_ref[layer, 0:1])
        acc = None
        for i in range(n_chunk):
            w_copies[i].wait()
            in_copy(0, AHEAD - n_chunk + i).start()
            in_copy(1, AHEAD - n_chunk + i).start()
            d = jnp.dot(x_in[:, i * step:(i + 1) * step], wq[i * step:(i + 1) * step], preferred_element_type=F32)
            acc = d if acc is None else acc + d
        qkv[...] = (acc + bq_ref[layer:layer + 1].astype(F32)).astype(BF16).astype(F32)

    scale = 1.0 / math.sqrt(head_dim)
    rows = n_local * GROUP
    head0 = lax.axis_index('tp') * n_local

    def update(g):
        base = pl.multiple_of(g * GROUP, GROUP)
        row16 = lax.broadcasted_iota(jnp.int32, (16, head_dim), 0)
        fresh = qkv[pl.ds(base, GROUP), :]
        row8 = lax.broadcasted_iota(jnp.int32, (GROUP, n_cols), 0)
        slots = jnp.zeros((GROUP, n_cols), jnp.int32)
        for b in range(GROUP):
            slot = slot_smem[g * GROUP + b]
            slots = jnp.where(row8 == b, slot, slots)
            first_row = slot * n_local
            start = pl.multiple_of((first_row // 16) * 16, 16)
            off = first_row - start
            for which, buf in ((1, kbuf), (2, vbuf)):
                block = buf[base + b, pl.ds(start, 16), :].astype(F32)
                for h in range(n_local):
                    new = fresh[b:b + 1, (3 * h + which) * head_dim:(3 * h + which + 1) * head_dim]
                    block = jnp.where(row16 == off + h, new, block)
                buf[base + b, pl.ds(start, 16), :] = block.astype(BF16)
        col = lax.broadcasted_iota(jnp.int32, (GROUP, n_cols), 1)
        allowed = jnp.logical_or(bias[1, pl.ds(base, GROUP)] > 0.5, col // n_local == slots)
        pos_g = bias[0, pl.ds(base, GROUP)]
        parts = []
        for h in range(n_local):
            num = (jnp.full((GROUP, n_cols), 1 + h, jnp.int32) + head0).astype(F32)
            slope = jnp.exp2(-8.0 * num / n_heads)
            parts.append(jnp.where(jnp.logical_and(allowed, col % n_local == h), slope * pos_g, -jnp.inf))
        queries = jnp.concatenate([fresh[:, 3 * h * head_dim:(3 * h + 1) * head_dim] for h in range(n_local)], axis=0)
        odd = lax.broadcasted_iota(jnp.int32, (rows, head_dim), 0) % 2 == 1
        q_pair = jnp.concatenate([jnp.where(odd, 0.0, queries), jnp.where(odd, queries, 0.0)], axis=1).astype(BF16)
        return base, q_pair, jnp.concatenate(parts, axis=0)

    def scores(base, q_pair, add):
        row_s = lax.broadcasted_iota(jnp.int32, (rows, n_cols), 0) % GROUP // 2
        s = None
        for b in range(0, GROUP, 2):
            keys = jnp.concatenate([kbuf[base + b], kbuf[base + b + 1]], axis=1)
            sb = lax.dot_general(q_pair, keys, (((1,), (1,)), ((), ())), preferred_element_type=F32)
            s = sb if s is None else jnp.where(row_s == b // 2, sb, s)
        return s * scale + add

    def softmax(s):
        top = jnp.max(s, axis=-1, keepdims=True)
        e = jnp.exp(s - top)
        return (e * (1.0 / jnp.sum(e, axis=-1, keepdims=True))).astype(BF16)

    def mix(base, p):
        row_o = lax.broadcasted_iota(jnp.int32, (rows, head_dim), 0) % GROUP
        o = None
        for b in range(0, GROUP, 2):
            values = jnp.concatenate([vbuf[base + b], vbuf[base + b + 1]], axis=1)
            ob = jnp.dot(p, values, preferred_element_type=F32)
            for i in range(2):
                oi = ob[:, i * head_dim:(i + 1) * head_dim]
                o = oi if o is None else jnp.where(row_o == b + i, oi, o)
        for h in range(n_local):
            attn[pl.ds(base, GROUP), h * head_dim:(h + 1) * head_dim] = o[h * GROUP:(h + 1) * GROUP]

    def groups(i, carry):
        todo = [i * SUB + j for j in range(SUB)]
        if first:
            for g in todo:
                in_copy(0, g).wait()
                in_copy(1, g).wait()

            @pl.when(todo[-1] + AHEAD < n_groups)
            def _():
                for g in todo:
                    in_copy(0, g + AHEAD).start()
                    in_copy(1, g + AHEAD).start()

            @pl.when(i == n_groups // SUB - 1)
            def _():
                for g in range(EARLY):
                    out_copy(0, g).start()
                    out_copy(1, g).start()
        state = [update(g) for g in todo]
        probs = [scores(*st) for st in state]
        for (base, _, _), s in zip(state, probs):
            mix(base, softmax(s))
        if not first:
            for g in todo:
                out_copy(0, g).start()
                out_copy(1, g).start()
        return carry

    lax.fori_loop(0, n_groups // SUB, groups, 0)
    attn_ref[...] = attn[...].astype(BF16)
    for c in old:
        c.wait()
    for g in range(EARLY if first else n_groups):
        out_copy(0, g).wait()
        out_copy(1, g).wait()


def reduce_kernel(layer, n_tp, last, *refs):
    (attn_ref, wo_hbm, res_ref, gain_ref, shift_ref, bo_ref, wu_hbm, bu_ref, wd_hbm, bd_ref) = refs[:10]
    if last:
        out_ref, rest = refs[10], refs[11:]
    else:
        (k_hbm, v_hbm, wq_hbm, bq_ref, k_raw, v_raw, out_ref, own_ref, kall, vall) = refs[10:20]
        rest = refs[20:]
    (wo, wu, wd, part_ref, part2, d2d, mid, got, gath, gath2, sem_w,
     pair_s, pair_r, chip_s, chip_r, ag_s, ag_r, agp_s, agp_r) = rest
    n_batch, width = part_ref.shape
    n_chip = n_tp // 2
    blk = n_batch // n_tp
    me = lax.axis_index('tp')
    x = me // 2
    c = me % 2
    partner = x * 2 + (1 - c)

    def chip(d):
        return lax.rem(x + d, n_chip)

    wo_copy = pltpu.make_async_copy(wo_hbm.at[layer], wo, sem_w.at[5])
    wo_copy.start()
    w_copies = [pltpu.make_async_copy(wu_hbm.at[layer], wu, sem_w.at[0]), pltpu.make_async_copy(wd_hbm.at[layer], wd, sem_w.at[1])]
    if not last:
        w_copies.append(pltpu.make_async_copy(k_hbm.at[layer + 1], kall.at[layer + 1], sem_w.at[2]))
        w_copies.append(pltpu.make_async_copy(v_hbm.at[layer + 1], vall.at[layer + 1], sem_w.at[3]))
        n_qkv = bq_ref.shape[1]
        wq = wu.at[:, pl.ds(0, n_qkv)]
        wq_copy = pltpu.make_async_copy(wq_hbm.at[layer + 1], wq, sem_w.at[4])
    barrier = pltpu.get_barrier_semaphore()
    peers = [partner] + [chip(d) * 2 + 1 - c for d in range(1, n_chip)]
    for peer in peers:
        pl.semaphore_signal(barrier, inc=1, device_id={'tp': peer}, device_id_type=MESH)
    wo_copy.wait()
    for w in w_copies:
        w.start()
    part_ref[...] = jnp.dot(attn_ref[...], wo[...], preferred_element_type=F32)
    pl.semaphore_wait(barrier, len(peers))

    sent = []
    order = [2, 1, 3, 0] if n_chip == 4 else list(range(1, n_chip)) + [0]

    def rows_of(core, d):
        return pl.ds(pl.multiple_of((core * n_chip + chip(d)) * blk, blk), blk)

    def reduce_scatter(phase, src):
        pair = {
            d: pltpu.make_async_remote_copy(
                src_ref=src.at[rows_of(1 - c, d)], dst_ref=d2d.at[phase, d], send_sem=pair_s.at[phase, d],
                recv_sem=pair_r.at[phase, d], device_id={'tp': partner}, device_id_type=MESH)
            for d in order
        }
        for d in order:
            pair[d].start()
        hops = {}
        for d in order:
            pair[d].wait_recv()
            mid[phase, d] = src[rows_of(c, d), :] + d2d[phase, d]
            hops[d] = pltpu.make_async_remote_copy(
                src_ref=mid.at[phase, d], dst_ref=got.at[phase, d], send_sem=chip_s.at[phase, d],
                recv_sem=chip_r.at[phase, d], device_id={'tp': chip(d) * 2 + 1 - c}, device_id_type=MESH)
            hops[d].start()
        acc = None
        for d in sorted(hops, key=lambda d: min(d, n_chip - d)):
            hops[d].wait_recv()
            acc = got[phase, d] if acc is None else acc + got[phase, d]
        sent.extend([*pair.values(), *hops.values()])
        return acc

    def all_gather(phase, buf, value):
        buf[1 - c, x] = value
        hops = {}
        for d in order[:-1]:
            hops[d] = pltpu.make_async_remote_copy(
                src_ref=buf.at[1 - c, x], dst_ref=buf.at[1 - c, x], send_sem=ag_s.at[phase, d], recv_sem=ag_r.at[phase, d],
                device_id={'tp': chip(d) * 2 + 1 - c}, device_id_type=MESH)
            hops[d].start()

        def pass_on(d):
            slot = lax.rem(x + n_chip - d, n_chip)
            half = 1 - c if d == 0 else c
            cp = pltpu.make_async_remote_copy(
                src_ref=buf.at[half, slot], dst_ref=buf.at[half, slot], send_sem=agp_s.at[phase, d], recv_sem=agp_r.at[phase, d],
                device_id={'tp': partner}, device_id_type=MESH)
            cp.start()
            return cp

        passed = [pass_on(0)]
        for d in sorted(hops, key=lambda d: min(d, n_chip - d)):
            hops[d].wait_recv()
            passed.append(pass_on(d))
        for cp in passed:
            cp.wait_recv()
        sent.extend([*passed, *hops.values()])
        return buf[...].astype(F32).reshape(n_batch, width)

    if last:
        res = res_ref[...].astype(F32)
    else:
        res = res_ref[rows_of(1 - c, 0), :].astype(F32)
    total = reduce_scatter(0, part_ref)
    x_mid = (res + total + bo_ref[layer:layer + 1].astype(F32)).astype(BF16).astype(F32)
    normed = all_gather(0, gath, layer_norm_f32(x_mid, gain_ref[layer, 1:2], shift_ref[layer, 1:2])).astype(BF16)
    w_copies[0].wait()
    up = jnp.dot(normed, wu[...], preferred_element_type=F32) + bu_ref[layer:layer + 1].astype(F32)
    act = jax.nn.gelu(up, approximate=True).astype(BF16)
    if not last:
        wq_copy.start()
    w_copies[1].wait()
    part2[...] = jnp.dot(act, wd[...], preferred_element_type=F32)
    total = reduce_scatter(1, part2)
    x_next = (x_mid + total + bd_ref[layer:layer + 1].astype(F32)).astype(BF16)
    if last:
        out_ref[...] = all_gather(1, gath2, x_next).astype(BF16)
    else:
        own_ref[...] = x_next
        nxt = layer_norm_f32(x_next.astype(F32), gain_ref[layer + 1, 0:1], shift_ref[layer + 1, 0:1])
        normed = all_gather(1, gath2, nxt).astype(BF16)
        wq_copy.wait()
        qkv = jnp.dot(normed, wu[:, :n_qkv], preferred_element_type=F32) + bq_ref[layer + 1:layer + 2].astype(F32)
        out_ref[...] = qkv.astype(BF16).astype(F32)
        for w in w_copies[2:]:
            w.wait()
    for cp in sent:
        cp.wait_send()


def solution(mesh):
    tp_size = mesh.shape['tp']
    vm = pl.BlockSpec(memory_space=pltpu.VMEM)
    sm = pl.BlockSpec(memory_space=pltpu.SMEM)
    hbm = pl.BlockSpec(memory_space=pltpu.HBM)

    def device_step(hidden, ln_gain, ln_shift, w_qkv, b_qkv, w_out, b_out, w_up, b_up, w_down, b_down, k_cache, v_cache, write_slot, key_pos, key_valid):
        n_layers, n_batch, cache_len, n_local, head_dim = k_cache.shape
        width = hidden.shape[-1]
        n_cols = cache_len * n_local
        flat = (n_layers, n_batch, n_cols, head_dim)
        in_hbm = functools.partial(pltpu.with_memory_space_constraint, memory_space=pltpu.HBM)
        k_in, v_in = in_hbm(k_cache.reshape(flat)), in_hbm(v_cache.reshape(flat))
        w_qkv, w_out, w_up, w_down = map(in_hbm, (w_qkv, w_out, w_up, w_down))
        x0 = hidden.reshape(n_batch, width)
        n_groups = n_batch // GROUP
        blk = n_batch // tp_size
        n_chip = tp_size // 2
        shape = jax.ShapeDtypeStruct(flat, BF16)
        held = pltpu.VMEM(flat, BF16)
        shared = [in_hbm(a) for a in (write_slot, key_pos, key_valid)]

        def attn(layer, x_in, caches):
            first = layer == 0
            n_qkv = b_qkv.shape[1]
            scratch = [
                pltpu.VMEM(key_pos.shape, jnp.int32),
                pltpu.VMEM(key_valid.shape, jnp.int32),
                pltpu.SMEM(write_slot.shape, jnp.int32),
                pltpu.VMEM((2, n_batch, n_cols), F32),
                pltpu.VMEM((n_batch, n_local * head_dim), F32),
                pltpu.SemaphoreType.DMA((5,)),
                pltpu.SemaphoreType.DMA((7,)),
                pltpu.SemaphoreType.DMA((4,)),
            ]
            alias = {}
            part = jax.ShapeDtypeStruct((n_batch, n_local * head_dim), BF16)
            outs, out_specs = (part, shape, shape, held, held), (vm, hbm, hbm, vm, vm)
            if first:
                ins = [in_hbm(a) for a in (x_in, ln_gain, ln_shift, b_qkv)] + [w_qkv] + shared + [k_in, v_in]
                specs = [hbm] * len(ins)
                scratch += [
                    pltpu.VMEM(x_in.shape, BF16),
                    pltpu.VMEM(ln_gain.shape, BF16),
                    pltpu.VMEM(ln_shift.shape, BF16),
                    pltpu.VMEM(b_qkv.shape, BF16),
                    pltpu.VMEM(w_qkv.shape[1:], BF16),
                    pltpu.VMEM((n_batch, n_qkv), F32),
                    pltpu.SemaphoreType.DMA((2, n_groups)),
                ]
            else:
                ins = [x_in] + shared + list(caches)
                specs = [vm] + [hbm] * len(shared) + [hbm] * 2 + [vm] * 2
                alias = {len(ins) - 4 + i: 1 + i for i in range(4)}
            return pl.pallas_call(
                functools.partial(attn_kernel, layer, n_local * tp_size, first),
                out_shape=outs,
                in_specs=specs,
                out_specs=out_specs,
                scratch_shapes=scratch,
                input_output_aliases=alias,
                compiler_params=pltpu.CompilerParams(vmem_limit_bytes=14 * MIB),
                name=f'attn_{layer}',
            )(*ins)

        def reduce(layer, part, res, caches=()):
            last = layer == n_layers - 1
            ins = [part, w_out, res, ln_gain, ln_shift, b_out, w_up, b_up, w_down, b_down]
            specs = [vm, hbm, vm, vm, vm, vm, hbm, vm, hbm, vm]
            outs = [jax.ShapeDtypeStruct((n_batch, width), BF16)]
            if not last:
                ins += [k_in, v_in, w_qkv, b_qkv, *caches]
                specs += [hbm, hbm, hbm, vm, vm, vm]
                outs = [jax.ShapeDtypeStruct((n_batch, b_qkv.shape[1]), F32)]
                outs += [jax.ShapeDtypeStruct((blk, width), BF16), held, held]
            dma = pltpu.SemaphoreType.DMA((2, n_chip))
            return pl.pallas_call(
                functools.partial(reduce_kernel, layer, tp_size, last),
                out_shape=tuple(outs),
                in_specs=specs,
                out_specs=tuple([vm] * len(outs)),
                scratch_shapes=[
                    pltpu.VMEM(w_out.shape[1:], BF16),
                    pltpu.VMEM(w_up.shape[1:], BF16),
                    pltpu.VMEM(w_down.shape[1:], BF16),
                    pltpu.VMEM((n_batch, width), F32),
                    pltpu.VMEM((n_batch, width), F32),
                    pltpu.VMEM((2, n_chip, blk, width), F32),
                    pltpu.VMEM((2, n_chip, blk, width), F32),
                    pltpu.VMEM((2, n_chip, blk, width), F32),
                    pltpu.VMEM((2, n_chip, blk, width), BF16),
                    pltpu.VMEM((2, n_chip, blk, width), BF16),
                    pltpu.SemaphoreType.DMA((6,)),
                ] + [dma] * 8,
                input_output_aliases={} if last else {len(ins) - 2: 2, len(ins) - 1: 3},
                compiler_params=pltpu.CompilerParams(vmem_limit_bytes=14 * MIB, collective_id=layer, has_side_effects=True),
                name=f'reduce_{layer}',
            )(*ins)

        part, k_new, v_new, k_held, v_held = attn(0, x0, None)
        qkv, x1, k_held, v_held = reduce(0, part, x0, (k_held, v_held))
        part, k_new, v_new, _, _ = attn(1, qkv, (k_new, v_new, k_held, v_held))
        (x_last,) = reduce(1, part, x1)
        return x_last[:, None, :], k_new.reshape(k_cache.shape), v_new.reshape(v_cache.shape)

    cache_spec = P(None, 'dp', None, 'tp', None)
    in_specs = (P('dp', None, None), P(), P(), P(None, None, 'tp'), P(None, 'tp'), P(None, 'tp', None), P(), P(None, None, 'tp'), P(None, 'tp'), P(None, 'tp', None), P(), cache_spec, cache_spec, P('dp'), P('dp', None), P('dp', None))
    out_specs = (P('dp', None, None), cache_spec, cache_spec)
    return jax.shard_map(device_step, mesh=mesh, in_specs=in_specs, out_specs=out_specs, check_vma=False)
```

```python
import functools
import math

import jax
import jax.numpy as jnp
from jax import lax
from jax.experimental import pallas as pl
from jax.experimental.pallas import tpu as pltpu
from jax.sharding import PartitionSpec as P

LN_EPS = 1e-5
MESH = pl.DeviceIdType.MESH
F32 = jnp.float32
BF16 = jnp.bfloat16
GROUP = 8
AHEAD = 6
SUB = 2
EARLY = 2
MIB = 2 ** 20


def layer_norm_f32(x_f32, gain, shift):
    mean_val = jnp.mean(x_f32, axis=-1, keepdims=True)
    centered = x_f32 - mean_val
    var_val = jnp.mean(centered * centered, axis=-1, keepdims=True)
    normed = centered * lax.rsqrt(var_val + LN_EPS)
    return (normed * gain.astype(F32) + shift.astype(F32)).astype(BF16)


def attn_kernel(layer, n_heads, first, *refs):
    if first:
        (x_in_ref, gain_in, shift_in, bq_in, wq_hbm, wo_hbm, slot_hbm, pos_in, valid_in, k_hbm, v_hbm,
         part_ref, k_out, v_out, kall, vall,
         pos_ref, valid_ref, slot_smem, wo, bias, attn, sem_w, sem_s, sem_out,
         x_ref, gain_ref, shift_ref, bq_ref, wq, qkv, sem_in) = refs
        old = []
    else:
        (qkv, wo_hbm, slot_hbm, pos_in, valid_in, k_part, v_part, k_raw, v_raw,
         part_ref, k_out, v_out, kall, vall,
         pos_ref, valid_ref, slot_smem, wo, bias, attn, sem_w, sem_s, sem_out) = refs
    kbuf, vbuf = kall.at[layer], vall.at[layer]
    n_batch, n_cols, head_dim = kbuf.shape
    n_groups = n_batch // GROUP
    n_local = attn.shape[1] // head_dim
    cache_len = n_cols // n_local
    n_chunk = 4
    pairs = [(slot_hbm, slot_smem), (pos_in, pos_ref), (valid_in, valid_ref)]
    if first:
        pairs = [(x_in_ref, x_ref), (gain_in, gain_ref), (shift_in, shift_ref), (bq_in, bq_ref)] + pairs
    small = [pltpu.make_async_copy(src, dst, sem_s.at[i]) for i, (src, dst) in enumerate(pairs)]
    for c in small:
        c.start()
    wo_copy = pltpu.make_async_copy(wo_hbm.at[layer], wo, sem_w.at[n_chunk])
    if first:
        step = x_ref.shape[1] // n_chunk
        w_copies = [
            pltpu.make_async_copy(wq_hbm.at[layer, pl.ds(i * step, step)], wq.at[pl.ds(i * step, step)], sem_w.at[i])
            for i in range(n_chunk)
        ]
        for c in w_copies:
            c.start()

    def in_copy(which, g):
        src, dst = ((k_hbm, kbuf), (v_hbm, vbuf))[which]
        return pltpu.make_async_copy(src.at[layer, pl.ds(g * GROUP, GROUP)], dst.at[pl.ds(g * GROUP, GROUP)], sem_in.at[which, g])

    def out_copy(which, g):
        src, dst = ((kbuf, k_out), (vbuf, v_out))[which]
        return pltpu.make_async_copy(src.at[pl.ds(g * GROUP, GROUP)], dst.at[layer, pl.ds(g * GROUP, GROUP)], sem_out.at[which])

    if first:
        for g in range(AHEAD - n_chunk):
            in_copy(0, g).start()
            in_copy(1, g).start()
    else:
        wo_copy.start()
        old = [
            pltpu.make_async_copy(src.at[layer - 1, pl.ds(g * GROUP, GROUP)], dst.at[layer - 1, pl.ds(g * GROUP, GROUP)], sem_out.at[2 + i])
            for g in range(EARLY, n_groups) for i, (src, dst) in enumerate(((kall, k_out), (vall, v_out)))
        ]
        for c in old:
            c.start()

    t_row = lax.broadcasted_iota(jnp.int32, (cache_len, n_cols), 0)
    t_col = lax.broadcasted_iota(jnp.int32, (cache_len, n_cols), 1) // n_local
    spread = (t_row == t_col).astype(BF16)
    for c in small:
        c.wait()
    pos = jnp.dot(pos_ref[...].astype(F32).astype(BF16), spread, preferred_element_type=F32)
    valid = jnp.dot(valid_ref[...].astype(F32).astype(BF16), spread, preferred_element_type=F32)
    bias[0] = pos
    bias[1] = valid

    if first:
        x_in = layer_norm_f32(x_ref[...].astype(F32), gain_ref[layer, 0:1], shift_ref[layer, 0:1])
        acc = None
        for i in range(n_chunk):
            w_copies[i].wait()
            in_copy(0, AHEAD - n_chunk + i).start()
            in_copy(1, AHEAD - n_chunk + i).start()
            d = jnp.dot(x_in[:, i * step:(i + 1) * step], wq[i * step:(i + 1) * step], preferred_element_type=F32)
            acc = d if acc is None else acc + d
        qkv[...] = (acc + bq_ref[layer:layer + 1].astype(F32)).astype(BF16).astype(F32)

    scale = 1.0 / math.sqrt(head_dim)
    rows = n_local * GROUP
    head0 = lax.axis_index('tp') * n_local

    def update(g):
        base = pl.multiple_of(g * GROUP, GROUP)
        row16 = lax.broadcasted_iota(jnp.int32, (16, head_dim), 0)
        fresh = qkv[pl.ds(base, GROUP), :]
        row8 = lax.broadcasted_iota(jnp.int32, (GROUP, n_cols), 0)
        slots = jnp.zeros((GROUP, n_cols), jnp.int32)
        for b in range(GROUP):
            slot = slot_smem[g * GROUP + b]
            slots = jnp.where(row8 == b, slot, slots)
            first_row = slot * n_local
            start = pl.multiple_of((first_row // 16) * 16, 16)
            off = first_row - start
            for which, buf in ((1, kbuf), (2, vbuf)):
                block = buf[base + b, pl.ds(start, 16), :].astype(F32)
                for h in range(n_local):
                    new = fresh[b:b + 1, (3 * h + which) * head_dim:(3 * h + which + 1) * head_dim]
                    block = jnp.where(row16 == off + h, new, block)
                buf[base + b, pl.ds(start, 16), :] = block.astype(BF16)
        col = lax.broadcasted_iota(jnp.int32, (GROUP, n_cols), 1)
        allowed = jnp.logical_or(bias[1, pl.ds(base, GROUP)] > 0.5, col // n_local == slots)
        pos_g = bias[0, pl.ds(base, GROUP)]
        parts = []
        for h in range(n_local):
            num = (jnp.full((GROUP, n_cols), 1 + h, jnp.int32) + head0).astype(F32)
            slope = jnp.exp2(-8.0 * num / n_heads)
            parts.append(jnp.where(jnp.logical_and(allowed, col % n_local == h), slope * pos_g, -jnp.inf))
        queries = jnp.concatenate([fresh[:, 3 * h * head_dim:(3 * h + 1) * head_dim] for h in range(n_local)], axis=0)
        odd = lax.broadcasted_iota(jnp.int32, (rows, head_dim), 0) % 2 == 1
        q_pair = jnp.concatenate([jnp.where(odd, 0.0, queries), jnp.where(odd, queries, 0.0)], axis=1).astype(BF16)
        return base, q_pair, jnp.concatenate(parts, axis=0)

    def scores(base, q_pair, add):
        row_s = lax.broadcasted_iota(jnp.int32, (rows, n_cols), 0) % GROUP // 2
        s = None
        for b in range(0, GROUP, 2):
            keys = jnp.concatenate([kbuf[base + b], kbuf[base + b + 1]], axis=1)
            sb = lax.dot_general(q_pair, keys, (((1,), (1,)), ((), ())), preferred_element_type=F32)
            s = sb if s is None else jnp.where(row_s == b // 2, sb, s)
        return s * scale + add

    def softmax(s):
        top = jnp.max(s, axis=-1, keepdims=True)
        e = jnp.exp(s - top)
        return (e * (1.0 / jnp.sum(e, axis=-1, keepdims=True))).astype(BF16)

    def mix(base, p):
        row_o = lax.broadcasted_iota(jnp.int32, (rows, head_dim), 0) % GROUP
        o = None
        for b in range(0, GROUP, 2):
            values = jnp.concatenate([vbuf[base + b], vbuf[base + b + 1]], axis=1)
            ob = jnp.dot(p, values, preferred_element_type=F32)
            for i in range(2):
                oi = ob[:, i * head_dim:(i + 1) * head_dim]
                o = oi if o is None else jnp.where(row_o == b + i, oi, o)
        for h in range(n_local):
            attn[pl.ds(base, GROUP), h * head_dim:(h + 1) * head_dim] = o[h * GROUP:(h + 1) * GROUP]

    def groups(i, carry):
        todo = [i * SUB + j for j in range(SUB)]
        if first:
            for g in todo:
                in_copy(0, g).wait()
                in_copy(1, g).wait()

            @pl.when(todo[-1] + AHEAD < n_groups)
            def _():
                for g in todo:
                    in_copy(0, g + AHEAD).start()
                    in_copy(1, g + AHEAD).start()

            @pl.when(i == n_groups // SUB - 2)
            def _():
                wo_copy.start()

            @pl.when(i == n_groups // SUB - 1)
            def _():
                for g in range(EARLY):
                    out_copy(0, g).start()
                    out_copy(1, g).start()
        state = [update(g) for g in todo]
        probs = [scores(*st) for st in state]
        for (base, _, _), s in zip(state, probs):
            mix(base, softmax(s))
        if not first:
            for g in todo:
                out_copy(0, g).start()
                out_copy(1, g).start()
        return carry

    lax.fori_loop(0, n_groups // SUB, groups, 0)
    wo_copy.wait()
    part_ref[...] = jnp.dot(attn[...].astype(BF16), wo[...], preferred_element_type=F32)
    for c in old:
        c.wait()
    for g in range(EARLY if first else n_groups):
        out_copy(0, g).wait()
        out_copy(1, g).wait()


def reduce_kernel(layer, n_tp, last, *refs):
    (part_ref, res_ref, gain_ref, shift_ref, bo_ref, wu_hbm, bu_ref, wd_hbm, bd_ref) = refs[:9]
    if last:
        out_ref, rest = refs[9], refs[10:]
    else:
        (k_hbm, v_hbm, wq_hbm, bq_ref, k_raw, v_raw, out_ref, own_ref, kall, vall) = refs[9:19]
        rest = refs[19:]
    (wu, wd, part2, d2d, mid, got, gath, gath2, sem_w,
     pair_s, pair_r, chip_s, chip_r, ag_s, ag_r, agp_s, agp_r) = rest
    n_batch, width = part_ref.shape
    n_chip = n_tp // 2
    blk = n_batch // n_tp
    me = lax.axis_index('tp')
    x = me // 2
    c = me % 2
    partner = x * 2 + (1 - c)

    def chip(d):
        return lax.rem(x + d, n_chip)

    w_copies = [pltpu.make_async_copy(wu_hbm.at[layer], wu, sem_w.at[0]), pltpu.make_async_copy(wd_hbm.at[layer], wd, sem_w.at[1])]
    if not last:
        w_copies.append(pltpu.make_async_copy(k_hbm.at[layer + 1], kall.at[layer + 1], sem_w.at[2]))
        w_copies.append(pltpu.make_async_copy(v_hbm.at[layer + 1], vall.at[layer + 1], sem_w.at[3]))
        n_qkv = bq_ref.shape[1]
        wq = wu.at[:, pl.ds(0, n_qkv)]
        wq_copy = pltpu.make_async_copy(wq_hbm.at[layer + 1], wq, sem_w.at[4])
    barrier = pltpu.get_barrier_semaphore()
    peers = [partner] + [chip(d) * 2 + 1 - c for d in range(1, n_chip)]
    for peer in peers:
        pl.semaphore_signal(barrier, inc=1, device_id={'tp': peer}, device_id_type=MESH)
    for w in w_copies:
        w.start()
    pl.semaphore_wait(barrier, len(peers))

    sent = []
    order = [2, 1, 3, 0] if n_chip == 4 else list(range(1, n_chip)) + [0]

    def rows_of(core, d):
        return pl.ds(pl.multiple_of((core * n_chip + chip(d)) * blk, blk), blk)

    def reduce_scatter(phase, src):
        pair = {
            d: pltpu.make_async_remote_copy(
                src_ref=src.at[rows_of(1 - c, d)], dst_ref=d2d.at[phase, d], send_sem=pair_s.at[phase, d],
                recv_sem=pair_r.at[phase, d], device_id={'tp': partner}, device_id_type=MESH)
            for d in order
        }
        for d in order:
            pair[d].start()
        hops = {}
        for d in order:
            pair[d].wait_recv()
            mid[phase, d] = src[rows_of(c, d), :] + d2d[phase, d]
            hops[d] = pltpu.make_async_remote_copy(
                src_ref=mid.at[phase, d], dst_ref=got.at[phase, d], send_sem=chip_s.at[phase, d],
                recv_sem=chip_r.at[phase, d], device_id={'tp': chip(d) * 2 + 1 - c}, device_id_type=MESH)
            hops[d].start()
        acc = None
        for d in sorted(hops, key=lambda d: min(d, n_chip - d)):
            hops[d].wait_recv()
            acc = got[phase, d] if acc is None else acc + got[phase, d]
        sent.extend([*pair.values(), *hops.values()])
        return acc

    def all_gather(phase, buf, value):
        buf[1 - c, x] = value
        hops = {}
        for d in order[:-1]:
            hops[d] = pltpu.make_async_remote_copy(
                src_ref=buf.at[1 - c, x], dst_ref=buf.at[1 - c, x], send_sem=ag_s.at[phase, d], recv_sem=ag_r.at[phase, d],
                device_id={'tp': chip(d) * 2 + 1 - c}, device_id_type=MESH)
            hops[d].start()

        def pass_on(d):
            slot = lax.rem(x + n_chip - d, n_chip)
            half = 1 - c if d == 0 else c
            cp = pltpu.make_async_remote_copy(
                src_ref=buf.at[half, slot], dst_ref=buf.at[half, slot], send_sem=agp_s.at[phase, d], recv_sem=agp_r.at[phase, d],
                device_id={'tp': partner}, device_id_type=MESH)
            cp.start()
            return cp

        passed = [pass_on(0)]
        for d in sorted(hops, key=lambda d: min(d, n_chip - d)):
            hops[d].wait_recv()
            passed.append(pass_on(d))
        for cp in passed:
            cp.wait_recv()
        sent.extend([*passed, *hops.values()])
        return buf[...].astype(F32).reshape(n_batch, width)

    if last:
        res = res_ref[...].astype(F32)
    else:
        res = res_ref[rows_of(1 - c, 0), :].astype(F32)
    total = reduce_scatter(0, part_ref)
    x_mid = (res + total + bo_ref[layer:layer + 1].astype(F32)).astype(BF16).astype(F32)
    normed = all_gather(0, gath, layer_norm_f32(x_mid, gain_ref[layer, 1:2], shift_ref[layer, 1:2])).astype(BF16)
    w_copies[0].wait()
    up = jnp.dot(normed, wu[...], preferred_element_type=F32) + bu_ref[layer:layer + 1].astype(F32)
    act = jax.nn.gelu(up, approximate=True).astype(BF16)
    if not last:
        wq_copy.start()
    w_copies[1].wait()
    part2[...] = jnp.dot(act, wd[...], preferred_element_type=F32)
    total = reduce_scatter(1, part2)
    x_next = (x_mid + total + bd_ref[layer:layer + 1].astype(F32)).astype(BF16)
    if last:
        out_ref[...] = all_gather(1, gath2, x_next).astype(BF16)
    else:
        own_ref[...] = x_next
        nxt = layer_norm_f32(x_next.astype(F32), gain_ref[layer + 1, 0:1], shift_ref[layer + 1, 0:1])
        normed = all_gather(1, gath2, nxt).astype(BF16)
        wq_copy.wait()
        qkv = jnp.dot(normed, wu[:, :n_qkv], preferred_element_type=F32) + bq_ref[layer + 1:layer + 2].astype(F32)
        out_ref[...] = qkv.astype(BF16).astype(F32)
        for w in w_copies[2:]:
            w.wait()
    for cp in sent:
        cp.wait_send()


def solution(mesh):
    tp_size = mesh.shape['tp']
    vm = pl.BlockSpec(memory_space=pltpu.VMEM)
    sm = pl.BlockSpec(memory_space=pltpu.SMEM)
    hbm = pl.BlockSpec(memory_space=pltpu.HBM)

    def device_step(hidden, ln_gain, ln_shift, w_qkv, b_qkv, w_out, b_out, w_up, b_up, w_down, b_down, k_cache, v_cache, write_slot, key_pos, key_valid):
        n_layers, n_batch, cache_len, n_local, head_dim = k_cache.shape
        width = hidden.shape[-1]
        n_cols = cache_len * n_local
        flat = (n_layers, n_batch, n_cols, head_dim)
        in_hbm = functools.partial(pltpu.with_memory_space_constraint, memory_space=pltpu.HBM)
        k_in, v_in = in_hbm(k_cache.reshape(flat)), in_hbm(v_cache.reshape(flat))
        w_qkv, w_out, w_up, w_down = map(in_hbm, (w_qkv, w_out, w_up, w_down))
        x0 = hidden.reshape(n_batch, width)
        n_groups = n_batch // GROUP
        blk = n_batch // tp_size
        n_chip = tp_size // 2
        shape = jax.ShapeDtypeStruct(flat, BF16)
        held = pltpu.VMEM(flat, BF16)
        shared = [in_hbm(a) for a in (write_slot, key_pos, key_valid)]

        def attn(layer, x_in, caches):
            first = layer == 0
            n_qkv = b_qkv.shape[1]
            scratch = [
                pltpu.VMEM(key_pos.shape, jnp.int32),
                pltpu.VMEM(key_valid.shape, jnp.int32),
                pltpu.SMEM(write_slot.shape, jnp.int32),
                pltpu.VMEM(w_out.shape[1:], BF16),
                pltpu.VMEM((2, n_batch, n_cols), F32),
                pltpu.VMEM((n_batch, n_local * head_dim), F32),
                pltpu.SemaphoreType.DMA((5,)),
                pltpu.SemaphoreType.DMA((7,)),
                pltpu.SemaphoreType.DMA((4,)),
            ]
            alias = {}
            part = jax.ShapeDtypeStruct((n_batch, width), F32)
            outs, out_specs = (part, shape, shape, held, held), (vm, hbm, hbm, vm, vm)
            if first:
                ins = [in_hbm(a) for a in (x_in, ln_gain, ln_shift, b_qkv)] + [w_qkv, w_out] + shared + [k_in, v_in]
                specs = [hbm] * len(ins)
                scratch += [
                    pltpu.VMEM(x_in.shape, BF16),
                    pltpu.VMEM(ln_gain.shape, BF16),
                    pltpu.VMEM(ln_shift.shape, BF16),
                    pltpu.VMEM(b_qkv.shape, BF16),
                    pltpu.VMEM(w_qkv.shape[1:], BF16),
                    pltpu.VMEM((n_batch, n_qkv), F32),
                    pltpu.SemaphoreType.DMA((2, n_groups)),
                ]
            else:
                ins = [x_in, w_out] + shared + list(caches)
                specs = [vm, hbm] + [hbm] * len(shared) + [hbm] * 2 + [vm] * 2
                alias = {len(ins) - 4 + i: 1 + i for i in range(4)}
            return pl.pallas_call(
                functools.partial(attn_kernel, layer, n_local * tp_size, first),
                out_shape=outs,
                in_specs=specs,
                out_specs=out_specs,
                scratch_shapes=scratch,
                input_output_aliases=alias,
                compiler_params=pltpu.CompilerParams(vmem_limit_bytes=13 * MIB),
                name=f'attn_{layer}',
            )(*ins)

        def reduce(layer, part, res, caches=()):
            last = layer == n_layers - 1
            ins = [part, res, ln_gain, ln_shift, b_out, w_up, b_up, w_down, b_down]
            specs = [vm, vm, vm, vm, vm, hbm, vm, hbm, vm]
            outs = [jax.ShapeDtypeStruct((n_batch, width), BF16)]
            if not last:
                ins += [k_in, v_in, w_qkv, b_qkv, *caches]
                specs += [hbm, hbm, hbm, vm, vm, vm]
                outs = [jax.ShapeDtypeStruct((n_batch, b_qkv.shape[1]), F32)]
                outs += [jax.ShapeDtypeStruct((blk, width), BF16), held, held]
            dma = pltpu.SemaphoreType.DMA((2, n_chip))
            return pl.pallas_call(
                functools.partial(reduce_kernel, layer, tp_size, last),
                out_shape=tuple(outs),
                in_specs=specs,
                out_specs=tuple([vm] * len(outs)),
                scratch_shapes=[
                    pltpu.VMEM(w_up.shape[1:], BF16),
                    pltpu.VMEM(w_down.shape[1:], BF16),
                    pltpu.VMEM((n_batch, width), F32),
                    pltpu.VMEM((2, n_chip, blk, width), F32),
                    pltpu.VMEM((2, n_chip, blk, width), F32),
                    pltpu.VMEM((2, n_chip, blk, width), F32),
                    pltpu.VMEM((2, n_chip, blk, width), BF16),
                    pltpu.VMEM((2, n_chip, blk, width), BF16),
                    pltpu.SemaphoreType.DMA((6,)),
                ] + [dma] * 8,
                input_output_aliases={} if last else {len(ins) - 2: 2, len(ins) - 1: 3},
                compiler_params=pltpu.CompilerParams(vmem_limit_bytes=13 * MIB, collective_id=layer, has_side_effects=True),
                name=f'reduce_{layer}',
            )(*ins)

        part, k_new, v_new, k_held, v_held = attn(0, x0, None)
        qkv, x1, k_held, v_held = reduce(0, part, x0, (k_held, v_held))
        part, k_new, v_new, _, _ = attn(1, qkv, (k_new, v_new, k_held, v_held))
        (x_last,) = reduce(1, part, x1)
        return x_last[:, None, :], k_new.reshape(k_cache.shape), v_new.reshape(v_cache.shape)

    cache_spec = P(None, 'dp', None, 'tp', None)
    in_specs = (P('dp', None, None), P(), P(), P(None, None, 'tp'), P(None, 'tp'), P(None, 'tp', None), P(), P(None, None, 'tp'), P(None, 'tp'), P(None, 'tp', None), P(), cache_spec, cache_spec, P('dp'), P('dp', None), P('dp', None))
    out_specs = (P('dp', None, None), cache_spec, cache_spec)
    return jax.shard_map(device_step, mesh=mesh, in_specs=in_specs, out_specs=out_specs, check_vma=False)
```

```python
import functools
import math

import jax
import jax.numpy as jnp
from jax import lax
from jax.experimental import pallas as pl
from jax.experimental.pallas import tpu as pltpu
from jax.sharding import PartitionSpec as P

LN_EPS = 1e-5
MESH = pl.DeviceIdType.MESH
F32 = jnp.float32
BF16 = jnp.bfloat16
GROUP = 8
AHEAD = 6
SUB = 2
EARLY = 4
MIB = 2 ** 20


def layer_norm_f32(x_f32, gain, shift):
    mean_val = jnp.mean(x_f32, axis=-1, keepdims=True)
    centered = x_f32 - mean_val
    var_val = jnp.mean(centered * centered, axis=-1, keepdims=True)
    normed = centered * lax.rsqrt(var_val + LN_EPS)
    return (normed * gain.astype(F32) + shift.astype(F32)).astype(BF16)


def attn_kernel(layer, n_heads, first, *refs):
    if first:
        (x_in_ref, gain_in, shift_in, bq_in, wq_hbm, wo_hbm, slot_hbm, pos_in, valid_in, k_hbm, v_hbm,
         part_ref, k_out, v_out, kall, vall,
         pos_ref, valid_ref, slot_smem, wo, bias, attn, sem_w, sem_s, sem_out,
         x_ref, gain_ref, shift_ref, bq_ref, wq, qkv, sem_in) = refs
        old = []
    else:
        (qkv, wo_hbm, slot_hbm, pos_in, valid_in, k_part, v_part, k_raw, v_raw,
         part_ref, k_out, v_out, kall, vall,
         pos_ref, valid_ref, slot_smem, wo, bias, attn, sem_w, sem_s, sem_out) = refs
    kbuf, vbuf = kall.at[layer], vall.at[layer]
    n_batch, n_cols, head_dim = kbuf.shape
    n_groups = n_batch // GROUP
    n_local = attn.shape[1] // head_dim
    cache_len = n_cols // n_local
    n_chunk = 4
    pairs = [(slot_hbm, slot_smem), (pos_in, pos_ref), (valid_in, valid_ref)]
    if first:
        pairs = [(x_in_ref, x_ref), (gain_in, gain_ref), (shift_in, shift_ref), (bq_in, bq_ref)] + pairs
    small = [pltpu.make_async_copy(src, dst, sem_s.at[i]) for i, (src, dst) in enumerate(pairs)]
    for c in small:
        c.start()
    wo_copy = pltpu.make_async_copy(wo_hbm.at[layer], wo, sem_w.at[n_chunk])
    if first:
        step = x_ref.shape[1] // n_chunk
        w_copies = [
            pltpu.make_async_copy(wq_hbm.at[layer, pl.ds(i * step, step)], wq.at[pl.ds(i * step, step)], sem_w.at[i])
            for i in range(n_chunk)
        ]
        for c in w_copies:
            c.start()

    def in_copy(which, g):
        src, dst = ((k_hbm, kbuf), (v_hbm, vbuf))[which]
        return pltpu.make_async_copy(src.at[layer, pl.ds(g * GROUP, GROUP)], dst.at[pl.ds(g * GROUP, GROUP)], sem_in.at[which, g])

    def out_copy(which, g):
        src, dst = ((kbuf, k_out), (vbuf, v_out))[which]
        return pltpu.make_async_copy(src.at[pl.ds(g * GROUP, GROUP)], dst.at[layer, pl.ds(g * GROUP, GROUP)], sem_out.at[which])

    if first:
        for g in range(AHEAD - n_chunk):
            in_copy(0, g).start()
            in_copy(1, g).start()
    else:
        wo_copy.start()
        old = [
            pltpu.make_async_copy(src.at[layer - 1, pl.ds(g * GROUP, GROUP)], dst.at[layer - 1, pl.ds(g * GROUP, GROUP)], sem_out.at[2 + i])
            for g in range(EARLY, n_groups) for i, (src, dst) in enumerate(((kall, k_out), (vall, v_out)))
        ]
        for c in old:
            c.start()

    t_row = lax.broadcasted_iota(jnp.int32, (cache_len, n_cols), 0)
    t_col = lax.broadcasted_iota(jnp.int32, (cache_len, n_cols), 1) // n_local
    spread = (t_row == t_col).astype(BF16)
    for c in small:
        c.wait()
    pos = jnp.dot(pos_ref[...].astype(F32).astype(BF16), spread, preferred_element_type=F32)
    valid = jnp.dot(valid_ref[...].astype(F32).astype(BF16), spread, preferred_element_type=F32)
    bias[0] = pos
    bias[1] = valid

    if first:
        x_in = layer_norm_f32(x_ref[...].astype(F32), gain_ref[layer, 0:1], shift_ref[layer, 0:1])
        acc = None
        for i in range(n_chunk):
            w_copies[i].wait()
            in_copy(0, AHEAD - n_chunk + i).start()
            in_copy(1, AHEAD - n_chunk + i).start()
            d = jnp.dot(x_in[:, i * step:(i + 1) * step], wq[i * step:(i + 1) * step], preferred_element_type=F32)
            acc = d if acc is None else acc + d
        qkv[...] = (acc + bq_ref[layer:layer + 1].astype(F32)).astype(BF16).astype(F32)

    scale = 1.0 / math.sqrt(head_dim)
    rows = n_local * GROUP
    head0 = lax.axis_index('tp') * n_local

    def update(g):
        base = pl.multiple_of(g * GROUP, GROUP)
        row16 = lax.broadcasted_iota(jnp.int32, (16, head_dim), 0)
        fresh = qkv[pl.ds(base, GROUP), :]
        row8 = lax.broadcasted_iota(jnp.int32, (GROUP, n_cols), 0)
        slots = jnp.zeros((GROUP, n_cols), jnp.int32)
        for b in range(GROUP):
            slot = slot_smem[g * GROUP + b]
            slots = jnp.where(row8 == b, slot, slots)
            first_row = slot * n_local
            start = pl.multiple_of((first_row // 16) * 16, 16)
            off = first_row - start
            for which, buf in ((1, kbuf), (2, vbuf)):
                block = buf[base + b, pl.ds(start, 16), :].astype(F32)
                for h in range(n_local):
                    new = fresh[b:b + 1, (3 * h + which) * head_dim:(3 * h + which + 1) * head_dim]
                    block = jnp.where(row16 == off + h, new, block)
                buf[base + b, pl.ds(start, 16), :] = block.astype(BF16)
        col = lax.broadcasted_iota(jnp.int32, (GROUP, n_cols), 1)
        allowed = jnp.logical_or(bias[1, pl.ds(base, GROUP)] > 0.5, col // n_local == slots)
        pos_g = bias[0, pl.ds(base, GROUP)]
        parts = []
        for h in range(n_local):
            num = (jnp.full((GROUP, n_cols), 1 + h, jnp.int32) + head0).astype(F32)
            slope = jnp.exp2(-8.0 * num / n_heads)
            parts.append(jnp.where(jnp.logical_and(allowed, col % n_local == h), slope * pos_g, -jnp.inf))
        queries = jnp.concatenate([fresh[:, 3 * h * head_dim:(3 * h + 1) * head_dim] for h in range(n_local)], axis=0)
        odd = lax.broadcasted_iota(jnp.int32, (rows, head_dim), 0) % 2 == 1
        q_pair = jnp.concatenate([jnp.where(odd, 0.0, queries), jnp.where(odd, queries, 0.0)], axis=1).astype(BF16)
        return base, q_pair, jnp.concatenate(parts, axis=0)

    def scores(base, q_pair, add):
        row_s = lax.broadcasted_iota(jnp.int32, (rows, n_cols), 0) % GROUP // 2
        s = None
        for b in range(0, GROUP, 2):
            keys = jnp.concatenate([kbuf[base + b], kbuf[base + b + 1]], axis=1)
            sb = lax.dot_general(q_pair, keys, (((1,), (1,)), ((), ())), preferred_element_type=F32)
            s = sb if s is None else jnp.where(row_s == b // 2, sb, s)
        return s * scale + add

    def softmax(s):
        top = jnp.max(s, axis=-1, keepdims=True)
        e = jnp.exp(s - top)
        return (e * (1.0 / jnp.sum(e, axis=-1, keepdims=True))).astype(BF16)

    def mix(base, p):
        row_o = lax.broadcasted_iota(jnp.int32, (rows, head_dim), 0) % GROUP
        o = None
        for b in range(0, GROUP, 2):
            values = jnp.concatenate([vbuf[base + b], vbuf[base + b + 1]], axis=1)
            ob = jnp.dot(p, values, preferred_element_type=F32)
            for i in range(2):
                oi = ob[:, i * head_dim:(i + 1) * head_dim]
                o = oi if o is None else jnp.where(row_o == b + i, oi, o)
        for h in range(n_local):
            attn[pl.ds(base, GROUP), h * head_dim:(h + 1) * head_dim] = o[h * GROUP:(h + 1) * GROUP]

    def groups(i, carry):
        todo = [i * SUB + j for j in range(SUB)]
        if first:
            for g in todo:
                in_copy(0, g).wait()
                in_copy(1, g).wait()

            @pl.when(todo[-1] + AHEAD < n_groups)
            def _():
                for g in todo:
                    in_copy(0, g + AHEAD).start()
                    in_copy(1, g + AHEAD).start()

            @pl.when(i == n_groups // SUB - 2)
            def _():
                wo_copy.start()

            @pl.when(i >= (n_groups - EARLY) // SUB)
            def _():
                for j in range(SUB):
                    g = i * SUB + j - (n_groups - EARLY)
                    out_copy(0, g).start()
                    out_copy(1, g).start()
        state = [update(g) for g in todo]
        probs = [scores(*st) for st in state]
        for (base, _, _), s in zip(state, probs):
            mix(base, softmax(s))
        if not first:
            for g in todo:
                out_copy(0, g).start()
                out_copy(1, g).start()
        return carry

    lax.fori_loop(0, n_groups // SUB, groups, 0)
    wo_copy.wait()
    part_ref[...] = jnp.dot(attn[...].astype(BF16), wo[...], preferred_element_type=F32)
    for c in old:
        c.wait()
    for g in range(EARLY if first else n_groups):
        out_copy(0, g).wait()
        out_copy(1, g).wait()


def reduce_kernel(layer, n_tp, last, *refs):
    (part_ref, res_ref, gain_ref, shift_ref, bo_ref, wu_hbm, bu_ref, wd_hbm, bd_ref) = refs[:9]
    if last:
        out_ref, rest = refs[9], refs[10:]
    else:
        (k_hbm, v_hbm, wq_hbm, bq_ref, k_raw, v_raw, out_ref, own_ref, kall, vall) = refs[9:19]
        rest = refs[19:]
    (wu, wd, part2, d2d, mid, got, gath, gath2, sem_w,
     pair_s, pair_r, chip_s, chip_r, ag_s, ag_r, agp_s, agp_r) = rest
    n_batch, width = part_ref.shape
    n_chip = n_tp // 2
    blk = n_batch // n_tp
    me = lax.axis_index('tp')
    x = me // 2
    c = me % 2
    partner = x * 2 + (1 - c)

    def chip(d):
        return lax.rem(x + d, n_chip)

    w_copies = [pltpu.make_async_copy(wu_hbm.at[layer], wu, sem_w.at[0]), pltpu.make_async_copy(wd_hbm.at[layer], wd, sem_w.at[1])]
    if not last:
        w_copies.append(pltpu.make_async_copy(k_hbm.at[layer + 1], kall.at[layer + 1], sem_w.at[2]))
        w_copies.append(pltpu.make_async_copy(v_hbm.at[layer + 1], vall.at[layer + 1], sem_w.at[3]))
        n_qkv = bq_ref.shape[1]
        wq = wu.at[:, pl.ds(0, n_qkv)]
        wq_copy = pltpu.make_async_copy(wq_hbm.at[layer + 1], wq, sem_w.at[4])
    barrier = pltpu.get_barrier_semaphore()
    peers = [partner] + [chip(d) * 2 + 1 - c for d in range(1, n_chip)]
    for peer in peers:
        pl.semaphore_signal(barrier, inc=1, device_id={'tp': peer}, device_id_type=MESH)
    for w in w_copies:
        w.start()
    pl.semaphore_wait(barrier, len(peers))

    sent = []
    order = [2, 1, 3, 0] if n_chip == 4 else list(range(1, n_chip)) + [0]

    def rows_of(core, d):
        return pl.ds(pl.multiple_of((core * n_chip + chip(d)) * blk, blk), blk)

    def reduce_scatter(phase, src):
        pair = {
            d: pltpu.make_async_remote_copy(
                src_ref=src.at[rows_of(1 - c, d)], dst_ref=d2d.at[phase, d], send_sem=pair_s.at[phase, d],
                recv_sem=pair_r.at[phase, d], device_id={'tp': partner}, device_id_type=MESH)
            for d in order
        }
        for d in order:
            pair[d].start()
        hops = {}
        for d in order:
            pair[d].wait_recv()
            mid[phase, d] = src[rows_of(c, d), :] + d2d[phase, d]
            hops[d] = pltpu.make_async_remote_copy(
                src_ref=mid.at[phase, d], dst_ref=got.at[phase, d], send_sem=chip_s.at[phase, d],
                recv_sem=chip_r.at[phase, d], device_id={'tp': chip(d) * 2 + 1 - c}, device_id_type=MESH)
            hops[d].start()
        acc = None
        for d in sorted(hops, key=lambda d: min(d, n_chip - d)):
            hops[d].wait_recv()
            acc = got[phase, d] if acc is None else acc + got[phase, d]
        sent.extend([*pair.values(), *hops.values()])
        return acc

    def all_gather(phase, buf, value):
        buf[1 - c, x] = value
        hops = {}
        for d in order[:-1]:
            hops[d] = pltpu.make_async_remote_copy(
                src_ref=buf.at[1 - c, x], dst_ref=buf.at[1 - c, x], send_sem=ag_s.at[phase, d], recv_sem=ag_r.at[phase, d],
                device_id={'tp': chip(d) * 2 + 1 - c}, device_id_type=MESH)
            hops[d].start()

        def pass_on(d):
            slot = lax.rem(x + n_chip - d, n_chip)
            half = 1 - c if d == 0 else c
            cp = pltpu.make_async_remote_copy(
                src_ref=buf.at[half, slot], dst_ref=buf.at[half, slot], send_sem=agp_s.at[phase, d], recv_sem=agp_r.at[phase, d],
                device_id={'tp': partner}, device_id_type=MESH)
            cp.start()
            return cp

        passed = [pass_on(0)]
        for d in sorted(hops, key=lambda d: min(d, n_chip - d)):
            hops[d].wait_recv()
            passed.append(pass_on(d))
        for cp in passed:
            cp.wait_recv()
        sent.extend([*passed, *hops.values()])
        return buf[...].astype(F32).reshape(n_batch, width)

    if last:
        res = res_ref[...].astype(F32)
    else:
        res = res_ref[rows_of(1 - c, 0), :].astype(F32)
    total = reduce_scatter(0, part_ref)
    x_mid = (res + total + bo_ref[layer:layer + 1].astype(F32)).astype(BF16).astype(F32)
    normed = all_gather(0, gath, layer_norm_f32(x_mid, gain_ref[layer, 1:2], shift_ref[layer, 1:2])).astype(BF16)
    w_copies[0].wait()
    up = jnp.dot(normed, wu[...], preferred_element_type=F32) + bu_ref[layer:layer + 1].astype(F32)
    act = jax.nn.gelu(up, approximate=True).astype(BF16)
    if not last:
        wq_copy.start()
    w_copies[1].wait()
    part2[...] = jnp.dot(act, wd[...], preferred_element_type=F32)
    total = reduce_scatter(1, part2)
    x_next = (x_mid + total + bd_ref[layer:layer + 1].astype(F32)).astype(BF16)
    if last:
        out_ref[...] = all_gather(1, gath2, x_next).astype(BF16)
    else:
        own_ref[...] = x_next
        nxt = layer_norm_f32(x_next.astype(F32), gain_ref[layer + 1, 0:1], shift_ref[layer + 1, 0:1])
        normed = all_gather(1, gath2, nxt).astype(BF16)
        wq_copy.wait()
        qkv = jnp.dot(normed, wu[:, :n_qkv], preferred_element_type=F32) + bq_ref[layer + 1:layer + 2].astype(F32)
        out_ref[...] = qkv.astype(BF16).astype(F32)
        for w in w_copies[2:]:
            w.wait()
    for cp in sent:
        cp.wait_send()


def solution(mesh):
    tp_size = mesh.shape['tp']
    vm = pl.BlockSpec(memory_space=pltpu.VMEM)
    sm = pl.BlockSpec(memory_space=pltpu.SMEM)
    hbm = pl.BlockSpec(memory_space=pltpu.HBM)

    def device_step(hidden, ln_gain, ln_shift, w_qkv, b_qkv, w_out, b_out, w_up, b_up, w_down, b_down, k_cache, v_cache, write_slot, key_pos, key_valid):
        n_layers, n_batch, cache_len, n_local, head_dim = k_cache.shape
        width = hidden.shape[-1]
        n_cols = cache_len * n_local
        flat = (n_layers, n_batch, n_cols, head_dim)
        in_hbm = functools.partial(pltpu.with_memory_space_constraint, memory_space=pltpu.HBM)
        k_in, v_in = in_hbm(k_cache.reshape(flat)), in_hbm(v_cache.reshape(flat))
        w_qkv, w_out, w_up, w_down = map(in_hbm, (w_qkv, w_out, w_up, w_down))
        x0 = hidden.reshape(n_batch, width)
        n_groups = n_batch // GROUP
        blk = n_batch // tp_size
        n_chip = tp_size // 2
        shape = jax.ShapeDtypeStruct(flat, BF16)
        held = pltpu.VMEM(flat, BF16)
        shared = [in_hbm(a) for a in (write_slot, key_pos, key_valid)]

        def attn(layer, x_in, caches):
            first = layer == 0
            n_qkv = b_qkv.shape[1]
            scratch = [
                pltpu.VMEM(key_pos.shape, jnp.int32),
                pltpu.VMEM(key_valid.shape, jnp.int32),
                pltpu.SMEM(write_slot.shape, jnp.int32),
                pltpu.VMEM(w_out.shape[1:], BF16),
                pltpu.VMEM((2, n_batch, n_cols), F32),
                pltpu.VMEM((n_batch, n_local * head_dim), F32),
                pltpu.SemaphoreType.DMA((5,)),
                pltpu.SemaphoreType.DMA((7,)),
                pltpu.SemaphoreType.DMA((4,)),
            ]
            alias = {}
            part = jax.ShapeDtypeStruct((n_batch, width), F32)
            outs, out_specs = (part, shape, shape, held, held), (vm, hbm, hbm, vm, vm)
            if first:
                ins = [in_hbm(a) for a in (x_in, ln_gain, ln_shift, b_qkv)] + [w_qkv, w_out] + shared + [k_in, v_in]
                specs = [hbm] * len(ins)
                scratch += [
                    pltpu.VMEM(x_in.shape, BF16),
                    pltpu.VMEM(ln_gain.shape, BF16),
                    pltpu.VMEM(ln_shift.shape, BF16),
                    pltpu.VMEM(b_qkv.shape, BF16),
                    pltpu.VMEM(w_qkv.shape[1:], BF16),
                    pltpu.VMEM((n_batch, n_qkv), F32),
                    pltpu.SemaphoreType.DMA((2, n_groups)),
                ]
            else:
                ins = [x_in, w_out] + shared + list(caches)
                specs = [vm, hbm] + [hbm] * len(shared) + [hbm] * 2 + [vm] * 2
                alias = {len(ins) - 4 + i: 1 + i for i in range(4)}
            return pl.pallas_call(
                functools.partial(attn_kernel, layer, n_local * tp_size, first),
                out_shape=outs,
                in_specs=specs,
                out_specs=out_specs,
                scratch_shapes=scratch,
                input_output_aliases=alias,
                compiler_params=pltpu.CompilerParams(vmem_limit_bytes=13 * MIB),
                name=f'attn_{layer}',
            )(*ins)

        def reduce(layer, part, res, caches=()):
            last = layer == n_layers - 1
            ins = [part, res, ln_gain, ln_shift, b_out, w_up, b_up, w_down, b_down]
            specs = [vm, vm, vm, vm, vm, hbm, vm, hbm, vm]
            outs = [jax.ShapeDtypeStruct((n_batch, width), BF16)]
            if not last:
                ins += [k_in, v_in, w_qkv, b_qkv, *caches]
                specs += [hbm, hbm, hbm, vm, vm, vm]
                outs = [jax.ShapeDtypeStruct((n_batch, b_qkv.shape[1]), F32)]
                outs += [jax.ShapeDtypeStruct((blk, width), BF16), held, held]
            dma = pltpu.SemaphoreType.DMA((2, n_chip))
            return pl.pallas_call(
                functools.partial(reduce_kernel, layer, tp_size, last),
                out_shape=tuple(outs),
                in_specs=specs,
                out_specs=tuple([vm] * len(outs)),
                scratch_shapes=[
                    pltpu.VMEM(w_up.shape[1:], BF16),
                    pltpu.VMEM(w_down.shape[1:], BF16),
                    pltpu.VMEM((n_batch, width), F32),
                    pltpu.VMEM((2, n_chip, blk, width), F32),
                    pltpu.VMEM((2, n_chip, blk, width), F32),
                    pltpu.VMEM((2, n_chip, blk, width), F32),
                    pltpu.VMEM((2, n_chip, blk, width), BF16),
                    pltpu.VMEM((2, n_chip, blk, width), BF16),
                    pltpu.SemaphoreType.DMA((6,)),
                ] + [dma] * 8,
                input_output_aliases={} if last else {len(ins) - 2: 2, len(ins) - 1: 3},
                compiler_params=pltpu.CompilerParams(vmem_limit_bytes=13 * MIB, collective_id=layer, has_side_effects=True),
                name=f'reduce_{layer}',
            )(*ins)

        part, k_new, v_new, k_held, v_held = attn(0, x0, None)
        qkv, x1, k_held, v_held = reduce(0, part, x0, (k_held, v_held))
        part, k_new, v_new, _, _ = attn(1, qkv, (k_new, v_new, k_held, v_held))
        (x_last,) = reduce(1, part, x1)
        return x_last[:, None, :], k_new.reshape(k_cache.shape), v_new.reshape(v_cache.shape)

    cache_spec = P(None, 'dp', None, 'tp', None)
    in_specs = (P('dp', None, None), P(), P(), P(None, None, 'tp'), P(None, 'tp'), P(None, 'tp', None), P(), P(None, None, 'tp'), P(None, 'tp'), P(None, 'tp', None), P(), cache_spec, cache_spec, P('dp'), P('dp', None), P('dp', None))
    out_specs = (P('dp', None, None), cache_spec, cache_spec)
    return jax.shard_map(device_step, mesh=mesh, in_specs=in_specs, out_specs=out_specs, check_vma=False)
```

```python
import functools
import math

import jax
import jax.numpy as jnp
from jax import lax
from jax.experimental import pallas as pl
from jax.experimental.pallas import tpu as pltpu
from jax.sharding import PartitionSpec as P

LN_EPS = 1e-5
MESH = pl.DeviceIdType.MESH
F32 = jnp.float32
BF16 = jnp.bfloat16
GROUP = 8
AHEAD = 6
SUB = 2
EARLY = 4
MIB = 2 ** 20


def layer_norm_f32(x_f32, gain, shift):
    mean_val = jnp.mean(x_f32, axis=-1, keepdims=True)
    centered = x_f32 - mean_val
    var_val = jnp.mean(centered * centered, axis=-1, keepdims=True)
    normed = centered * lax.rsqrt(var_val + LN_EPS)
    return (normed * gain.astype(F32) + shift.astype(F32)).astype(BF16)


def attn_kernel(layer, n_heads, first, *refs):
    if first:
        (x_in_ref, gain_in, shift_in, bq_in, wq_hbm, wo_hbm, slot_hbm, pos_in, valid_in, k_hbm, v_hbm,
         part_ref, k_out, v_out, kall, vall,
         pos_ref, valid_ref, slot_smem, wo, bias, attn, sem_w, sem_s, sem_out,
         x_ref, gain_ref, shift_ref, bq_ref, wq, qkv, sem_in) = refs
        old = []
    else:
        (qkv, wo_hbm, slot_hbm, pos_in, valid_in, k_part, v_part, k_raw, v_raw,
         part_ref, k_out, v_out, kall, vall,
         pos_ref, valid_ref, slot_smem, wo, bias, attn, sem_w, sem_s, sem_out) = refs
    kbuf, vbuf = kall.at[layer], vall.at[layer]
    n_batch, n_cols, head_dim = kbuf.shape
    n_groups = n_batch // GROUP
    n_local = attn.shape[1] // head_dim
    cache_len = n_cols // n_local
    n_chunk = 4
    pairs = [(slot_hbm, slot_smem), (pos_in, pos_ref), (valid_in, valid_ref)]
    if first:
        pairs = [(x_in_ref, x_ref), (gain_in, gain_ref), (shift_in, shift_ref), (bq_in, bq_ref)] + pairs
    small = [pltpu.make_async_copy(src, dst, sem_s.at[i]) for i, (src, dst) in enumerate(pairs)]
    for c in small:
        c.start()
    wo_copy = pltpu.make_async_copy(wo_hbm.at[layer], wo, sem_w.at[n_chunk])
    if first:
        step = x_ref.shape[1] // n_chunk
        w_copies = [
            pltpu.make_async_copy(wq_hbm.at[layer, pl.ds(i * step, step)], wq.at[pl.ds(i * step, step)], sem_w.at[i])
            for i in range(n_chunk)
        ]
        for c in w_copies:
            c.start()

    def in_copy(which, g):
        src, dst = ((k_hbm, kbuf), (v_hbm, vbuf))[which]
        return pltpu.make_async_copy(src.at[layer, pl.ds(g * GROUP, GROUP)], dst.at[pl.ds(g * GROUP, GROUP)], sem_in.at[which, g])

    def out_copy(which, g):
        src, dst = ((kbuf, k_out), (vbuf, v_out))[which]
        return pltpu.make_async_copy(src.at[pl.ds(g * GROUP, GROUP)], dst.at[layer, pl.ds(g * GROUP, GROUP)], sem_out.at[which])

    if first:
        for g in range(AHEAD - n_chunk):
            in_copy(0, g).start()
            in_copy(1, g).start()
    else:
        wo_copy.start()
        old = [
            pltpu.make_async_copy(src.at[layer - 1, pl.ds(g * GROUP, GROUP)], dst.at[layer - 1, pl.ds(g * GROUP, GROUP)], sem_out.at[2 + i])
            for g in range(EARLY, n_groups) for i, (src, dst) in enumerate(((kall, k_out), (vall, v_out)))
        ]
        for c in old:
            c.start()

    t_row = lax.broadcasted_iota(jnp.int32, (cache_len, n_cols), 0)
    t_col = lax.broadcasted_iota(jnp.int32, (cache_len, n_cols), 1) // n_local
    spread = (t_row == t_col).astype(BF16)
    for c in small:
        c.wait()
    pos = jnp.dot(pos_ref[...].astype(F32).astype(BF16), spread, preferred_element_type=F32)
    valid = jnp.dot(valid_ref[...].astype(F32).astype(BF16), spread, preferred_element_type=F32)
    bias[0] = pos
    bias[1] = valid

    if first:
        x_in = layer_norm_f32(x_ref[...].astype(F32), gain_ref[layer, 0:1], shift_ref[layer, 0:1])
        acc = None
        for i in range(n_chunk):
            w_copies[i].wait()
            in_copy(0, AHEAD - n_chunk + i).start()
            in_copy(1, AHEAD - n_chunk + i).start()
            d = jnp.dot(x_in[:, i * step:(i + 1) * step], wq[i * step:(i + 1) * step], preferred_element_type=F32)
            acc = d if acc is None else acc + d
        qkv[...] = (acc + bq_ref[layer:layer + 1].astype(F32)).astype(BF16).astype(F32)

    scale = 1.0 / math.sqrt(head_dim)
    rows = n_local * GROUP
    head0 = lax.axis_index('tp') * n_local

    def update(g):
        base = pl.multiple_of(g * GROUP, GROUP)
        row16 = lax.broadcasted_iota(jnp.int32, (16, head_dim), 0)
        fresh = qkv[pl.ds(base, GROUP), :]
        row8 = lax.broadcasted_iota(jnp.int32, (GROUP, n_cols), 0)
        slots = jnp.zeros((GROUP, n_cols), jnp.int32)
        for b in range(GROUP):
            slot = slot_smem[g * GROUP + b]
            slots = jnp.where(row8 == b, slot, slots)
            first_row = slot * n_local
            start = pl.multiple_of((first_row // 16) * 16, 16)
            off = first_row - start
            for which, buf in ((1, kbuf), (2, vbuf)):
                block = buf[base + b, pl.ds(start, 16), :].astype(F32)
                for h in range(n_local):
                    new = fresh[b:b + 1, (3 * h + which) * head_dim:(3 * h + which + 1) * head_dim]
                    block = jnp.where(row16 == off + h, new, block)
                buf[base + b, pl.ds(start, 16), :] = block.astype(BF16)
        col = lax.broadcasted_iota(jnp.int32, (GROUP, n_cols), 1)
        allowed = jnp.logical_or(bias[1, pl.ds(base, GROUP)] > 0.5, col // n_local == slots)
        pos_g = bias[0, pl.ds(base, GROUP)]
        parts = []
        for h in range(n_local):
            num = (jnp.full((GROUP, n_cols), 1 + h, jnp.int32) + head0).astype(F32)
            slope = jnp.exp2(-8.0 * num / n_heads)
            parts.append(jnp.where(jnp.logical_and(allowed, col % n_local == h), slope * pos_g, -jnp.inf))
        queries = jnp.concatenate([fresh[:, 3 * h * head_dim:(3 * h + 1) * head_dim] for h in range(n_local)], axis=0)
        odd = lax.broadcasted_iota(jnp.int32, (rows, head_dim), 0) % 2 == 1
        q_pair = jnp.concatenate([jnp.where(odd, 0.0, queries), jnp.where(odd, queries, 0.0)], axis=1).astype(BF16)
        return base, q_pair, jnp.concatenate(parts, axis=0)

    def scores(base, q_pair, add):
        row_s = lax.broadcasted_iota(jnp.int32, (rows, n_cols), 0) % GROUP // 2
        s = None
        for b in range(0, GROUP, 2):
            keys = jnp.concatenate([kbuf[base + b], kbuf[base + b + 1]], axis=1)
            sb = lax.dot_general(q_pair, keys, (((1,), (1,)), ((), ())), preferred_element_type=F32)
            s = sb if s is None else jnp.where(row_s == b // 2, sb, s)
        return s * scale + add

    def softmax(s):
        top = jnp.max(s, axis=-1, keepdims=True)
        e = jnp.exp(s - top)
        return (e * (1.0 / jnp.sum(e, axis=-1, keepdims=True))).astype(BF16)

    def mix(base, p):
        row_o = lax.broadcasted_iota(jnp.int32, (rows, head_dim), 0) % GROUP
        o = None
        for b in range(0, GROUP, 2):
            values = jnp.concatenate([vbuf[base + b], vbuf[base + b + 1]], axis=1)
            ob = jnp.dot(p, values, preferred_element_type=F32)
            for i in range(2):
                oi = ob[:, i * head_dim:(i + 1) * head_dim]
                o = oi if o is None else jnp.where(row_o == b + i, oi, o)
        for h in range(n_local):
            attn[pl.ds(base, GROUP), h * head_dim:(h + 1) * head_dim] = o[h * GROUP:(h + 1) * GROUP]

    def groups(i, carry):
        todo = [i * SUB + j for j in range(SUB)]
        if first:
            for g in todo:
                in_copy(0, g).wait()
                in_copy(1, g).wait()

            @pl.when(todo[-1] + AHEAD < n_groups)
            def _():
                for g in todo:
                    in_copy(0, g + AHEAD).start()
                    in_copy(1, g + AHEAD).start()

            @pl.when(i == n_groups // SUB - 2)
            def _():
                wo_copy.start()

            @pl.when(i >= (n_groups - EARLY) // SUB)
            def _():
                for j in range(SUB):
                    g = i * SUB + j - (n_groups - EARLY)
                    out_copy(0, g).start()
                    out_copy(1, g).start()
        state = [update(g) for g in todo]
        probs = [scores(*st) for st in state]
        for (base, _, _), s in zip(state, probs):
            mix(base, softmax(s))
        if not first:
            for g in todo:
                out_copy(0, g).start()
                out_copy(1, g).start()
        return carry

    lax.fori_loop(0, n_groups // SUB, groups, 0)
    wo_copy.wait()
    part_ref[...] = jnp.dot(attn[...].astype(BF16), wo[...], preferred_element_type=F32)
    for c in old:
        c.wait()
    for g in range(EARLY if first else n_groups):
        out_copy(0, g).wait()
        out_copy(1, g).wait()


def reduce_kernel(layer, n_tp, last, *refs):
    (part_ref, res_ref, gain_ref, shift_ref, bo_ref, wu_hbm, bu_ref, wd_hbm, bd_ref) = refs[:9]
    if last:
        out_ref, rest = refs[9], refs[10:]
    else:
        (k_hbm, v_hbm, wq_hbm, bq_ref, k_raw, v_raw, out_ref, own_ref, kall, vall) = refs[9:19]
        rest = refs[19:]
    (wu, wd, part2, d2d, mid, got, gath, gath2, sem_w,
     pair_s, pair_r, chip_s, chip_r, ag_s, ag_r, agp_s, agp_r) = rest
    n_batch, width = part_ref.shape
    n_chip = n_tp // 2
    blk = n_batch // n_tp
    me = lax.axis_index('tp')
    x = me // 2
    c = me % 2
    partner = x * 2 + (1 - c)

    def chip(d):
        return lax.rem(x + d, n_chip)

    w_copies = [pltpu.make_async_copy(wu_hbm.at[layer], wu, sem_w.at[0]), pltpu.make_async_copy(wd_hbm.at[layer], wd, sem_w.at[1])]
    if not last:
        w_copies.append(pltpu.make_async_copy(k_hbm.at[layer + 1], kall.at[layer + 1], sem_w.at[2]))
        w_copies.append(pltpu.make_async_copy(v_hbm.at[layer + 1], vall.at[layer + 1], sem_w.at[3]))
        n_qkv = bq_ref.shape[1]
        wq = wu.at[:, pl.ds(0, n_qkv)]
        wq_copy = pltpu.make_async_copy(wq_hbm.at[layer + 1], wq, sem_w.at[4])
    barrier = pltpu.get_barrier_semaphore()
    peers = [partner] + [chip(d) * 2 + 1 - c for d in range(1, n_chip)]
    for peer in peers:
        pl.semaphore_signal(barrier, inc=1, device_id={'tp': peer}, device_id_type=MESH)
    for w in w_copies[:2]:
        w.start()
    pl.semaphore_wait(barrier, len(peers))

    sent = []
    order = [2, 1, 3, 0] if n_chip == 4 else list(range(1, n_chip)) + [0]

    def rows_of(core, d):
        return pl.ds(pl.multiple_of((core * n_chip + chip(d)) * blk, blk), blk)

    far = order[:-1]
    by_distance = sorted(order, key=lambda d: min(d, n_chip - d))

    def remote(src, dst, send_sem, recv_sem, to):
        return pltpu.make_async_remote_copy(src_ref=src, dst_ref=dst, send_sem=send_sem, recv_sem=recv_sem, device_id={'tp': to}, device_id_type=MESH)

    def reduce_scatter(phase, src, fills):
        part = width // len(fills)
        pair, hops = [], []
        for k, fill in enumerate(fills):
            sem, cols = phase + k, pl.ds(k * part, part)
            if fill is not None:
                fill(k * part, part)
            pair.append({
                d: remote(src.at[rows_of(1 - c, d), cols], d2d.at[phase, d, :, cols], pair_s.at[sem, d], pair_r.at[sem, d], partner)
                for d in order
            })
            for d in order:
                pair[k][d].start()
        for k in range(len(fills)):
            sem, cols = phase + k, pl.ds(k * part, part)
            hops.append({})
            for d in order:
                pair[k][d].wait_recv()
                mid[phase, d, :, cols] = src[rows_of(c, d), cols] + d2d[phase, d, :, cols]
                hops[k][d] = remote(mid.at[phase, d, :, cols], got.at[phase, d, :, cols], chip_s.at[sem, d], chip_r.at[sem, d], chip(d) * 2 + 1 - c)
                hops[k][d].start()
        sums = []
        for k in range(len(fills)):
            acc = None
            for d in by_distance:
                hops[k][d].wait_recv()
                term = got[phase, d, :, pl.ds(k * part, part)]
                acc = term if acc is None else acc + term
            sums.append(acc)
            sent.extend([*pair[k].values(), *hops[k].values()])
        return sums[0] if len(sums) == 1 else jnp.concatenate(sums, axis=1)

    def all_gather(phase, buf, value, parts, consume):
        buf[1 - c, x] = value
        part = width // parts

        def pass_on(k, d):
            slot = lax.rem(x + n_chip - d, n_chip)
            ref = buf.at[c if d else 1 - c, slot, :, pl.ds(k * part, part)]
            return remote(ref, ref, agp_s.at[phase + k, d], agp_r.at[phase + k, d], partner)

        hops, passed = [], []
        for k in range(parts):
            ref = buf.at[1 - c, x, :, pl.ds(k * part, part)]
            hops.append({d: remote(ref, ref, ag_s.at[phase + k, d], ag_r.at[phase + k, d], chip(d) * 2 + 1 - c) for d in far})
            for d in far:
                hops[k][d].start()
            passed.append([pass_on(k, 0)])
            passed[k][0].start()
        for k in range(parts):
            for d in by_distance[1:]:
                hops[k][d].wait_recv()
                passed[k].append(pass_on(k, d))
                passed[k][-1].start()
        out = None
        for k in range(parts):
            for cp in passed[k]:
                cp.wait_recv()
            rows = buf[:, :, :, k * part:(k + 1) * part].astype(F32).reshape(n_batch, part).astype(BF16)
            term = consume(k * part, part, rows)
            out = term if out is None else out + term
            sent.extend([*passed[k], *hops[k].values()])
        return out

    def product(ref, n_cols):
        return lambda lo, size, rows: jnp.dot(rows, ref[lo:lo + size, :n_cols], preferred_element_type=F32)

    if last:
        res = res_ref[...].astype(F32)
    else:
        res = res_ref[rows_of(1 - c, 0), :].astype(F32)
    total = reduce_scatter(0, part_ref, [None])
    for w in w_copies[2:]:
        w.start()
    x_mid = (res + total + bo_ref[layer:layer + 1].astype(F32)).astype(BF16).astype(F32)
    w_copies[0].wait()
    normed = layer_norm_f32(x_mid, gain_ref[layer, 1:2], shift_ref[layer, 1:2])
    up = all_gather(0, gath, normed, 2, product(wu, wu.shape[1])) + bu_ref[layer:layer + 1].astype(F32)
    act = jax.nn.gelu(up, approximate=True).astype(BF16)
    if not last:
        wq_copy.start()
    w_copies[1].wait()

    def down(lo, size):
        part2[:, lo:lo + size] = jnp.dot(act, wd[:, lo:lo + size], preferred_element_type=F32)

    total = reduce_scatter(1, part2, [down, down])
    x_next = (x_mid + total + bd_ref[layer:layer + 1].astype(F32)).astype(BF16)
    if last:
        out_ref[...] = all_gather(2, gath2, x_next, 1, lambda lo, size, rows: rows)
    else:
        own_ref[...] = x_next
        nxt = layer_norm_f32(x_next.astype(F32), gain_ref[layer + 1, 0:1], shift_ref[layer + 1, 0:1])
        wq_copy.wait()
        qkv = all_gather(2, gath2, nxt, 2, product(wu, n_qkv)) + bq_ref[layer + 1:layer + 2].astype(F32)
        out_ref[...] = qkv.astype(BF16).astype(F32)
        for w in w_copies[2:]:
            w.wait()
    for cp in sent:
        cp.wait_send()


def solution(mesh):
    tp_size = mesh.shape['tp']
    vm = pl.BlockSpec(memory_space=pltpu.VMEM)
    sm = pl.BlockSpec(memory_space=pltpu.SMEM)
    hbm = pl.BlockSpec(memory_space=pltpu.HBM)

    def device_step(hidden, ln_gain, ln_shift, w_qkv, b_qkv, w_out, b_out, w_up, b_up, w_down, b_down, k_cache, v_cache, write_slot, key_pos, key_valid):
        n_layers, n_batch, cache_len, n_local, head_dim = k_cache.shape
        width = hidden.shape[-1]
        n_cols = cache_len * n_local
        flat = (n_layers, n_batch, n_cols, head_dim)
        in_hbm = functools.partial(pltpu.with_memory_space_constraint, memory_space=pltpu.HBM)
        k_in, v_in = in_hbm(k_cache.reshape(flat)), in_hbm(v_cache.reshape(flat))
        w_qkv, w_out, w_up, w_down = map(in_hbm, (w_qkv, w_out, w_up, w_down))
        x0 = hidden.reshape(n_batch, width)
        n_groups = n_batch // GROUP
        blk = n_batch // tp_size
        n_chip = tp_size // 2
        shape = jax.ShapeDtypeStruct(flat, BF16)
        held = pltpu.VMEM(flat, BF16)
        shared = [in_hbm(a) for a in (write_slot, key_pos, key_valid)]

        def attn(layer, x_in, caches):
            first = layer == 0
            n_qkv = b_qkv.shape[1]
            scratch = [
                pltpu.VMEM(key_pos.shape, jnp.int32),
                pltpu.VMEM(key_valid.shape, jnp.int32),
                pltpu.SMEM(write_slot.shape, jnp.int32),
                pltpu.VMEM(w_out.shape[1:], BF16),
                pltpu.VMEM((2, n_batch, n_cols), F32),
                pltpu.VMEM((n_batch, n_local * head_dim), F32),
                pltpu.SemaphoreType.DMA((5,)),
                pltpu.SemaphoreType.DMA((7,)),
                pltpu.SemaphoreType.DMA((4,)),
            ]
            alias = {}
            part = jax.ShapeDtypeStruct((n_batch, width), F32)
            outs, out_specs = (part, shape, shape, held, held), (vm, hbm, hbm, vm, vm)
            if first:
                ins = [in_hbm(a) for a in (x_in, ln_gain, ln_shift, b_qkv)] + [w_qkv, w_out] + shared + [k_in, v_in]
                specs = [hbm] * len(ins)
                scratch += [
                    pltpu.VMEM(x_in.shape, BF16),
                    pltpu.VMEM(ln_gain.shape, BF16),
                    pltpu.VMEM(ln_shift.shape, BF16),
                    pltpu.VMEM(b_qkv.shape, BF16),
                    pltpu.VMEM(w_qkv.shape[1:], BF16),
                    pltpu.VMEM((n_batch, n_qkv), F32),
                    pltpu.SemaphoreType.DMA((2, n_groups)),
                ]
            else:
                ins = [x_in, w_out] + shared + list(caches)
                specs = [vm, hbm] + [hbm] * len(shared) + [hbm] * 2 + [vm] * 2
                alias = {len(ins) - 4 + i: 1 + i for i in range(4)}
            return pl.pallas_call(
                functools.partial(attn_kernel, layer, n_local * tp_size, first),
                out_shape=outs,
                in_specs=specs,
                out_specs=out_specs,
                scratch_shapes=scratch,
                input_output_aliases=alias,
                compiler_params=pltpu.CompilerParams(vmem_limit_bytes=13 * MIB),
                name=f'attn_{layer}',
            )(*ins)

        def reduce(layer, part, res, caches=()):
            last = layer == n_layers - 1
            ins = [part, res, ln_gain, ln_shift, b_out, w_up, b_up, w_down, b_down]
            specs = [vm, vm, vm, vm, vm, hbm, vm, hbm, vm]
            outs = [jax.ShapeDtypeStruct((n_batch, width), BF16)]
            if not last:
                ins += [k_in, v_in, w_qkv, b_qkv, *caches]
                specs += [hbm, hbm, hbm, vm, vm, vm]
                outs = [jax.ShapeDtypeStruct((n_batch, b_qkv.shape[1]), F32)]
                outs += [jax.ShapeDtypeStruct((blk, width), BF16), held, held]
            dma = pltpu.SemaphoreType.DMA((4, n_chip))
            return pl.pallas_call(
                functools.partial(reduce_kernel, layer, tp_size, last),
                out_shape=tuple(outs),
                in_specs=specs,
                out_specs=tuple([vm] * len(outs)),
                scratch_shapes=[
                    pltpu.VMEM(w_up.shape[1:], BF16),
                    pltpu.VMEM(w_down.shape[1:], BF16),
                    pltpu.VMEM((n_batch, width), F32),
                    pltpu.VMEM((2, n_chip, blk, width), F32),
                    pltpu.VMEM((2, n_chip, blk, width), F32),
                    pltpu.VMEM((2, n_chip, blk, width), F32),
                    pltpu.VMEM((2, n_chip, blk, width), BF16),
                    pltpu.VMEM((2, n_chip, blk, width), BF16),
                    pltpu.SemaphoreType.DMA((6,)),
                ] + [dma] * 8,
                input_output_aliases={} if last else {len(ins) - 2: 2, len(ins) - 1: 3},
                compiler_params=pltpu.CompilerParams(vmem_limit_bytes=13 * MIB, collective_id=layer, has_side_effects=True),
                name=f'reduce_{layer}',
            )(*ins)

        part, k_new, v_new, k_held, v_held = attn(0, x0, None)
        qkv, x1, k_held, v_held = reduce(0, part, x0, (k_held, v_held))
        part, k_new, v_new, _, _ = attn(1, qkv, (k_new, v_new, k_held, v_held))
        (x_last,) = reduce(1, part, x1)
        return x_last[:, None, :], k_new.reshape(k_cache.shape), v_new.reshape(v_cache.shape)

    cache_spec = P(None, 'dp', None, 'tp', None)
    in_specs = (P('dp', None, None), P(), P(), P(None, None, 'tp'), P(None, 'tp'), P(None, 'tp', None), P(), P(None, None, 'tp'), P(None, 'tp'), P(None, 'tp', None), P(), cache_spec, cache_spec, P('dp'), P('dp', None), P('dp', None))
    out_specs = (P('dp', None, None), cache_spec, cache_spec)
    return jax.shard_map(device_step, mesh=mesh, in_specs=in_specs, out_specs=out_specs, check_vma=False)
```

```python
import functools
import math

import jax
import jax.numpy as jnp
from jax import lax
from jax.experimental import pallas as pl
from jax.experimental.pallas import tpu as pltpu
from jax.sharding import PartitionSpec as P

LN_EPS = 1e-5
MESH = pl.DeviceIdType.MESH
F32 = jnp.float32
BF16 = jnp.bfloat16
GROUP = 8
AHEAD = 6
SUB = 2
EARLY = 4
MIB = 2 ** 20


def layer_norm_f32(x_f32, gain, shift):
    mean_val = jnp.mean(x_f32, axis=-1, keepdims=True)
    centered = x_f32 - mean_val
    var_val = jnp.mean(centered * centered, axis=-1, keepdims=True)
    normed = centered * lax.rsqrt(var_val + LN_EPS)
    return (normed * gain.astype(F32) + shift.astype(F32)).astype(BF16)


def attn_kernel(layer, n_heads, first, *refs):
    if first:
        (x_in_ref, gain_in, shift_in, bq_in, wq_hbm, wo_hbm, slot_hbm, pos_in, valid_in, k_hbm, v_hbm,
         part_ref, k_out, v_out, kall, vall,
         pos_ref, valid_ref, slot_smem, wo, bias, attn, sem_w, sem_s, sem_out,
         x_ref, gain_ref, shift_ref, bq_ref, wq, qkv, sem_in) = refs
        old = []
    else:
        (qkv, wo_hbm, slot_hbm, pos_in, valid_in, k_part, v_part, k_raw, v_raw,
         part_ref, k_out, v_out, kall, vall,
         pos_ref, valid_ref, slot_smem, wo, bias, attn, sem_w, sem_s, sem_out) = refs
    kbuf, vbuf = kall.at[layer], vall.at[layer]
    n_batch, n_cols, head_dim = kbuf.shape
    n_groups = n_batch // GROUP
    n_local = attn.shape[1] // head_dim
    cache_len = n_cols // n_local
    n_chunk = 4
    pairs = [(slot_hbm, slot_smem), (pos_in, pos_ref), (valid_in, valid_ref)]
    if first:
        pairs = [(x_in_ref, x_ref), (gain_in, gain_ref), (shift_in, shift_ref), (bq_in, bq_ref)] + pairs
    small = [pltpu.make_async_copy(src, dst, sem_s.at[i]) for i, (src, dst) in enumerate(pairs)]
    for c in small:
        c.start()
    wo_copy = pltpu.make_async_copy(wo_hbm.at[layer], wo, sem_w.at[n_chunk])
    if first:
        step = x_ref.shape[1] // n_chunk
        w_copies = [
            pltpu.make_async_copy(wq_hbm.at[layer, pl.ds(i * step, step)], wq.at[pl.ds(i * step, step)], sem_w.at[i])
            for i in range(n_chunk)
        ]
        for c in w_copies:
            c.start()

    def in_copy(which, g):
        src, dst = ((k_hbm, kbuf), (v_hbm, vbuf))[which]
        return pltpu.make_async_copy(src.at[layer, pl.ds(g * GROUP, GROUP)], dst.at[pl.ds(g * GROUP, GROUP)], sem_in.at[which, g])

    def out_copy(which, g):
        src, dst = ((kbuf, k_out), (vbuf, v_out))[which]
        return pltpu.make_async_copy(src.at[pl.ds(g * GROUP, GROUP)], dst.at[layer, pl.ds(g * GROUP, GROUP)], sem_out.at[which])

    if first:
        for g in range(AHEAD - n_chunk):
            in_copy(0, g).start()
            in_copy(1, g).start()
    else:
        wo_copy.start()
        old = [
            pltpu.make_async_copy(src.at[layer - 1, pl.ds(g * GROUP, GROUP)], dst.at[layer - 1, pl.ds(g * GROUP, GROUP)], sem_out.at[2 + i])
            for g in range(EARLY, n_groups) for i, (src, dst) in enumerate(((kall, k_out), (vall, v_out)))
        ]
        for c in old:
            c.start()

    t_row = lax.broadcasted_iota(jnp.int32, (cache_len, n_cols), 0)
    t_col = lax.broadcasted_iota(jnp.int32, (cache_len, n_cols), 1) // n_local
    spread = (t_row == t_col).astype(BF16)
    for c in small:
        c.wait()
    pos = jnp.dot(pos_ref[...].astype(F32).astype(BF16), spread, preferred_element_type=F32)
    valid = jnp.dot(valid_ref[...].astype(F32).astype(BF16), spread, preferred_element_type=F32)
    bias[0] = pos
    bias[1] = valid

    if first:
        x_in = layer_norm_f32(x_ref[...].astype(F32), gain_ref[layer, 0:1], shift_ref[layer, 0:1])
        acc = None
        for i in range(n_chunk):
            w_copies[i].wait()
            in_copy(0, AHEAD - n_chunk + i).start()
            in_copy(1, AHEAD - n_chunk + i).start()
            d = jnp.dot(x_in[:, i * step:(i + 1) * step], wq[i * step:(i + 1) * step], preferred_element_type=F32)
            acc = d if acc is None else acc + d
        qkv[...] = (acc + bq_ref[layer:layer + 1].astype(F32)).astype(BF16).astype(F32)

    scale = 1.0 / math.sqrt(head_dim)
    rows = n_local * GROUP
    head0 = lax.axis_index('tp') * n_local

    def update(g):
        base = pl.multiple_of(g * GROUP, GROUP)
        row16 = lax.broadcasted_iota(jnp.int32, (16, head_dim), 0)
        fresh = qkv[pl.ds(base, GROUP), :]
        row8 = lax.broadcasted_iota(jnp.int32, (GROUP, n_cols), 0)
        slots = jnp.zeros((GROUP, n_cols), jnp.int32)
        for b in range(GROUP):
            slot = slot_smem[g * GROUP + b]
            slots = jnp.where(row8 == b, slot, slots)
            first_row = slot * n_local
            start = pl.multiple_of((first_row // 16) * 16, 16)
            off = first_row - start
            for which, buf in ((1, kbuf), (2, vbuf)):
                block = buf[base + b, pl.ds(start, 16), :].astype(F32)
                for h in range(n_local):
                    new = fresh[b:b + 1, (3 * h + which) * head_dim:(3 * h + which + 1) * head_dim]
                    block = jnp.where(row16 == off + h, new, block)
                buf[base + b, pl.ds(start, 16), :] = block.astype(BF16)
        col = lax.broadcasted_iota(jnp.int32, (GROUP, n_cols), 1)
        allowed = jnp.logical_or(bias[1, pl.ds(base, GROUP)] > 0.5, col // n_local == slots)
        pos_g = bias[0, pl.ds(base, GROUP)]
        parts = []
        for h in range(n_local):
            num = (jnp.full((GROUP, n_cols), 1 + h, jnp.int32) + head0).astype(F32)
            slope = jnp.exp2(-8.0 * num / n_heads)
            parts.append(jnp.where(jnp.logical_and(allowed, col % n_local == h), slope * pos_g, -jnp.inf))
        queries = jnp.concatenate([fresh[:, 3 * h * head_dim:(3 * h + 1) * head_dim] for h in range(n_local)], axis=0)
        odd = lax.broadcasted_iota(jnp.int32, (rows, head_dim), 0) % 2 == 1
        q_pair = jnp.concatenate([jnp.where(odd, 0.0, queries), jnp.where(odd, queries, 0.0)], axis=1).astype(BF16)
        return base, q_pair, jnp.concatenate(parts, axis=0)

    def scores(base, q_pair, add):
        row_s = lax.broadcasted_iota(jnp.int32, (rows, n_cols), 0) % GROUP // 2
        s = None
        for b in range(0, GROUP, 2):
            keys = jnp.concatenate([kbuf[base + b], kbuf[base + b + 1]], axis=1)
            sb = lax.dot_general(q_pair, keys, (((1,), (1,)), ((), ())), preferred_element_type=F32)
            s = sb if s is None else jnp.where(row_s == b // 2, sb, s)
        return s * scale + add

    def softmax(s):
        top = jnp.max(s, axis=-1, keepdims=True)
        e = jnp.exp(s - top)
        return (e * (1.0 / jnp.sum(e, axis=-1, keepdims=True))).astype(BF16)

    def mix(base, p):
        row_o = lax.broadcasted_iota(jnp.int32, (rows, head_dim), 0) % GROUP
        o = None
        for b in range(0, GROUP, 2):
            values = jnp.concatenate([vbuf[base + b], vbuf[base + b + 1]], axis=1)
            ob = jnp.dot(p, values, preferred_element_type=F32)
            for i in range(2):
                oi = ob[:, i * head_dim:(i + 1) * head_dim]
                o = oi if o is None else jnp.where(row_o == b + i, oi, o)
        for h in range(n_local):
            attn[pl.ds(base, GROUP), h * head_dim:(h + 1) * head_dim] = o[h * GROUP:(h + 1) * GROUP]

    def groups(i, carry):
        todo = [i * SUB + j for j in range(SUB)]
        if first:
            for g in todo:
                in_copy(0, g).wait()
                in_copy(1, g).wait()

            @pl.when(todo[-1] + AHEAD < n_groups)
            def _():
                for g in todo:
                    in_copy(0, g + AHEAD).start()
                    in_copy(1, g + AHEAD).start()

            @pl.when(i == n_groups // SUB - 2)
            def _():
                wo_copy.start()

            @pl.when(i >= (n_groups - EARLY) // SUB)
            def _():
                for j in range(SUB):
                    g = i * SUB + j - (n_groups - EARLY)
                    out_copy(0, g).start()
                    out_copy(1, g).start()
        state = [update(g) for g in todo]
        probs = [scores(*st) for st in state]
        for (base, _, _), s in zip(state, probs):
            mix(base, softmax(s))
        if not first:
            for g in todo:
                out_copy(0, g).start()
                out_copy(1, g).start()
        return carry

    lax.fori_loop(0, n_groups // SUB, groups, 0)
    wo_copy.wait()
    part_ref[...] = jnp.dot(attn[...].astype(BF16), wo[...], preferred_element_type=F32)
    for c in old:
        c.wait()
    for g in range(EARLY if first else n_groups):
        out_copy(0, g).wait()
        out_copy(1, g).wait()


def reduce_kernel(layer, n_tp, last, *refs):
    (part_ref, res_ref, gain_ref, shift_ref, bo_ref, wu_hbm, bu_ref, wd_hbm, bd_ref) = refs[:9]
    if last:
        out_ref, rest = refs[9], refs[10:]
    else:
        (k_hbm, v_hbm, wq_hbm, bq_ref, k_raw, v_raw, out_ref, own_ref, kall, vall) = refs[9:19]
        rest = refs[19:]
    (wu, wd, part2, d2d, mid, got, gath, gath2, sem_w,
     pair_s, pair_r, chip_s, chip_r, ag_s, ag_r, agp_s, agp_r) = rest
    n_batch, width = part_ref.shape
    n_chip = n_tp // 2
    blk = n_batch // n_tp
    me = lax.axis_index('tp')
    x = me // 2
    c = me % 2
    partner = x * 2 + (1 - c)

    def chip(d):
        return lax.rem(x + d, n_chip)

    w_copies = [pltpu.make_async_copy(wu_hbm.at[layer], wu, sem_w.at[0]), pltpu.make_async_copy(wd_hbm.at[layer], wd, sem_w.at[1])]
    if not last:
        w_copies.append(pltpu.make_async_copy(k_hbm.at[layer + 1], kall.at[layer + 1], sem_w.at[2]))
        w_copies.append(pltpu.make_async_copy(v_hbm.at[layer + 1], vall.at[layer + 1], sem_w.at[3]))
        n_qkv = bq_ref.shape[1]
        wq = wu.at[:, pl.ds(0, n_qkv)]
        wq_copy = pltpu.make_async_copy(wq_hbm.at[layer + 1], wq, sem_w.at[4])
    barrier = pltpu.get_barrier_semaphore()
    peers = [partner] + [chip(d) * 2 + 1 - c for d in range(1, n_chip)]
    for peer in peers:
        pl.semaphore_signal(barrier, inc=1, device_id={'tp': peer}, device_id_type=MESH)
    for w in w_copies[:2]:
        w.start()
    pl.semaphore_wait(barrier, len(peers))

    sent = []
    order = [2, 1, 3, 0] if n_chip == 4 else list(range(1, n_chip)) + [0]

    def rows_of(core, d):
        return pl.ds(pl.multiple_of((core * n_chip + chip(d)) * blk, blk), blk)

    far = order[:-1]
    by_distance = sorted(order, key=lambda d: min(d, n_chip - d))

    def remote(src, dst, send_sem, recv_sem, to):
        return pltpu.make_async_remote_copy(src_ref=src, dst_ref=dst, send_sem=send_sem, recv_sem=recv_sem, device_id={'tp': to}, device_id_type=MESH)

    def reduce_scatter(phase, src, fills):
        part = width // len(fills)
        pair, hops = [], []
        for k, fill in enumerate(fills):
            sem, cols = phase + k, pl.ds(k * part, part)
            if fill is not None:
                fill(k * part, part)
            pair.append({
                d: remote(src.at[rows_of(1 - c, d), cols], d2d.at[phase, d, :, cols], pair_s.at[sem, d], pair_r.at[sem, d], partner)
                for d in order
            })
            for d in order:
                pair[k][d].start()
        for k in range(len(fills)):
            sem, cols = phase + k, pl.ds(k * part, part)
            hops.append({})
            for d in order:
                pair[k][d].wait_recv()
                mid[phase, d, :, cols] = src[rows_of(c, d), cols] + d2d[phase, d, :, cols]
                hops[k][d] = remote(mid.at[phase, d, :, cols], got.at[phase, d, :, cols], chip_s.at[sem, d], chip_r.at[sem, d], chip(d) * 2 + 1 - c)
                hops[k][d].start()
        sums = []
        for k in range(len(fills)):
            acc = None
            for d in by_distance:
                hops[k][d].wait_recv()
                term = got[phase, d, :, pl.ds(k * part, part)]
                acc = term if acc is None else acc + term
            sums.append(acc)
            sent.extend([*pair[k].values(), *hops[k].values()])
        return sums[0] if len(sums) == 1 else jnp.concatenate(sums, axis=1)

    def all_gather(phase, buf, value, parts, consume):
        buf[1 - c, x] = value
        part = width // parts

        def pass_on(k, d):
            slot = lax.rem(x + n_chip - d, n_chip)
            ref = buf.at[c if d else 1 - c, slot, :, pl.ds(k * part, part)]
            return remote(ref, ref, agp_s.at[phase + k, d], agp_r.at[phase + k, d], partner)

        hops, passed = [], []
        for k in range(parts):
            ref = buf.at[1 - c, x, :, pl.ds(k * part, part)]
            hops.append({d: remote(ref, ref, ag_s.at[phase + k, d], ag_r.at[phase + k, d], chip(d) * 2 + 1 - c) for d in far})
            for d in far:
                hops[k][d].start()
            passed.append([pass_on(k, 0)])
            passed[k][0].start()
        for k in range(parts):
            for d in by_distance[1:]:
                hops[k][d].wait_recv()
                passed[k].append(pass_on(k, d))
                passed[k][-1].start()
        out = None
        for k in range(parts):
            for cp in passed[k]:
                cp.wait_recv()
            rows = buf[:, :, :, k * part:(k + 1) * part].astype(F32).reshape(n_batch, part).astype(BF16)
            term = consume(k * part, part, rows)
            out = term if out is None else out + term
            sent.extend([*passed[k], *hops[k].values()])
        return out

    def product(ref, n_cols):
        return lambda lo, size, rows: jnp.dot(rows, ref[lo:lo + size, :n_cols], preferred_element_type=F32)

    if last:
        res = res_ref[...].astype(F32)
    else:
        res = res_ref[rows_of(1 - c, 0), :].astype(F32)
    total = reduce_scatter(0, part_ref, [None])
    for w in w_copies[2:]:
        w.start()
    x_mid = (res + total + bo_ref[layer:layer + 1].astype(F32)).astype(BF16).astype(F32)
    w_copies[0].wait()
    normed = layer_norm_f32(x_mid, gain_ref[layer, 1:2], shift_ref[layer, 1:2])
    up = all_gather(0, gath, normed, 1, product(wu, wu.shape[1])) + bu_ref[layer:layer + 1].astype(F32)
    act = jax.nn.gelu(up, approximate=True).astype(BF16)
    if not last:
        wq_copy.start()
    w_copies[1].wait()

    def down(lo, size):
        part2[:, lo:lo + size] = jnp.dot(act, wd[:, lo:lo + size], preferred_element_type=F32)

    total = reduce_scatter(1, part2, [down, down])
    x_next = (x_mid + total + bd_ref[layer:layer + 1].astype(F32)).astype(BF16)
    if last:
        out_ref[...] = all_gather(2, gath2, x_next, 1, lambda lo, size, rows: rows)
    else:
        own_ref[...] = x_next
        nxt = layer_norm_f32(x_next.astype(F32), gain_ref[layer + 1, 0:1], shift_ref[layer + 1, 0:1])
        wq_copy.wait()
        qkv = all_gather(2, gath2, nxt, 1, product(wu, n_qkv)) + bq_ref[layer + 1:layer + 2].astype(F32)
        out_ref[...] = qkv.astype(BF16).astype(F32)
        for w in w_copies[2:]:
            w.wait()
    for cp in sent:
        cp.wait_send()


def solution(mesh):
    tp_size = mesh.shape['tp']
    vm = pl.BlockSpec(memory_space=pltpu.VMEM)
    sm = pl.BlockSpec(memory_space=pltpu.SMEM)
    hbm = pl.BlockSpec(memory_space=pltpu.HBM)

    def device_step(hidden, ln_gain, ln_shift, w_qkv, b_qkv, w_out, b_out, w_up, b_up, w_down, b_down, k_cache, v_cache, write_slot, key_pos, key_valid):
        n_layers, n_batch, cache_len, n_local, head_dim = k_cache.shape
        width = hidden.shape[-1]
        n_cols = cache_len * n_local
        flat = (n_layers, n_batch, n_cols, head_dim)
        in_hbm = functools.partial(pltpu.with_memory_space_constraint, memory_space=pltpu.HBM)
        k_in, v_in = in_hbm(k_cache.reshape(flat)), in_hbm(v_cache.reshape(flat))
        w_qkv, w_out, w_up, w_down = map(in_hbm, (w_qkv, w_out, w_up, w_down))
        x0 = hidden.reshape(n_batch, width)
        n_groups = n_batch // GROUP
        blk = n_batch // tp_size
        n_chip = tp_size // 2
        shape = jax.ShapeDtypeStruct(flat, BF16)
        held = pltpu.VMEM(flat, BF16)
        shared = [in_hbm(a) for a in (write_slot, key_pos, key_valid)]

        def attn(layer, x_in, caches):
            first = layer == 0
            n_qkv = b_qkv.shape[1]
            scratch = [
                pltpu.VMEM(key_pos.shape, jnp.int32),
                pltpu.VMEM(key_valid.shape, jnp.int32),
                pltpu.SMEM(write_slot.shape, jnp.int32),
                pltpu.VMEM(w_out.shape[1:], BF16),
                pltpu.VMEM((2, n_batch, n_cols), F32),
                pltpu.VMEM((n_batch, n_local * head_dim), F32),
                pltpu.SemaphoreType.DMA((5,)),
                pltpu.SemaphoreType.DMA((7,)),
                pltpu.SemaphoreType.DMA((4,)),
            ]
            alias = {}
            part = jax.ShapeDtypeStruct((n_batch, width), F32)
            outs, out_specs = (part, shape, shape, held, held), (vm, hbm, hbm, vm, vm)
            if first:
                ins = [in_hbm(a) for a in (x_in, ln_gain, ln_shift, b_qkv)] + [w_qkv, w_out] + shared + [k_in, v_in]
                specs = [hbm] * len(ins)
                scratch += [
                    pltpu.VMEM(x_in.shape, BF16),
                    pltpu.VMEM(ln_gain.shape, BF16),
                    pltpu.VMEM(ln_shift.shape, BF16),
                    pltpu.VMEM(b_qkv.shape, BF16),
                    pltpu.VMEM(w_qkv.shape[1:], BF16),
                    pltpu.VMEM((n_batch, n_qkv), F32),
                    pltpu.SemaphoreType.DMA((2, n_groups)),
                ]
            else:
                ins = [x_in, w_out] + shared + list(caches)
                specs = [vm, hbm] + [hbm] * len(shared) + [hbm] * 2 + [vm] * 2
                alias = {len(ins) - 4 + i: 1 + i for i in range(4)}
            return pl.pallas_call(
                functools.partial(attn_kernel, layer, n_local * tp_size, first),
                out_shape=outs,
                in_specs=specs,
                out_specs=out_specs,
                scratch_shapes=scratch,
                input_output_aliases=alias,
                compiler_params=pltpu.CompilerParams(vmem_limit_bytes=13 * MIB),
                name=f'attn_{layer}',
            )(*ins)

        def reduce(layer, part, res, caches=()):
            last = layer == n_layers - 1
            ins = [part, res, ln_gain, ln_shift, b_out, w_up, b_up, w_down, b_down]
            specs = [vm, vm, vm, vm, vm, hbm, vm, hbm, vm]
            outs = [jax.ShapeDtypeStruct((n_batch, width), BF16)]
            if not last:
                ins += [k_in, v_in, w_qkv, b_qkv, *caches]
                specs += [hbm, hbm, hbm, vm, vm, vm]
                outs = [jax.ShapeDtypeStruct((n_batch, b_qkv.shape[1]), F32)]
                outs += [jax.ShapeDtypeStruct((blk, width), BF16), held, held]
            dma = pltpu.SemaphoreType.DMA((4, n_chip))
            return pl.pallas_call(
                functools.partial(reduce_kernel, layer, tp_size, last),
                out_shape=tuple(outs),
                in_specs=specs,
                out_specs=tuple([vm] * len(outs)),
                scratch_shapes=[
                    pltpu.VMEM(w_up.shape[1:], BF16),
                    pltpu.VMEM(w_down.shape[1:], BF16),
                    pltpu.VMEM((n_batch, width), F32),
                    pltpu.VMEM((2, n_chip, blk, width), F32),
                    pltpu.VMEM((2, n_chip, blk, width), F32),
                    pltpu.VMEM((2, n_chip, blk, width), F32),
                    pltpu.VMEM((2, n_chip, blk, width), BF16),
                    pltpu.VMEM((2, n_chip, blk, width), BF16),
                    pltpu.SemaphoreType.DMA((6,)),
                ] + [dma] * 8,
                input_output_aliases={} if last else {len(ins) - 2: 2, len(ins) - 1: 3},
                compiler_params=pltpu.CompilerParams(vmem_limit_bytes=13 * MIB, collective_id=layer, has_side_effects=True),
                name=f'reduce_{layer}',
            )(*ins)

        part, k_new, v_new, k_held, v_held = attn(0, x0, None)
        qkv, x1, k_held, v_held = reduce(0, part, x0, (k_held, v_held))
        part, k_new, v_new, _, _ = attn(1, qkv, (k_new, v_new, k_held, v_held))
        (x_last,) = reduce(1, part, x1)
        return x_last[:, None, :], k_new.reshape(k_cache.shape), v_new.reshape(v_cache.shape)

    cache_spec = P(None, 'dp', None, 'tp', None)
    in_specs = (P('dp', None, None), P(), P(), P(None, None, 'tp'), P(None, 'tp'), P(None, 'tp', None), P(), P(None, None, 'tp'), P(None, 'tp'), P(None, 'tp', None), P(), cache_spec, cache_spec, P('dp'), P('dp', None), P('dp', None))
    out_specs = (P('dp', None, None), cache_spec, cache_spec)
    return jax.shard_map(device_step, mesh=mesh, in_specs=in_specs, out_specs=out_specs, check_vma=False)
```

```python
import functools
import math

import jax
import jax.numpy as jnp
from jax import lax
from jax.experimental import pallas as pl
from jax.experimental.pallas import tpu as pltpu
from jax.sharding import PartitionSpec as P

LN_EPS = 1e-5
MESH = pl.DeviceIdType.MESH
F32 = jnp.float32
BF16 = jnp.bfloat16
GROUP = 8
AHEAD = 6
SUB = 2
EARLY = 4
MIB = 2 ** 20


def layer_norm_f32(x_f32, gain, shift):
    mean_val = jnp.mean(x_f32, axis=-1, keepdims=True)
    centered = x_f32 - mean_val
    var_val = jnp.mean(centered * centered, axis=-1, keepdims=True)
    normed = centered * lax.rsqrt(var_val + LN_EPS)
    return (normed * gain.astype(F32) + shift.astype(F32)).astype(BF16)


def attn_kernel(layer, n_heads, first, *refs):
    if first:
        (x_in_ref, gain_in, shift_in, bq_in, wq_hbm, wo_hbm, slot_hbm, pos_in, valid_in, k_hbm, v_hbm,
         part_ref, k_out, v_out, kall, vall,
         pos_ref, valid_ref, slot_smem, wo, bias, attn, sem_w, sem_s, sem_out,
         x_ref, gain_ref, shift_ref, bq_ref, wq, qkv, sem_in) = refs
        old = []
    else:
        (qkv, wo_hbm, slot_hbm, pos_in, valid_in, k_part, v_part, k_raw, v_raw,
         part_ref, k_out, v_out, kall, vall,
         pos_ref, valid_ref, slot_smem, wo, bias, attn, sem_w, sem_s, sem_out) = refs
    kbuf, vbuf = kall.at[layer], vall.at[layer]
    n_batch, n_cols, head_dim = kbuf.shape
    n_groups = n_batch // GROUP
    n_local = attn.shape[1] // head_dim
    cache_len = n_cols // n_local
    n_chunk = 4
    pairs = [(slot_hbm, slot_smem), (pos_in, pos_ref), (valid_in, valid_ref)]
    if first:
        pairs = [(x_in_ref, x_ref), (gain_in, gain_ref), (shift_in, shift_ref), (bq_in, bq_ref)] + pairs
    small = [pltpu.make_async_copy(src, dst, sem_s.at[i]) for i, (src, dst) in enumerate(pairs)]
    for c in small:
        c.start()
    wo_copy = pltpu.make_async_copy(wo_hbm.at[layer], wo, sem_w.at[n_chunk])
    if first:
        step = x_ref.shape[1] // n_chunk
        w_copies = [
            pltpu.make_async_copy(wq_hbm.at[layer, pl.ds(i * step, step)], wq.at[pl.ds(i * step, step)], sem_w.at[i])
            for i in range(n_chunk)
        ]
        for c in w_copies:
            c.start()

    def in_copy(which, g):
        src, dst = ((k_hbm, kbuf), (v_hbm, vbuf))[which]
        return pltpu.make_async_copy(src.at[layer, pl.ds(g * GROUP, GROUP)], dst.at[pl.ds(g * GROUP, GROUP)], sem_in.at[which, g])

    def out_copy(which, g):
        src, dst = ((kbuf, k_out), (vbuf, v_out))[which]
        return pltpu.make_async_copy(src.at[pl.ds(g * GROUP, GROUP)], dst.at[layer, pl.ds(g * GROUP, GROUP)], sem_out.at[which])

    if first:
        for g in range(AHEAD - n_chunk):
            in_copy(0, g).start()
            in_copy(1, g).start()
    else:
        wo_copy.start()
        old = [
            pltpu.make_async_copy(src.at[layer - 1, pl.ds(g * GROUP, GROUP)], dst.at[layer - 1, pl.ds(g * GROUP, GROUP)], sem_out.at[2 + i])
            for g in range(EARLY, n_groups) for i, (src, dst) in enumerate(((kall, k_out), (vall, v_out)))
        ]
        for c in old:
            c.start()

    t_row = lax.broadcasted_iota(jnp.int32, (cache_len, n_cols), 0)
    t_col = lax.broadcasted_iota(jnp.int32, (cache_len, n_cols), 1) // n_local
    spread = (t_row == t_col).astype(BF16)
    for c in small:
        c.wait()
    pos = jnp.dot(pos_ref[...].astype(F32).astype(BF16), spread, preferred_element_type=F32)
    valid = jnp.dot(valid_ref[...].astype(F32).astype(BF16), spread, preferred_element_type=F32)
    bias[0] = pos
    bias[1] = valid

    if first:
        x_in = layer_norm_f32(x_ref[...].astype(F32), gain_ref[layer, 0:1], shift_ref[layer, 0:1])
        acc = None
        for i in range(n_chunk):
            w_copies[i].wait()
            in_copy(0, AHEAD - n_chunk + i).start()
            in_copy(1, AHEAD - n_chunk + i).start()
            d = jnp.dot(x_in[:, i * step:(i + 1) * step], wq[i * step:(i + 1) * step], preferred_element_type=F32)
            acc = d if acc is None else acc + d
        qkv[...] = (acc + bq_ref[layer:layer + 1].astype(F32)).astype(BF16).astype(F32)

    scale = 1.0 / math.sqrt(head_dim)
    rows = n_local * GROUP
    head0 = lax.axis_index('tp') * n_local

    def update(g):
        base = pl.multiple_of(g * GROUP, GROUP)
        row16 = lax.broadcasted_iota(jnp.int32, (16, head_dim), 0)
        fresh = qkv[pl.ds(base, GROUP), :]
        row8 = lax.broadcasted_iota(jnp.int32, (GROUP, n_cols), 0)
        slots = jnp.zeros((GROUP, n_cols), jnp.int32)
        for b in range(GROUP):
            slot = slot_smem[g * GROUP + b]
            slots = jnp.where(row8 == b, slot, slots)
            first_row = slot * n_local
            start = pl.multiple_of((first_row // 16) * 16, 16)
            off = first_row - start
            for which, buf in ((1, kbuf), (2, vbuf)):
                block = buf[base + b, pl.ds(start, 16), :].astype(F32)
                for h in range(n_local):
                    new = fresh[b:b + 1, (3 * h + which) * head_dim:(3 * h + which + 1) * head_dim]
                    block = jnp.where(row16 == off + h, new, block)
                buf[base + b, pl.ds(start, 16), :] = block.astype(BF16)
        col = lax.broadcasted_iota(jnp.int32, (GROUP, n_cols), 1)
        allowed = jnp.logical_or(bias[1, pl.ds(base, GROUP)] > 0.5, col // n_local == slots)
        pos_g = bias[0, pl.ds(base, GROUP)]
        parts = []
        for h in range(n_local):
            num = (jnp.full((GROUP, n_cols), 1 + h, jnp.int32) + head0).astype(F32)
            slope = jnp.exp2(-8.0 * num / n_heads)
            parts.append(jnp.where(jnp.logical_and(allowed, col % n_local == h), slope * pos_g, -jnp.inf))
        queries = jnp.concatenate([fresh[:, 3 * h * head_dim:(3 * h + 1) * head_dim] for h in range(n_local)], axis=0)
        odd = lax.broadcasted_iota(jnp.int32, (rows, head_dim), 0) % 2 == 1
        q_pair = jnp.concatenate([jnp.where(odd, 0.0, queries), jnp.where(odd, queries, 0.0)], axis=1).astype(BF16)
        return base, q_pair, jnp.concatenate(parts, axis=0)

    def scores(base, q_pair, add):
        row_s = lax.broadcasted_iota(jnp.int32, (rows, n_cols), 0) % GROUP // 2
        s = None
        for b in range(0, GROUP, 2):
            keys = jnp.concatenate([kbuf[base + b], kbuf[base + b + 1]], axis=1)
            sb = lax.dot_general(q_pair, keys, (((1,), (1,)), ((), ())), preferred_element_type=F32)
            s = sb if s is None else jnp.where(row_s == b // 2, sb, s)
        return s * scale + add

    def softmax(s):
        top = jnp.max(s, axis=-1, keepdims=True)
        e = jnp.exp(s - top)
        return (e * (1.0 / jnp.sum(e, axis=-1, keepdims=True))).astype(BF16)

    def mix(base, p):
        row_o = lax.broadcasted_iota(jnp.int32, (rows, head_dim), 0) % GROUP
        o = None
        for b in range(0, GROUP, 2):
            values = jnp.concatenate([vbuf[base + b], vbuf[base + b + 1]], axis=1)
            ob = jnp.dot(p, values, preferred_element_type=F32)
            for i in range(2):
                oi = ob[:, i * head_dim:(i + 1) * head_dim]
                o = oi if o is None else jnp.where(row_o == b + i, oi, o)
        for h in range(n_local):
            attn[pl.ds(base, GROUP), h * head_dim:(h + 1) * head_dim] = o[h * GROUP:(h + 1) * GROUP]

    def groups(i, carry):
        todo = [i * SUB + j for j in range(SUB)]
        if first:
            for g in todo:
                in_copy(0, g).wait()
                in_copy(1, g).wait()

            @pl.when(todo[-1] + AHEAD < n_groups)
            def _():
                for g in todo:
                    in_copy(0, g + AHEAD).start()
                    in_copy(1, g + AHEAD).start()

            @pl.when(i == n_groups // SUB - 2)
            def _():
                wo_copy.start()

            @pl.when(i >= (n_groups - EARLY) // SUB)
            def _():
                for j in range(SUB):
                    g = i * SUB + j - (n_groups - EARLY)
                    out_copy(0, g).start()
                    out_copy(1, g).start()
        state = [update(g) for g in todo]
        probs = [scores(*st) for st in state]
        for (base, _, _), s in zip(state, probs):
            mix(base, softmax(s))
        if not first:
            for g in todo:
                out_copy(0, g).start()
                out_copy(1, g).start()
        return carry

    lax.fori_loop(0, n_groups // SUB, groups, 0)
    wo_copy.wait()
    part_ref[...] = jnp.dot(attn[...].astype(BF16), wo[...], preferred_element_type=F32)
    for c in old:
        c.wait()
    for g in range(EARLY if first else n_groups):
        out_copy(0, g).wait()
        out_copy(1, g).wait()


def reduce_kernel(layer, n_tp, last, *refs):
    (part_ref, res_ref, gain_ref, shift_ref, bo_ref, wu_hbm, bu_ref, wd_hbm, bd_ref) = refs[:9]
    if last:
        out_ref, rest = refs[9], refs[10:]
    else:
        (k_hbm, v_hbm, wq_hbm, bq_ref, k_raw, v_raw, out_ref, own_ref, kall, vall) = refs[9:19]
        rest = refs[19:]
    (wu, wd, part2, d2d, mid, got, gath, gath2, sem_w,
     pair_s, pair_r, chip_s, chip_r, ag_s, ag_r, agp_s, agp_r) = rest
    n_batch, width = part_ref.shape
    n_chip = n_tp // 2
    blk = n_batch // n_tp
    me = lax.axis_index('tp')
    x = me // 2
    c = me % 2
    partner = x * 2 + (1 - c)

    def chip(d):
        return lax.rem(x + d, n_chip)

    w_copies = [pltpu.make_async_copy(wu_hbm.at[layer], wu, sem_w.at[0]), pltpu.make_async_copy(wd_hbm.at[layer], wd, sem_w.at[1])]
    if not last:
        w_copies.append(pltpu.make_async_copy(k_hbm.at[layer + 1], kall.at[layer + 1], sem_w.at[2]))
        w_copies.append(pltpu.make_async_copy(v_hbm.at[layer + 1], vall.at[layer + 1], sem_w.at[3]))
        n_qkv = bq_ref.shape[1]
        wq = wu.at[:, pl.ds(0, n_qkv)]
        wq_copy = pltpu.make_async_copy(wq_hbm.at[layer + 1], wq, sem_w.at[4])
    barrier = pltpu.get_barrier_semaphore()
    peers = [partner] + [chip(d) * 2 + 1 - c for d in range(1, n_chip)]
    for peer in peers:
        pl.semaphore_signal(barrier, inc=1, device_id={'tp': peer}, device_id_type=MESH)
    for w in w_copies[:2]:
        w.start()
    pl.semaphore_wait(barrier, len(peers))

    sent = []
    order = [2, 1, 3, 0] if n_chip == 4 else list(range(1, n_chip)) + [0]

    def rows_of(core, d):
        return pl.ds(pl.multiple_of((core * n_chip + chip(d)) * blk, blk), blk)

    far = order[:-1]
    by_distance = sorted(order, key=lambda d: min(d, n_chip - d))

    def remote(src, dst, send_sem, recv_sem, to):
        return pltpu.make_async_remote_copy(src_ref=src, dst_ref=dst, send_sem=send_sem, recv_sem=recv_sem, device_id={'tp': to}, device_id_type=MESH)

    def reduce_scatter(phase, src, fills):
        part = width // len(fills)
        pair, hops = [], []
        for k, fill in enumerate(fills):
            sem, cols = phase + k, pl.ds(k * part, part)
            if fill is not None:
                fill(k * part, part)
            pair.append({
                d: remote(src.at[rows_of(1 - c, d), cols], d2d.at[phase, d, :, cols], pair_s.at[sem, d], pair_r.at[sem, d], partner)
                for d in order
            })
            for d in order:
                pair[k][d].start()
        for k in range(len(fills)):
            sem, cols = phase + k, pl.ds(k * part, part)
            hops.append({})
            for d in order:
                pair[k][d].wait_recv()
                mid[phase, d, :, cols] = src[rows_of(c, d), cols] + d2d[phase, d, :, cols]
                hops[k][d] = remote(mid.at[phase, d, :, cols], got.at[phase, d, :, cols], chip_s.at[sem, d], chip_r.at[sem, d], chip(d) * 2 + 1 - c)
                hops[k][d].start()
        sums = []
        for k in range(len(fills)):
            acc = None
            for d in by_distance:
                hops[k][d].wait_recv()
                term = got[phase, d, :, pl.ds(k * part, part)]
                acc = term if acc is None else acc + term
            sums.append(acc)
            sent.extend([*pair[k].values(), *hops[k].values()])
        return sums[0] if len(sums) == 1 else jnp.concatenate(sums, axis=1)

    def all_gather(phase, buf, value, parts, consume):
        buf[1 - c, x] = value
        part = width // parts

        def pass_on(k, d):
            slot = lax.rem(x + n_chip - d, n_chip)
            ref = buf.at[c if d else 1 - c, slot, :, pl.ds(k * part, part)]
            return remote(ref, ref, agp_s.at[phase + k, d], agp_r.at[phase + k, d], partner)

        hops, passed = [], []
        for k in range(parts):
            ref = buf.at[1 - c, x, :, pl.ds(k * part, part)]
            hops.append({d: remote(ref, ref, ag_s.at[phase + k, d], ag_r.at[phase + k, d], chip(d) * 2 + 1 - c) for d in far})
            hops[k][far[0]].start()
            passed.append([pass_on(k, 0)])
        for k in range(parts):
            for d in far[1:]:
                hops[k][d].start()
            passed[k][0].start()
        for k in range(parts):
            for d in by_distance[1:]:
                hops[k][d].wait_recv()
                passed[k].append(pass_on(k, d))
                passed[k][-1].start()
        out = None
        for k in range(parts):
            for cp in passed[k]:
                cp.wait_recv()
            rows = buf[:, :, :, k * part:(k + 1) * part].astype(F32).reshape(n_batch, part).astype(BF16)
            term = consume(k * part, part, rows)
            out = term if out is None else out + term
            sent.extend([*passed[k], *hops[k].values()])
        return out

    def product(ref, n_cols):
        return lambda lo, size, rows: jnp.dot(rows, ref[lo:lo + size, :n_cols], preferred_element_type=F32)

    if last:
        res = res_ref[...].astype(F32)
    else:
        res = res_ref[rows_of(1 - c, 0), :].astype(F32)
    total = reduce_scatter(0, part_ref, [None])
    for w in w_copies[2:]:
        w.start()
    x_mid = (res + total + bo_ref[layer:layer + 1].astype(F32)).astype(BF16).astype(F32)
    w_copies[0].wait()
    normed = layer_norm_f32(x_mid, gain_ref[layer, 1:2], shift_ref[layer, 1:2])
    up = all_gather(0, gath, normed, 2, product(wu, wu.shape[1])) + bu_ref[layer:layer + 1].astype(F32)
    act = jax.nn.gelu(up, approximate=True).astype(BF16)
    if not last:
        wq_copy.start()
    w_copies[1].wait()

    def down(lo, size):
        part2[:, lo:lo + size] = jnp.dot(act, wd[:, lo:lo + size], preferred_element_type=F32)

    total = reduce_scatter(1, part2, [down])
    x_next = (x_mid + total + bd_ref[layer:layer + 1].astype(F32)).astype(BF16)
    if last:
        out_ref[...] = all_gather(2, gath2, x_next, 1, lambda lo, size, rows: rows)
    else:
        own_ref[...] = x_next
        nxt = layer_norm_f32(x_next.astype(F32), gain_ref[layer + 1, 0:1], shift_ref[layer + 1, 0:1])
        wq_copy.wait()
        qkv = all_gather(2, gath2, nxt, 2, product(wu, n_qkv)) + bq_ref[layer + 1:layer + 2].astype(F32)
        out_ref[...] = qkv.astype(BF16).astype(F32)
        for w in w_copies[2:]:
            w.wait()
    for cp in sent:
        cp.wait_send()


def solution(mesh):
    tp_size = mesh.shape['tp']
    vm = pl.BlockSpec(memory_space=pltpu.VMEM)
    sm = pl.BlockSpec(memory_space=pltpu.SMEM)
    hbm = pl.BlockSpec(memory_space=pltpu.HBM)

    def device_step(hidden, ln_gain, ln_shift, w_qkv, b_qkv, w_out, b_out, w_up, b_up, w_down, b_down, k_cache, v_cache, write_slot, key_pos, key_valid):
        n_layers, n_batch, cache_len, n_local, head_dim = k_cache.shape
        width = hidden.shape[-1]
        n_cols = cache_len * n_local
        flat = (n_layers, n_batch, n_cols, head_dim)
        in_hbm = functools.partial(pltpu.with_memory_space_constraint, memory_space=pltpu.HBM)
        k_in, v_in = in_hbm(k_cache.reshape(flat)), in_hbm(v_cache.reshape(flat))
        w_qkv, w_out, w_up, w_down = map(in_hbm, (w_qkv, w_out, w_up, w_down))
        x0 = hidden.reshape(n_batch, width)
        n_groups = n_batch // GROUP
        blk = n_batch // tp_size
        n_chip = tp_size // 2
        shape = jax.ShapeDtypeStruct(flat, BF16)
        held = pltpu.VMEM(flat, BF16)
        shared = [in_hbm(a) for a in (write_slot, key_pos, key_valid)]

        def attn(layer, x_in, caches):
            first = layer == 0
            n_qkv = b_qkv.shape[1]
            scratch = [
                pltpu.VMEM(key_pos.shape, jnp.int32),
                pltpu.VMEM(key_valid.shape, jnp.int32),
                pltpu.SMEM(write_slot.shape, jnp.int32),
                pltpu.VMEM(w_out.shape[1:], BF16),
                pltpu.VMEM((2, n_batch, n_cols), F32),
                pltpu.VMEM((n_batch, n_local * head_dim), F32),
                pltpu.SemaphoreType.DMA((5,)),
                pltpu.SemaphoreType.DMA((7,)),
                pltpu.SemaphoreType.DMA((4,)),
            ]
            alias = {}
            part = jax.ShapeDtypeStruct((n_batch, width), F32)
            outs, out_specs = (part, shape, shape, held, held), (vm, hbm, hbm, vm, vm)
            if first:
                ins = [in_hbm(a) for a in (x_in, ln_gain, ln_shift, b_qkv)] + [w_qkv, w_out] + shared + [k_in, v_in]
                specs = [hbm] * len(ins)
                scratch += [
                    pltpu.VMEM(x_in.shape, BF16),
                    pltpu.VMEM(ln_gain.shape, BF16),
                    pltpu.VMEM(ln_shift.shape, BF16),
                    pltpu.VMEM(b_qkv.shape, BF16),
                    pltpu.VMEM(w_qkv.shape[1:], BF16),
                    pltpu.VMEM((n_batch, n_qkv), F32),
                    pltpu.SemaphoreType.DMA((2, n_groups)),
                ]
            else:
                ins = [x_in, w_out] + shared + list(caches)
                specs = [vm, hbm] + [hbm] * len(shared) + [hbm] * 2 + [vm] * 2
                alias = {len(ins) - 4 + i: 1 + i for i in range(4)}
            return pl.pallas_call(
                functools.partial(attn_kernel, layer, n_local * tp_size, first),
                out_shape=outs,
                in_specs=specs,
                out_specs=out_specs,
                scratch_shapes=scratch,
                input_output_aliases=alias,
                compiler_params=pltpu.CompilerParams(vmem_limit_bytes=13 * MIB),
                name=f'attn_{layer}',
            )(*ins)

        def reduce(layer, part, res, caches=()):
            last = layer == n_layers - 1
            ins = [part, res, ln_gain, ln_shift, b_out, w_up, b_up, w_down, b_down]
            specs = [vm, vm, vm, vm, vm, hbm, vm, hbm, vm]
            outs = [jax.ShapeDtypeStruct((n_batch, width), BF16)]
            if not last:
                ins += [k_in, v_in, w_qkv, b_qkv, *caches]
                specs += [hbm, hbm, hbm, vm, vm, vm]
                outs = [jax.ShapeDtypeStruct((n_batch, b_qkv.shape[1]), F32)]
                outs += [jax.ShapeDtypeStruct((blk, width), BF16), held, held]
            dma = pltpu.SemaphoreType.DMA((4, n_chip))
            return pl.pallas_call(
                functools.partial(reduce_kernel, layer, tp_size, last),
                out_shape=tuple(outs),
                in_specs=specs,
                out_specs=tuple([vm] * len(outs)),
                scratch_shapes=[
                    pltpu.VMEM(w_up.shape[1:], BF16),
                    pltpu.VMEM(w_down.shape[1:], BF16),
                    pltpu.VMEM((n_batch, width), F32),
                    pltpu.VMEM((2, n_chip, blk, width), F32),
                    pltpu.VMEM((2, n_chip, blk, width), F32),
                    pltpu.VMEM((2, n_chip, blk, width), F32),
                    pltpu.VMEM((2, n_chip, blk, width), BF16),
                    pltpu.VMEM((2, n_chip, blk, width), BF16),
                    pltpu.SemaphoreType.DMA((6,)),
                ] + [dma] * 8,
                input_output_aliases={} if last else {len(ins) - 2: 2, len(ins) - 1: 3},
                compiler_params=pltpu.CompilerParams(vmem_limit_bytes=13 * MIB, collective_id=layer, has_side_effects=True),
                name=f'reduce_{layer}',
            )(*ins)

        part, k_new, v_new, k_held, v_held = attn(0, x0, None)
        qkv, x1, k_held, v_held = reduce(0, part, x0, (k_held, v_held))
        part, k_new, v_new, _, _ = attn(1, qkv, (k_new, v_new, k_held, v_held))
        (x_last,) = reduce(1, part, x1)
        return x_last[:, None, :], k_new.reshape(k_cache.shape), v_new.reshape(v_cache.shape)

    cache_spec = P(None, 'dp', None, 'tp', None)
    in_specs = (P('dp', None, None), P(), P(), P(None, None, 'tp'), P(None, 'tp'), P(None, 'tp', None), P(), P(None, None, 'tp'), P(None, 'tp'), P(None, 'tp', None), P(), cache_spec, cache_spec, P('dp'), P('dp', None), P('dp', None))
    out_specs = (P('dp', None, None), cache_spec, cache_spec)
    return jax.shard_map(device_step, mesh=mesh, in_specs=in_specs, out_specs=out_specs, check_vma=False)
```

```python
import functools
import math

import jax
import jax.numpy as jnp
from jax import lax
from jax.experimental import pallas as pl
from jax.experimental.pallas import tpu as pltpu
from jax.sharding import PartitionSpec as P

LN_EPS = 1e-5
MESH = pl.DeviceIdType.MESH
F32 = jnp.float32
BF16 = jnp.bfloat16
GROUP = 8
AHEAD = 6
SUB = 2
EARLY = 4
MIB = 2 ** 20


def layer_norm_f32(x_f32, gain, shift):
    mean_val = jnp.mean(x_f32, axis=-1, keepdims=True)
    centered = x_f32 - mean_val
    var_val = jnp.mean(centered * centered, axis=-1, keepdims=True)
    normed = centered * lax.rsqrt(var_val + LN_EPS)
    return (normed * gain.astype(F32) + shift.astype(F32)).astype(BF16)


def attn_kernel(layer, n_heads, first, *refs):
    if first:
        (x_in_ref, gain_in, shift_in, bq_in, wq_hbm, wo_hbm, slot_hbm, pos_in, valid_in, k_hbm, v_hbm,
         part_ref, k_out, v_out, kall, vall,
         pos_ref, valid_ref, slot_smem, wo, bias, attn, sem_w, sem_s, sem_out,
         x_ref, gain_ref, shift_ref, bq_ref, wq, qkv, sem_in) = refs
        old = []
    else:
        (qkv, wo_hbm, slot_hbm, pos_in, valid_in, k_part, v_part, k_raw, v_raw,
         part_ref, k_out, v_out, kall, vall,
         pos_ref, valid_ref, slot_smem, wo, bias, attn, sem_w, sem_s, sem_out) = refs
    kbuf, vbuf = kall.at[layer], vall.at[layer]
    n_batch, n_cols, head_dim = kbuf.shape
    n_groups = n_batch // GROUP
    n_local = attn.shape[1] // head_dim
    cache_len = n_cols // n_local
    n_chunk = 4
    pairs = [(slot_hbm, slot_smem), (pos_in, pos_ref), (valid_in, valid_ref)]
    if first:
        pairs = [(x_in_ref, x_ref), (gain_in, gain_ref), (shift_in, shift_ref), (bq_in, bq_ref)] + pairs
    small = [pltpu.make_async_copy(src, dst, sem_s.at[i]) for i, (src, dst) in enumerate(pairs)]
    for c in small:
        c.start()
    wo_copy = pltpu.make_async_copy(wo_hbm.at[layer], wo, sem_w.at[n_chunk])
    if first:
        step = x_ref.shape[1] // n_chunk
        w_copies = [
            pltpu.make_async_copy(wq_hbm.at[layer, pl.ds(i * step, step)], wq.at[pl.ds(i * step, step)], sem_w.at[i])
            for i in range(n_chunk)
        ]
        for c in w_copies:
            c.start()

    def in_copy(which, g):
        src, dst = ((k_hbm, kbuf), (v_hbm, vbuf))[which]
        return pltpu.make_async_copy(src.at[layer, pl.ds(g * GROUP, GROUP)], dst.at[pl.ds(g * GROUP, GROUP)], sem_in.at[which, g])

    def out_copy(which, g):
        src, dst = ((kbuf, k_out), (vbuf, v_out))[which]
        return pltpu.make_async_copy(src.at[pl.ds(g * GROUP, GROUP)], dst.at[layer, pl.ds(g * GROUP, GROUP)], sem_out.at[which])

    if first:
        for g in range(AHEAD - n_chunk):
            in_copy(0, g).start()
            in_copy(1, g).start()
    else:
        wo_copy.start()
        old = [
            pltpu.make_async_copy(src.at[layer - 1, pl.ds(g * GROUP, GROUP)], dst.at[layer - 1, pl.ds(g * GROUP, GROUP)], sem_out.at[2 + i])
            for g in range(EARLY, n_groups) for i, (src, dst) in enumerate(((kall, k_out), (vall, v_out)))
        ]
        for c in old:
            c.start()

    t_row = lax.broadcasted_iota(jnp.int32, (cache_len, n_cols), 0)
    t_col = lax.broadcasted_iota(jnp.int32, (cache_len, n_cols), 1) // n_local
    spread = (t_row == t_col).astype(BF16)
    for c in small:
        c.wait()
    pos = jnp.dot(pos_ref[...].astype(F32).astype(BF16), spread, preferred_element_type=F32)
    valid = jnp.dot(valid_ref[...].astype(F32).astype(BF16), spread, preferred_element_type=F32)
    bias[0] = pos
    bias[1] = valid

    if first:
        x_in = layer_norm_f32(x_ref[...].astype(F32), gain_ref[layer, 0:1], shift_ref[layer, 0:1])
        acc = None
        for i in range(n_chunk):
            w_copies[i].wait()
            in_copy(0, AHEAD - n_chunk + i).start()
            in_copy(1, AHEAD - n_chunk + i).start()
            d = jnp.dot(x_in[:, i * step:(i + 1) * step], wq[i * step:(i + 1) * step], preferred_element_type=F32)
            acc = d if acc is None else acc + d
        qkv[...] = (acc + bq_ref[layer:layer + 1].astype(F32)).astype(BF16).astype(F32)

    scale = 1.0 / math.sqrt(head_dim)
    rows = n_local * GROUP
    head0 = lax.axis_index('tp') * n_local

    def update(g):
        base = pl.multiple_of(g * GROUP, GROUP)
        row16 = lax.broadcasted_iota(jnp.int32, (16, head_dim), 0)
        fresh = qkv[pl.ds(base, GROUP), :]
        row8 = lax.broadcasted_iota(jnp.int32, (GROUP, n_cols), 0)
        slots = jnp.zeros((GROUP, n_cols), jnp.int32)
        for b in range(GROUP):
            slot = slot_smem[g * GROUP + b]
            slots = jnp.where(row8 == b, slot, slots)
            first_row = slot * n_local
            start = pl.multiple_of((first_row // 16) * 16, 16)
            off = first_row - start
            for which, buf in ((1, kbuf), (2, vbuf)):
                block = buf[base + b, pl.ds(start, 16), :].astype(F32)
                for h in range(n_local):
                    new = fresh[b:b + 1, (3 * h + which) * head_dim:(3 * h + which + 1) * head_dim]
                    block = jnp.where(row16 == off + h, new, block)
                buf[base + b, pl.ds(start, 16), :] = block.astype(BF16)
        col = lax.broadcasted_iota(jnp.int32, (GROUP, n_cols), 1)
        allowed = jnp.logical_or(bias[1, pl.ds(base, GROUP)] > 0.5, col // n_local == slots)
        pos_g = bias[0, pl.ds(base, GROUP)]
        parts = []
        for h in range(n_local):
            num = (jnp.full((GROUP, n_cols), 1 + h, jnp.int32) + head0).astype(F32)
            slope = jnp.exp2(-8.0 * num / n_heads)
            parts.append(jnp.where(jnp.logical_and(allowed, col % n_local == h), slope * pos_g, -jnp.inf))
        queries = jnp.concatenate([fresh[:, 3 * h * head_dim:(3 * h + 1) * head_dim] for h in range(n_local)], axis=0)
        odd = lax.broadcasted_iota(jnp.int32, (rows, head_dim), 0) % 2 == 1
        q_pair = jnp.concatenate([jnp.where(odd, 0.0, queries), jnp.where(odd, queries, 0.0)], axis=1).astype(BF16)
        return base, q_pair, jnp.concatenate(parts, axis=0)

    def scores(base, q_pair, add):
        row_s = lax.broadcasted_iota(jnp.int32, (rows, n_cols), 0) % GROUP // 2
        s = None
        for b in range(0, GROUP, 2):
            keys = jnp.concatenate([kbuf[base + b], kbuf[base + b + 1]], axis=1)
            sb = lax.dot_general(q_pair, keys, (((1,), (1,)), ((), ())), preferred_element_type=F32)
            s = sb if s is None else jnp.where(row_s == b // 2, sb, s)
        return s * scale + add

    def softmax(s):
        top = jnp.max(s, axis=-1, keepdims=True)
        e = jnp.exp(s - top)
        return (e * (1.0 / jnp.sum(e, axis=-1, keepdims=True))).astype(BF16)

    def mix(base, p):
        row_o = lax.broadcasted_iota(jnp.int32, (rows, head_dim), 0) % GROUP
        o = None
        for b in range(0, GROUP, 2):
            values = jnp.concatenate([vbuf[base + b], vbuf[base + b + 1]], axis=1)
            ob = jnp.dot(p, values, preferred_element_type=F32)
            for i in range(2):
                oi = ob[:, i * head_dim:(i + 1) * head_dim]
                o = oi if o is None else jnp.where(row_o == b + i, oi, o)
        for h in range(n_local):
            attn[pl.ds(base, GROUP), h * head_dim:(h + 1) * head_dim] = o[h * GROUP:(h + 1) * GROUP]

    def groups(i, carry):
        todo = [i * SUB + j for j in range(SUB)]
        if first:
            for g in todo:
                in_copy(0, g).wait()
                in_copy(1, g).wait()

            @pl.when(todo[-1] + AHEAD < n_groups)
            def _():
                for g in todo:
                    in_copy(0, g + AHEAD).start()
                    in_copy(1, g + AHEAD).start()

            @pl.when(i == n_groups // SUB - 2)
            def _():
                wo_copy.start()

            @pl.when(i >= (n_groups - EARLY) // SUB)
            def _():
                for j in range(SUB):
                    g = i * SUB + j - (n_groups - EARLY)
                    out_copy(0, g).start()
                    out_copy(1, g).start()
        state = [update(g) for g in todo]
        probs = [scores(*st) for st in state]
        for (base, _, _), s in zip(state, probs):
            mix(base, softmax(s))
        if not first:
            for g in todo:
                out_copy(0, g).start()
                out_copy(1, g).start()
        return carry

    lax.fori_loop(0, n_groups // SUB, groups, 0)
    wo_copy.wait()
    part_ref[...] = jnp.dot(attn[...].astype(BF16), wo[...], preferred_element_type=F32)
    for c in old:
        c.wait()
    for g in range(EARLY if first else n_groups):
        out_copy(0, g).wait()
        out_copy(1, g).wait()


def reduce_kernel(layer, n_tp, last, *refs):
    (part_ref, res_ref, gain_ref, shift_ref, bo_ref, wu_hbm, bu_ref, wd_hbm, bd_ref) = refs[:9]
    if last:
        out_ref, rest = refs[9], refs[10:]
    else:
        (k_hbm, v_hbm, wq_hbm, bq_ref, k_raw, v_raw, out_ref, own_ref, kall, vall) = refs[9:19]
        rest = refs[19:]
    (wu, wd, part2, d2d, mid, got, gath, gath2, sem_w,
     pair_s, pair_r, chip_s, chip_r, ag_s, ag_r, agp_s, agp_r) = rest
    n_batch, width = part_ref.shape
    n_chip = n_tp // 2
    blk = n_batch // n_tp
    me = lax.axis_index('tp')
    x = me // 2
    c = me % 2
    partner = x * 2 + (1 - c)

    def chip(d):
        return lax.rem(x + d, n_chip)

    w_copies = [pltpu.make_async_copy(wu_hbm.at[layer], wu, sem_w.at[0]), pltpu.make_async_copy(wd_hbm.at[layer], wd, sem_w.at[1])]
    if not last:
        w_copies.append(pltpu.make_async_copy(k_hbm.at[layer + 1], kall.at[layer + 1], sem_w.at[2]))
        w_copies.append(pltpu.make_async_copy(v_hbm.at[layer + 1], vall.at[layer + 1], sem_w.at[3]))
        n_qkv = bq_ref.shape[1]
        wq = wu.at[:, pl.ds(0, n_qkv)]
        wq_copy = pltpu.make_async_copy(wq_hbm.at[layer + 1], wq, sem_w.at[4])
    barrier = pltpu.get_barrier_semaphore()
    peers = [partner] + [chip(d) * 2 + 1 - c for d in range(1, n_chip)]
    for peer in peers:
        pl.semaphore_signal(barrier, inc=1, device_id={'tp': peer}, device_id_type=MESH)
    for w in w_copies:
        w.start()
    pl.semaphore_wait(barrier, len(peers))

    sent = []
    order = [1, 3, 2, 0] if n_chip == 4 else list(range(1, n_chip)) + [0]

    def rows_of(core, d):
        return pl.ds(pl.multiple_of((core * n_chip + chip(d)) * blk, blk), blk)

    def reduce_scatter(phase, src):
        pair = {
            d: pltpu.make_async_remote_copy(
                src_ref=src.at[rows_of(1 - c, d)], dst_ref=d2d.at[phase, d], send_sem=pair_s.at[phase, d],
                recv_sem=pair_r.at[phase, d], device_id={'tp': partner}, device_id_type=MESH)
            for d in order
        }
        for d in order:
            pair[d].start()
        hops = {}
        for d in order:
            pair[d].wait_recv()
            mid[phase, d] = src[rows_of(c, d), :] + d2d[phase, d]
            hops[d] = pltpu.make_async_remote_copy(
                src_ref=mid.at[phase, d], dst_ref=got.at[phase, d], send_sem=chip_s.at[phase, d],
                recv_sem=chip_r.at[phase, d], device_id={'tp': chip(d) * 2 + 1 - c}, device_id_type=MESH)
            hops[d].start()
        acc = None
        for d in sorted(hops, key=lambda d: min(d, n_chip - d)):
            hops[d].wait_recv()
            acc = got[phase, d] if acc is None else acc + got[phase, d]
        sent.extend([*pair.values(), *hops.values()])
        return acc

    def all_gather(phase, buf, value):
        buf[1 - c, x] = value
        hops = {}
        for d in order[:-1]:
            hops[d] = pltpu.make_async_remote_copy(
                src_ref=buf.at[1 - c, x], dst_ref=buf.at[1 - c, x], send_sem=ag_s.at[phase, d], recv_sem=ag_r.at[phase, d],
                device_id={'tp': chip(d) * 2 + 1 - c}, device_id_type=MESH)
            hops[d].start()

        def pass_on(d):
            slot = lax.rem(x + n_chip - d, n_chip)
            half = 1 - c if d == 0 else c
            cp = pltpu.make_async_remote_copy(
                src_ref=buf.at[half, slot], dst_ref=buf.at[half, slot], send_sem=agp_s.at[phase, d], recv_sem=agp_r.at[phase, d],
                device_id={'tp': partner}, device_id_type=MESH)
            cp.start()
            return cp

        passed = [pass_on(0)]
        for d in sorted(hops, key=lambda d: min(d, n_chip - d)):
            hops[d].wait_recv()
            passed.append(pass_on(d))
        for cp in passed:
            cp.wait_recv()
        sent.extend([*passed, *hops.values()])
        return buf[...].astype(F32).reshape(n_batch, width)

    if last:
        res = res_ref[...].astype(F32)
    else:
        res = res_ref[rows_of(1 - c, 0), :].astype(F32)
    total = reduce_scatter(0, part_ref)
    x_mid = (res + total + bo_ref[layer:layer + 1].astype(F32)).astype(BF16).astype(F32)
    normed = all_gather(0, gath, layer_norm_f32(x_mid, gain_ref[layer, 1:2], shift_ref[layer, 1:2])).astype(BF16)
    w_copies[0].wait()
    up = jnp.dot(normed, wu[...], preferred_element_type=F32) + bu_ref[layer:layer + 1].astype(F32)
    act = jax.nn.gelu(up, approximate=True).astype(BF16)
    if not last:
        wq_copy.start()
    w_copies[1].wait()
    part2[...] = jnp.dot(act, wd[...], preferred_element_type=F32)
    total = reduce_scatter(1, part2)
    x_next = (x_mid + total + bd_ref[layer:layer + 1].astype(F32)).astype(BF16)
    if last:
        out_ref[...] = all_gather(1, gath2, x_next).astype(BF16)
    else:
        own_ref[...] = x_next
        nxt = layer_norm_f32(x_next.astype(F32), gain_ref[layer + 1, 0:1], shift_ref[layer + 1, 0:1])
        normed = all_gather(1, gath2, nxt).astype(BF16)
        wq_copy.wait()
        qkv = jnp.dot(normed, wu[:, :n_qkv], preferred_element_type=F32) + bq_ref[layer + 1:layer + 2].astype(F32)
        out_ref[...] = qkv.astype(BF16).astype(F32)
        for w in w_copies[2:]:
            w.wait()
    for cp in sent:
        cp.wait_send()


def solution(mesh):
    tp_size = mesh.shape['tp']
    vm = pl.BlockSpec(memory_space=pltpu.VMEM)
    sm = pl.BlockSpec(memory_space=pltpu.SMEM)
    hbm = pl.BlockSpec(memory_space=pltpu.HBM)

    def device_step(hidden, ln_gain, ln_shift, w_qkv, b_qkv, w_out, b_out, w_up, b_up, w_down, b_down, k_cache, v_cache, write_slot, key_pos, key_valid):
        n_layers, n_batch, cache_len, n_local, head_dim = k_cache.shape
        width = hidden.shape[-1]
        n_cols = cache_len * n_local
        flat = (n_layers, n_batch, n_cols, head_dim)
        in_hbm = functools.partial(pltpu.with_memory_space_constraint, memory_space=pltpu.HBM)
        k_in, v_in = in_hbm(k_cache.reshape(flat)), in_hbm(v_cache.reshape(flat))
        w_qkv, w_out, w_up, w_down = map(in_hbm, (w_qkv, w_out, w_up, w_down))
        x0 = hidden.reshape(n_batch, width)
        n_groups = n_batch // GROUP
        blk = n_batch // tp_size
        n_chip = tp_size // 2
        shape = jax.ShapeDtypeStruct(flat, BF16)
        held = pltpu.VMEM(flat, BF16)
        shared = [in_hbm(a) for a in (write_slot, key_pos, key_valid)]

        def attn(layer, x_in, caches):
            first = layer == 0
            n_qkv = b_qkv.shape[1]
            scratch = [
                pltpu.VMEM(key_pos.shape, jnp.int32),
                pltpu.VMEM(key_valid.shape, jnp.int32),
                pltpu.SMEM(write_slot.shape, jnp.int32),
                pltpu.VMEM(w_out.shape[1:], BF16),
                pltpu.VMEM((2, n_batch, n_cols), F32),
                pltpu.VMEM((n_batch, n_local * head_dim), F32),
                pltpu.SemaphoreType.DMA((5,)),
                pltpu.SemaphoreType.DMA((7,)),
                pltpu.SemaphoreType.DMA((4,)),
            ]
            alias = {}
            part = jax.ShapeDtypeStruct((n_batch, width), F32)
            outs, out_specs = (part, shape, shape, held, held), (vm, hbm, hbm, vm, vm)
            if first:
                ins = [in_hbm(a) for a in (x_in, ln_gain, ln_shift, b_qkv)] + [w_qkv, w_out] + shared + [k_in, v_in]
                specs = [hbm] * len(ins)
                scratch += [
                    pltpu.VMEM(x_in.shape, BF16),
                    pltpu.VMEM(ln_gain.shape, BF16),
                    pltpu.VMEM(ln_shift.shape, BF16),
                    pltpu.VMEM(b_qkv.shape, BF16),
                    pltpu.VMEM(w_qkv.shape[1:], BF16),
                    pltpu.VMEM((n_batch, n_qkv), F32),
                    pltpu.SemaphoreType.DMA((2, n_groups)),
                ]
            else:
                ins = [x_in, w_out] + shared + list(caches)
                specs = [vm, hbm] + [hbm] * len(shared) + [hbm] * 2 + [vm] * 2
                alias = {len(ins) - 4 + i: 1 + i for i in range(4)}
            return pl.pallas_call(
                functools.partial(attn_kernel, layer, n_local * tp_size, first),
                out_shape=outs,
                in_specs=specs,
                out_specs=out_specs,
                scratch_shapes=scratch,
                input_output_aliases=alias,
                compiler_params=pltpu.CompilerParams(vmem_limit_bytes=13 * MIB),
                name=f'attn_{layer}',
            )(*ins)

        def reduce(layer, part, res, caches=()):
            last = layer == n_layers - 1
            ins = [part, res, ln_gain, ln_shift, b_out, w_up, b_up, w_down, b_down]
            specs = [vm, vm, vm, vm, vm, hbm, vm, hbm, vm]
            outs = [jax.ShapeDtypeStruct((n_batch, width), BF16)]
            if not last:
                ins += [k_in, v_in, w_qkv, b_qkv, *caches]
                specs += [hbm, hbm, hbm, vm, vm, vm]
                outs = [jax.ShapeDtypeStruct((n_batch, b_qkv.shape[1]), F32)]
                outs += [jax.ShapeDtypeStruct((blk, width), BF16), held, held]
            dma = pltpu.SemaphoreType.DMA((2, n_chip))
            return pl.pallas_call(
                functools.partial(reduce_kernel, layer, tp_size, last),
                out_shape=tuple(outs),
                in_specs=specs,
                out_specs=tuple([vm] * len(outs)),
                scratch_shapes=[
                    pltpu.VMEM(w_up.shape[1:], BF16),
                    pltpu.VMEM(w_down.shape[1:], BF16),
                    pltpu.VMEM((n_batch, width), F32),
                    pltpu.VMEM((2, n_chip, blk, width), F32),
                    pltpu.VMEM((2, n_chip, blk, width), F32),
                    pltpu.VMEM((2, n_chip, blk, width), F32),
                    pltpu.VMEM((2, n_chip, blk, width), BF16),
                    pltpu.VMEM((2, n_chip, blk, width), BF16),
                    pltpu.SemaphoreType.DMA((6,)),
                ] + [dma] * 8,
                input_output_aliases={} if last else {len(ins) - 2: 2, len(ins) - 1: 3},
                compiler_params=pltpu.CompilerParams(vmem_limit_bytes=13 * MIB, collective_id=layer, has_side_effects=True),
                name=f'reduce_{layer}',
            )(*ins)

        part, k_new, v_new, k_held, v_held = attn(0, x0, None)
        qkv, x1, k_held, v_held = reduce(0, part, x0, (k_held, v_held))
        part, k_new, v_new, _, _ = attn(1, qkv, (k_new, v_new, k_held, v_held))
        (x_last,) = reduce(1, part, x1)
        return x_last[:, None, :], k_new.reshape(k_cache.shape), v_new.reshape(v_cache.shape)

    cache_spec = P(None, 'dp', None, 'tp', None)
    in_specs = (P('dp', None, None), P(), P(), P(None, None, 'tp'), P(None, 'tp'), P(None, 'tp', None), P(), P(None, None, 'tp'), P(None, 'tp'), P(None, 'tp', None), P(), cache_spec, cache_spec, P('dp'), P('dp', None), P('dp', None))
    out_specs = (P('dp', None, None), cache_spec, cache_spec)
    return jax.shard_map(device_step, mesh=mesh, in_specs=in_specs, out_specs=out_specs, check_vma=False)
```
